32 devices in a mesh: pair: 1 (over z), tp: 4 (over y), side: 8 (over x, core).
Axes of the slice: x: 4, y: 4, z: 1, core: 2. Of those that a mesh axis runs over, the one named last changes fastest.
The devices are a block of a 4x4x8 slice.
Arguments:
- x: bfloat16 [2048, 3072], P(('pair', 'side'))
- req_len: int32 [8], P('pair')
- dest: int32 [8], P('pair')
- w_qkv: bfloat16 [1, 3072, 5120], replicated
- w_out: bfloat16 [1, 3072, 3072], replicated
- w_gate: bfloat16 [1, 3072, 8192], replicated
- w_up: bfloat16 [1, 3072, 8192], replicated
- w_down: bfloat16 [1, 8192, 3072], replicated
- y_tok: bfloat16 [8, 16, 3072], P(('pair', 'side'))
- k_cache: bfloat16 [8, 1, 16, 64, 8, 128], P(('pair', 'side'), None, None, None, 'tp')
- v_cache: bfloat16 [8, 1, 16, 64, 8, 128], P(('pair', 'side'), None, None, None, 'tp')
- c_len: int32 [8, 16], P(('pair', 'side'))
Outputs:
- output 1: bfloat16 [2048, 3072], P(('pair', 'side'))
- output 2: bfloat16 [8, 16, 3072], P(('pair', 'side'))
- output 3: bfloat16 [8, 1, 448, 8, 128], P(('pair', 'side'), None, None, 'tp')
- output 4: bfloat16 [8, 1, 448, 8, 128], P(('pair', 'side'), None, None, 'tp')
- output 5: bfloat16 [8, 1, 16, 64, 8, 128], P(('pair', 'side'), None, None, None, 'tp')
- output 6: bfloat16 [8, 1, 16, 64, 8, 128], P(('pair', 'side'), None, None, None, 'tp')
All inputs are finite; a program needn't handle non-finite values.
Results may differ from the reference program's by a relative error of at most 0.0112437.
Values are sent between devices in bfloat16 or wider.
A program may use at most 768 MiB of HBM per device.

```python
import jax
import jax.numpy as jnp
from jax import lax

TP_SIZE = 4
SIDE_SIZE = 8
MODEL_DIM = 3072
HEADS = 24
KV_HEADS = 8
HEAD_DIM = 128
FF_DIM = 8192
LAYERS = 1
PROMPT_ROWS = 256
BATCH = 16
CACHE_LEN = 64
SEQ_LEN = PROMPT_ROWS * SIDE_SIZE
MAX_REQ = 2 * PROMPT_ROWS - PROMPT_ROWS // 4
GROUP_REP = HEADS // KV_HEADS
KV_LOCAL = KV_HEADS // TP_SIZE
Q_COLS = HEADS * HEAD_DIM
KV_COLS = KV_HEADS * HEAD_DIM
ROPE_BASE = 10000.0
NORM_EPS = 1e-5


def draw_normal(key, shape, scale):
    return (jax.random.normal(key, shape, jnp.float32) * scale).astype(jnp.bfloat16)


def draw_lengths(key):
    quarter = PROMPT_ROWS // 4
    eighth = PROMPT_ROWS // 8
    key_first, key_gap = jax.random.split(key)
    first_len = jax.random.randint(key_first, (SIDE_SIZE // 2,), quarter, 2 * PROMPT_ROWS - quarter + 1)
    gap_len = jax.random.randint(key_gap, (SIDE_SIZE // 2,), 0, eighth + 1)
    first_len = first_len.at[0].set(MAX_REQ)
    gap_len = gap_len.at[0].set(eighth)
    second_len = 2 * PROMPT_ROWS - gap_len - first_len
    return jnp.stack([first_len, second_len], axis=1).reshape(SIDE_SIZE).astype(jnp.int32)


def draw_cache_lengths(key):
    lengths = jax.random.randint(key, (SIDE_SIZE, BATCH), CACHE_LEN // 2, CACHE_LEN)
    lengths = lengths.at[:, 0].set(CACHE_LEN - 1)
    lengths = lengths.at[:, 1].set(CACHE_LEN // 2)
    return lengths.astype(jnp.int32)


def setup_inputs(seed: int = 0, part: int = 0) -> dict:
    part_keys = jax.random.split(jax.random.fold_in(jax.random.key(seed), part), 7)
    weight_keys = jax.random.split(jax.random.key(seed + 1), 5)
    cache_shape = (SIDE_SIZE, LAYERS, BATCH, CACHE_LEN, KV_HEADS, HEAD_DIM)
    return {
        'x': draw_normal(part_keys[0], (SEQ_LEN, MODEL_DIM), 1.0),
        'req_len': draw_lengths(part_keys[1]),
        'dest': jax.random.permutation(part_keys[2], SIDE_SIZE).astype(jnp.int32),
        'w_qkv': draw_normal(weight_keys[0], (LAYERS, MODEL_DIM, Q_COLS + 2 * KV_COLS), MODEL_DIM ** -0.5),
        'w_out': draw_normal(weight_keys[1], (LAYERS, Q_COLS, MODEL_DIM), Q_COLS ** -0.5),
        'w_gate': draw_normal(weight_keys[2], (LAYERS, MODEL_DIM, FF_DIM), MODEL_DIM ** -0.5),
        'w_up': draw_normal(weight_keys[3], (LAYERS, MODEL_DIM, FF_DIM), MODEL_DIM ** -0.5),
        'w_down': draw_normal(weight_keys[4], (LAYERS, FF_DIM, MODEL_DIM), FF_DIM ** -0.5),
        'y_tok': draw_normal(part_keys[3], (SIDE_SIZE, BATCH, MODEL_DIM), 1.0),
        'k_cache': draw_normal(part_keys[4], cache_shape, 1.0),
        'v_cache': draw_normal(part_keys[5], cache_shape, 1.0),
        'c_len': draw_cache_lengths(part_keys[6]),
    }


def rms_norm(hidden):
    wide_vals = hidden.astype(jnp.float32)
    norm_scale = lax.rsqrt(jnp.mean(wide_vals * wide_vals, axis=-1, keepdims=True) + NORM_EPS)
    return (wide_vals * norm_scale).astype(jnp.bfloat16)


def rotary(vectors, positions):
    half_dim = HEAD_DIM // 2
    inv_freq = ROPE_BASE ** (-jnp.arange(half_dim, dtype=jnp.float32) / half_dim)
    angles = positions.astype(jnp.float32)[:, None, None] * inv_freq
    cos_val = jnp.cos(angles)
    sin_val = jnp.sin(angles)
    wide_vals = vectors.astype(jnp.float32)
    lead_half = wide_vals[..., :half_dim]
    tail_half = wide_vals[..., half_dim:]
    return jnp.concatenate([lead_half * cos_val - tail_half * sin_val, tail_half * cos_val + lead_half * sin_val], axis=-1).astype(jnp.bfloat16)


def b_order(array_in, axis):
    shape_in = array_in.shape
    split_shape = shape_in[:axis] + (KV_LOCAL, TP_SIZE) + shape_in[axis + 1:]
    return jnp.swapaxes(array_in.reshape(split_shape), axis, axis + 1).reshape(shape_in)


def split_qkv(w_qkv):
    return w_qkv[..., :Q_COLS], w_qkv[..., Q_COLS:Q_COLS + KV_COLS], w_qkv[..., Q_COLS + KV_COLS:]


def project(hidden, wq_l, wk_l, wv_l, positions):
    row_count = hidden.shape[0]
    normed = rms_norm(hidden)
    query = jnp.dot(normed, wq_l, preferred_element_type=jnp.float32).astype(jnp.bfloat16)
    key_new = jnp.dot(normed, wk_l, preferred_element_type=jnp.float32).astype(jnp.bfloat16)
    value_new = jnp.dot(normed, wv_l, preferred_element_type=jnp.float32).astype(jnp.bfloat16)
    query = rotary(query.reshape(row_count, HEADS, HEAD_DIM), positions)
    key_new = rotary(key_new.reshape(row_count, KV_HEADS, HEAD_DIM), positions)
    return query.reshape(row_count, KV_HEADS, GROUP_REP, HEAD_DIM), key_new, value_new.reshape(row_count, KV_HEADS, HEAD_DIM)


def finish_layer(hidden, context, wo_l, wg_l, wu_l, wd_l):
    attn_out = jnp.dot(context, wo_l, preferred_element_type=jnp.float32).astype(jnp.bfloat16)
    hidden = (hidden.astype(jnp.float32) + attn_out.astype(jnp.float32)).astype(jnp.bfloat16)
    normed = rms_norm(hidden)
    gate = jnp.dot(normed, wg_l, preferred_element_type=jnp.float32).astype(jnp.bfloat16)
    upper = jnp.dot(normed, wu_l, preferred_element_type=jnp.float32).astype(jnp.bfloat16)
    activated = (jax.nn.silu(gate.astype(jnp.float32)) * upper.astype(jnp.float32)).astype(jnp.bfloat16)
    down = jnp.dot(activated, wd_l, preferred_element_type=jnp.float32).astype(jnp.bfloat16)
    return (hidden.astype(jnp.float32) + down.astype(jnp.float32)).astype(jnp.bfloat16)


def prefill(x, req_len, w_qkv, w_out, w_gate, w_up, w_down):
    row_ids = jnp.arange(SEQ_LEN)
    past_end = row_ids[:, None] >= jnp.cumsum(req_len)[None, :]
    seg_id = jnp.sum(past_end.astype(jnp.int32), axis=1)
    positions = row_ids - jnp.sum(jnp.where(past_end, req_len[None, :], 0), axis=1)
    allowed = (seg_id[:, None] == seg_id[None, :]) & (row_ids[None, :] <= row_ids[:, None])
    w_q, w_k, w_v = split_qkv(w_qkv)

    def head_attention(operands):
        q_head, k_head, v_head = operands
        scores = jnp.einsum('srd,td->rst', q_head.astype(jnp.float32), k_head.astype(jnp.float32)) * HEAD_DIM ** -0.5
        scores = jnp.where(allowed[None], scores, -1e30)
        attn_prob = jax.nn.softmax(scores, axis=-1).astype(jnp.bfloat16)
        return jnp.einsum('rst,td->srd', attn_prob.astype(jnp.float32), v_head.astype(jnp.float32)).astype(jnp.bfloat16)

    def layer_step(hidden, weights):
        wq_l, wk_l, wv_l, wo_l, wg_l, wu_l, wd_l = weights
        query, key_new, value_new = project(hidden, wq_l, wk_l, wv_l, positions)
        context = lax.map(head_attention, (jnp.swapaxes(query, 0, 1), jnp.swapaxes(key_new, 0, 1), jnp.swapaxes(value_new, 0, 1)))
        context = jnp.swapaxes(context, 0, 1).reshape(SEQ_LEN, Q_COLS)
        return finish_layer(hidden, context, wo_l, wg_l, wu_l, wd_l), (key_new, value_new)

    return lax.scan(layer_step, x, (w_q, w_k, w_v, w_out, w_gate, w_up, w_down))


def install(full, req_len, dest):
    starts = jnp.cumsum(req_len) - req_len
    match = dest[None, :] == jnp.arange(SIDE_SIZE)[:, None]
    start_of = jnp.sum(jnp.where(match, starts[None, :], 0), axis=1)
    length_of = jnp.sum(jnp.where(match, req_len[None, :], 0), axis=1)
    padded = jnp.concatenate([full, jnp.zeros((LAYERS, MAX_REQ, KV_HEADS, HEAD_DIM), full.dtype)], axis=1)

    def one_group(start_row, length):
        piece = lax.dynamic_slice_in_dim(padded, start_row, MAX_REQ, axis=1)
        keep = (jnp.arange(MAX_REQ) < length)[None, :, None, None]
        return b_order(jnp.where(keep, piece, jnp.zeros_like(piece)), 2)

    return jax.vmap(one_group)(start_of, length_of)


def decode(y_tok, k_cache, v_cache, c_len, w_qkv, w_out, w_gate, w_up, w_down):
    w_q, w_k, w_v = split_qkv(w_qkv)
    wq_b = b_order(w_q.reshape(LAYERS, MODEL_DIM, KV_HEADS, GROUP_REP * HEAD_DIM), 2).reshape(LAYERS, MODEL_DIM, Q_COLS)
    wk_b = b_order(w_k.reshape(LAYERS, MODEL_DIM, KV_HEADS, HEAD_DIM), 2).reshape(LAYERS, MODEL_DIM, KV_COLS)
    wv_b = b_order(w_v.reshape(LAYERS, MODEL_DIM, KV_HEADS, HEAD_DIM), 2).reshape(LAYERS, MODEL_DIM, KV_COLS)
    wo_b = b_order(w_out.reshape(LAYERS, KV_HEADS, GROUP_REP * HEAD_DIM, MODEL_DIM), 1).reshape(LAYERS, Q_COLS, MODEL_DIM)
    cache_pos = jnp.arange(CACHE_LEN)

    def one_group(operands):
        tokens, k_group, v_group, lengths = operands
        visible = cache_pos[None, :] <= lengths[:, None]
        at_slot = (cache_pos[None, :] == lengths[:, None])[:, :, None, None]

        def layer_step(hidden, weights):
            wq_l, wk_l, wv_l, wo_l, wg_l, wu_l, wd_l, k_layer, v_layer = weights
            query, key_new, value_new = project(hidden, wq_l, wk_l, wv_l, lengths)
            k_layer = jnp.where(at_slot, key_new[:, None], k_layer)
            v_layer = jnp.where(at_slot, value_new[:, None], v_layer)
            scores = jnp.einsum('bkrd,btkd->bkrt', query.astype(jnp.float32), k_layer.astype(jnp.float32)) * HEAD_DIM ** -0.5
            scores = jnp.where(visible[:, None, None, :], scores, -1e30)
            attn_prob = jax.nn.softmax(scores, axis=-1).astype(jnp.bfloat16)
            context = jnp.einsum('bkrt,btkd->bkrd', attn_prob.astype(jnp.float32), v_layer.astype(jnp.float32)).astype(jnp.bfloat16)
            hidden = finish_layer(hidden, context.reshape(BATCH, Q_COLS), wo_l, wg_l, wu_l, wd_l)
            return hidden, (k_layer, v_layer)

        hidden, (k_new, v_new) = lax.scan(layer_step, tokens, (wq_b, wk_b, wv_b, wo_b, w_gate, w_up, w_down, k_group, v_group))
        return hidden, k_new, v_new

    return lax.map(one_group, (y_tok, k_cache, v_cache, c_len))


def reference(x, req_len, dest, w_qkv, w_out, w_gate, w_up, w_down, y_tok, k_cache, v_cache, c_len):
    hidden, (keys_all, values_all) = prefill(x, req_len, w_qkv, w_out, w_gate, w_up, w_down)
    k_prompt = install(keys_all, req_len, dest)
    v_prompt = install(values_all, req_len, dest)
    dec_out, k_new, v_new = decode(y_tok, k_cache, v_cache, c_len, w_qkv, w_out, w_gate, w_up, w_down)
    return (hidden, dec_out, k_prompt, v_prompt, k_new, v_new)
```

```python
import jax
import jax.numpy as jnp
from jax import lax
from jax.experimental import pallas as pl
from jax.experimental.pallas import tpu as pltpu
from jax.sharding import PartitionSpec as P

ROPE_BASE = 10000.0
NORM_EPS = 1e-5
BF = jnp.bfloat16
F32 = jnp.float32
CW = 256
GU_SLOTS = 8
MESH = pl.DeviceIdType.MESH


def mult(v, m):
    return pl.multiple_of(v, m)


def make_kernel(tp_size, side_size, R, D, B, T, Q, KV, HD, F, max_req):
    heads_local = Q // HD // tp_size
    rep = heads_local // 2
    hw = rep * HD
    qw = 2 * hw
    RT = R // tp_size
    DH = D // 2
    FH = F // 2
    M1 = R + B
    M2 = 2 * RT + 2 * B
    n_kv, n_q = 2 * 2 * HD // CW, qw // CW
    n_o, n_g, n_d = DH // CW, FH // CW, DH // CW
    wo_base = (n_kv + n_q) * D
    gu_base = wo_base + n_o * Q
    slab_rows = gu_base + GU_SLOTS * 2 * D
    CK = B * T * 2
    PR = max_req * 2
    scale = HD ** -0.5
    nblk = side_size

    def kernel(x_h, y_h, wqkv_h, wo_h, wg_h, wu_h, wd_h, kc_h, vc_h, rl, dst, cl, fq,
               hid_o, dec_o, kp_o, vp_o, kn_o, vn_o,
               slab, xs, ys, xn, raw, qs, kva, knv, kcs, vcs, cos_s, sin_s,
               dcs, cst, ctxr, xres, hf, hn, act, outst, hid, decb, kps, vps,
               in_sem, w_sem, g_sem, d_sem, xr_s, xr_r, kx_s, kx_r, cx_s, cx_r, cf_s, cf_r,
               dx_s, dx_r, df_s, df_r, h_s, h_r, a_s, a_r, f_s, f_r, r_s, r_r, o_sem):
        side = lax.axis_index('side')
        tp = lax.axis_index('tp')
        core = lax.rem(side, 2)
        oc = 1 - core
        partner = side + 1 - 2 * core
        left = lax.rem(side + side_size - 2, side_size)
        right = lax.rem(side + 2, side_size)
        far = lax.rem(side + 4, side_size)
        p_left = lax.rem(partner + side_size - 2, side_size)
        p_right = lax.rem(partner + 2, side_size)
        p_far = lax.rem(partner + 4, side_size)

        def at(d):
            return lax.rem(tp + d, tp_size)

        def dev(s, t):
            return {'side': s, 'tp': t}

        q_cols0, k_cols0, v_cols0 = 0, Q, Q + KV
        hcol = [tp * hw, (tp + tp_size) * hw]
        kcol = [k_cols0 + tp * HD, k_cols0 + (tp + tp_size) * HD]
        vcol = [v_cols0 + tp * HD, v_cols0 + (tp + tp_size) * HD]

        def pieces(u):
            if u == 0:
                return [(kcol[0], 0, HD), (kcol[1], HD, HD)]
            if u == 1:
                return [(vcol[0], 0, HD), (vcol[1], HD, HD)]
            lo, hi = (u - 2) * CW, (u - 1) * CW
            out = []
            for j in range(2):
                a, b = max(lo, j * hw), min(hi, (j + 1) * hw)
                if a < b:
                    out.append((hcol[j] + (a - j * hw), a - lo, b - a))
            return out

        def start_qkv(u):
            for src, d0, w in pieces(u):
                pltpu.make_async_copy(wqkv_h.at[:, pl.ds(mult(src, 128), w)],
                                      slab.at[pl.ds(u * D, D), pl.ds(d0, w)], w_sem.at[u]).start()

        def slab_wait(base, rows, sem):
            pltpu.make_async_copy(slab.at[pl.ds(base, rows), :], slab.at[pl.ds(base, rows), :], sem).wait()

        def start_wo(u):
            col = mult(core * DH + u * CW, 128)
            for t in range(tp_size):
                for j in range(2):
                    pltpu.make_async_copy(wo_h.at[pl.ds((t + j * tp_size) * hw, hw), pl.ds(col, CW)],
                                          slab.at[pl.ds(wo_base + u * Q + t * qw + j * hw, hw), :],
                                          w_sem.at[n_kv + n_q + u]).start()

        def start_gu(j, slot):
            col = mult(core * FH + j * CW, 128)
            base = mult(gu_base + slot * (2 * D), 256)
            pltpu.make_async_copy(wg_h.at[:, pl.ds(col, CW)], slab.at[pl.ds(base, D), :], g_sem.at[slot]).start()
            pltpu.make_async_copy(wu_h.at[:, pl.ds(col, CW)], slab.at[pl.ds(mult(base + D, 256), D), :], g_sem.at[slot]).start()

        def d_copy(n):
            return pltpu.make_async_copy(wd_h.at[:, pl.ds(mult(core * DH + n * CW, 128), CW)],
                                         slab.at[pl.ds(mult(n * F, 256), F), :], d_sem.at[n])

        x_in = pltpu.make_async_copy(x_h, xs, in_sem.at[0])
        y_in = pltpu.make_async_copy(y_h, ys, in_sem.at[1])
        x_in.start()
        y_in.start()
        for u in range(n_kv + n_q):
            start_qkv(u)

        peers = [(partner, tp), (left, tp), (right, tp), (side, at(1)), (side, at(tp_size - 1)), (side, at(2)),
                 (partner, at(1)), (partner, at(tp_size - 1))]
        barrier = pltpu.get_barrier_semaphore()
        for s, t in peers:
            pl.semaphore_signal(barrier, inc=1, device_id=dev(s, t), device_id_type=MESH)

        kc_in = pltpu.make_async_copy(kc_h, kcs, in_sem.at[2])
        vc_in = pltpu.make_async_copy(vc_h, vcs, in_sem.at[3])
        kc_in.start()
        vc_in.start()
        row_t = mult(tp * RT, RT)
        my_cols = mult(core * DH, 128)
        xres_l = [pltpu.make_async_copy(x_h.at[pl.ds(row_t, RT), pl.ds(my_cols, DH)],
                                        xres.at[pl.ds(mult(core * RT, RT), RT), :], in_sem.at[4]),
                  pltpu.make_async_copy(y_h.at[:, pl.ds(my_cols, DH)],
                                        xres.at[pl.ds(mult(2 * RT + core * B, B), B), :], in_sem.at[5])]
        for cp in xres_l:
            cp.start()

        def seg_of(rows):
            seg = jnp.zeros_like(rows)
            total = jnp.int32(0)
            for r in range(nblk):
                total = total + rl[r]
                seg = jnp.where(rows >= total, total, seg)
            return seg

        idx = lax.broadcasted_iota(jnp.int32, (M1, 1), 0)
        rows = idx + side * R
        pos = rows - seg_of(rows)
        for b in range(B):
            pos = jnp.where(idx == R + b, cl[b], pos)
        ang = pos.astype(F32) * fq[0:1, :]
        cos_s[...] = jnp.cos(ang)
        sin_s[...] = jnp.sin(ang) * fq[1:2, :]

        def norm(v):
            w = v.astype(F32)
            sc = lax.rsqrt(jnp.sum(w * w, axis=-1, keepdims=True) / D + NORM_EPS)
            return (w * sc).astype(BF)

        x_in.wait()

        def norm_x(i, c):
            r = pl.ds(mult(i * 32, 32), 32)
            xn[r, :] = norm(xs[r, :])
            return c

        lax.fori_loop(0, R // 32, norm_x, 0)
        y_in.wait()
        xn[pl.ds(R, B), :] = norm(ys[...])

        pl.semaphore_wait(barrier, len(peers))

        def remote(src, dst_ref, ss, rs, s, t):
            return pltpu.make_async_remote_copy(src_ref=src, dst_ref=dst_ref, send_sem=ss, recv_sem=rs,
                                                device_id=dev(s, t), device_id_type=MESH)

        his_cols = mult(oc * DH, 128)
        xres_r = [remote(x_h.at[pl.ds(row_t, RT), pl.ds(his_cols, DH)], xres.at[pl.ds(mult(core * RT, RT), RT), :],
                         xr_s.at[0], xr_r.at[0], partner, tp),
                  remote(y_h.at[:, pl.ds(his_cols, DH)], xres.at[pl.ds(mult(2 * RT + core * B, B), B), :],
                         xr_s.at[1], xr_r.at[1], partner, tp)]
        for cp in xres_r:
            cp.start()

        def project(u):
            w = slab[pl.ds(mult(u * D, 256), D), :]
            raw[u] = jnp.dot(xn[...], w, preferred_element_type=F32).astype(BF)

        def rope(v):
            w = v.astype(F32)
            return (w * cos_s[...] + pltpu.roll(w, HD // 2, 1) * sin_s[...]).astype(BF)

        def project_loop(i, c):
            slab_wait(mult(i * D, 256), D, w_sem.at[i])
            project(i)
            return c

        for u in range(n_o):
            start_wo(u)
        lax.fori_loop(0, n_kv, project_loop, 0)
        for j in range(2):
            k_j = rope(raw[0, :, pl.ds(j * HD, HD)])
            kva[side, j] = k_j[:R]
            knv[pl.ds(j * B, B), pl.ds(0, HD)] = k_j[R:]
            v_j = raw[1, :, pl.ds(j * HD, HD)]
            kva[side, 2 + j] = v_j[:R]
            knv[pl.ds(j * B, B), pl.ds(HD, HD)] = v_j[R:]
        knv[:, pl.ds(2 * HD, HD)] = jnp.ones((2 * B, HD), BF)

        lo, hi = pl.ds(0, 2), pl.ds(2, 2)
        kx = [remote(kva.at[side], kva.at[side], kx_s.at[0], kx_r.at[0], partner, tp),
              remote(kva.at[side], kva.at[side], kx_s.at[1], kx_r.at[1], right, tp),
              remote(kva.at[side], kva.at[side], kx_s.at[2], kx_r.at[2], left, tp),
              remote(kva.at[left, lo], kva.at[left, lo], kx_s.at[3], kx_r.at[3], right, tp),
              remote(kva.at[right, hi], kva.at[right, hi], kx_s.at[4], kx_r.at[4], left, tp),
              remote(kva.at[left], kva.at[left], kx_s.at[5], kx_r.at[5], partner, tp),
              remote(kva.at[right], kva.at[right], kx_s.at[6], kx_r.at[6], partner, tp),
              remote(kva.at[far, lo], kva.at[far, lo], kx_s.at[7], kx_r.at[7], partner, tp),
              remote(kva.at[far, hi], kva.at[far, hi], kx_s.at[8], kx_r.at[8], partner, tp)]
        for i in (1, 0, 2):
            kx[i].start()

        def got(i):
            blk = (partner, left, right, far, far, p_left, p_right, p_far, p_far)[i]
            ref = kva.at[blk, lo] if i in (3, 7) else kva.at[blk, hi] if i in (4, 8) else kva.at[blk]
            pltpu.make_async_copy(ref, ref, kx_r.at[i]).wait()

        lax.fori_loop(n_kv, n_kv + n_q, project_loop, 0)
        for slot in range(GU_SLOTS):
            start_gu(slot, slot)
        d_copy(0).start()
        for h in range(heads_local):
            u, off = divmod(h * HD, CW)
            qs[h] = rope(raw[2 + u, :, pl.ds(off, HD)])

        kc_in.wait()
        vc_in.wait()
        lane2 = lax.broadcasted_iota(jnp.int32, (1, 2 * B), 1)
        len2 = jnp.zeros((1, 2 * B), jnp.int32)
        for b in range(B):
            len2 = jnp.where(lax.rem(lane2, B) == b, cl[b], len2)
        code2 = (lax.rem(lane2, B) * T + len2) * 2 + lane2 // B
        CH = 256

        def insert(i, c):
            r0 = mult(i * CH, CH)
            rr = lax.broadcasted_iota(jnp.int32, (CH, 1), 0) + r0
            pick = jnp.where(rr == code2, 1.0, 0.0).astype(BF)
            new = jnp.dot(pick, knv[...], preferred_element_type=F32)
            hit = new[:, 2 * HD:] > 0.5
            sl = pl.ds(r0, CH)
            kcs[sl, :] = jnp.where(hit, new[:, :HD], kcs[sl, :].astype(F32)).astype(BF)
            vcs[sl, :] = jnp.where(hit, new[:, HD:2 * HD], vcs[sl, :].astype(F32)).astype(BF)
            return c

        lax.fori_loop(0, CK // CH, insert, 0)
        kn_out = pltpu.make_async_copy(kcs, kn_o, o_sem.at[0])
        vn_out = pltpu.make_async_copy(vcs, vn_o, o_sem.at[1])
        kn_out.start()
        vn_out.start()

        HB = heads_local * B
        q_dec = qs[:, pl.ds(R, B), :].reshape(HB, HD)
        s_dec = lax.dot_general(q_dec, kcs[...], (((1,), (1,)), ((), ())), preferred_element_type=F32) * scale
        qi = lax.broadcasted_iota(jnp.int32, (HB, 1), 0)
        ki = lax.broadcasted_iota(jnp.int32, (1, CK), 1)
        q_len = jnp.zeros((HB, 1), jnp.int32)
        for b in range(B):
            q_len = jnp.where(lax.rem(qi, B) == b, cl[b], q_len)
        q_code = lax.rem(qi, B) * 2 + qi // (rep * B)
        k_code = (ki // (2 * T)) * 2 + lax.rem(ki, 2)
        k_pos = lax.rem(ki // 2, T)
        s_dec = jnp.where((q_code == k_code) & (k_pos <= q_len), s_dec, -1e30)
        e_dec = jnp.exp(s_dec - jnp.max(s_dec, axis=-1, keepdims=True))
        p_dec = (e_dec / jnp.sum(e_dec, axis=-1, keepdims=True)).astype(BF)
        c_dec = jnp.dot(p_dec, vcs[...], preferred_element_type=F32).astype(BF)
        for h in range(heads_local):
            dcs[:, pl.ds(h * HD, HD)] = c_dec[h * B:(h + 1) * B]
        dec_rows = pl.ds(mult(2 * RT + core * B, B), B)
        hops = (2, 1, 3, 0)
        srcs = (2, 3, 1)
        dx = [remote(dcs, ctxr.at[tp, dec_rows, :], dx_s.at[k], dx_r.at[k], side, at(hops[k])) for k in range(3)]
        for cp in dx:
            cp.start()
        ctxr[tp, dec_rows, :] = dcs[...]
        df_own = remote(dcs, ctxr.at[tp, dec_rows, :], df_s.at[3], df_r.at[3], partner, tp)
        df_own.start()

        got(1)
        kx[5].start()
        kx[3].start()
        got(2)
        kx[6].start()
        kx[4].start()

        df = []
        for k in range(3):
            ref = ctxr.at[at(srcs[k]), dec_rows, :]
            pltpu.make_async_copy(ref, ref, dx_r.at[k]).wait()
            df.append(remote(ref, ref, df_s.at[k], df_r.at[k], partner, tp))
            df[k].start()

        got(0)
        got(5)

        blks = [lax.rem(side + side_size - 2, side_size), lax.rem(side + side_size - 1, side_size), side]
        pre_rows = pl.ds(mult(core * RT, RT), RT)
        key_row = (side - 2) * R + lax.broadcasted_iota(jnp.int32, (1, 3 * R), 1)
        cx = []
        for k in range(4):
            r0 = mult(at(hops[k]) * RT, RT)
            q_row = side * R + r0 + lax.broadcasted_iota(jnp.int32, (RT, 1), 0)
            q_seg = seg_of(q_row)

            def head(h, c, k=k, r0=r0, q_row=q_row, q_seg=q_seg):
                q = qs[h, pl.ds(r0, RT), :]
                j = h // rep
                s = jnp.concatenate([lax.dot_general(q, kva[b, j], (((1,), (1,)), ((), ())), preferred_element_type=F32)
                                     for b in blks], axis=-1) * scale
                s = jnp.where((key_row >= q_seg) & (key_row <= q_row), s, -1e30)
                e = jnp.exp(s - jnp.max(s, axis=-1, keepdims=True))
                p = (e / jnp.sum(e, axis=-1, keepdims=True)).astype(BF)
                o = jnp.zeros((RT, HD), F32)
                for i, b in enumerate(blks):
                    o = o + jnp.dot(p[:, i * R:(i + 1) * R], kva[b, 2 + j], preferred_element_type=F32)
                cst[k, :, pl.ds(mult(h * HD, HD), HD)] = o.astype(BF)
                return c

            lax.fori_loop(0, heads_local, head, 0)
            if k < 3:
                cx.append(remote(cst.at[k], ctxr.at[tp, pre_rows, :], cx_s.at[k], cx_r.at[k], side, at(hops[k])))
                cx[k].start()
        ctxr[tp, pre_rows, :] = cst[3]
        cf = [None] * 4
        cf[3] = remote(cst.at[3], ctxr.at[tp, pre_rows, :], cf_s.at[3], cf_r.at[3], partner, tp)
        cf[3].start()
        for i in (3, 4):
            got(i)
            kx[i + 4].start()
        for k in range(3):
            ref = ctxr.at[at(srcs[k]), pre_rows, :]
            pltpu.make_async_copy(ref, ref, cx_r.at[k]).wait()
            cf[k] = remote(ref, ref, cf_s.at[k], cf_r.at[k], partner, tp)
            cf[k].start()

        p_pre = pl.ds(mult(oc * RT, RT), RT)
        p_dec_rows = pl.ds(mult(2 * RT + oc * B, B), B)
        for k in range(4):
            t = at(srcs[k]) if k < 3 else tp
            ref = ctxr.at[t, p_pre, :]
            pltpu.make_async_copy(ref, ref, cf_r.at[k]).wait()
            ref = ctxr.at[t, p_dec_rows, :]
            pltpu.make_async_copy(ref, ref, df_r.at[k]).wait()
        for cp in xres_l:
            cp.wait()
        for i, cp in enumerate(xres_r):
            cp.wait_send()
        ref = xres.at[p_pre, :]
        pltpu.make_async_copy(ref, ref, xr_r.at[0]).wait()
        ref = xres.at[p_dec_rows, :]
        pltpu.make_async_copy(ref, ref, xr_r.at[1]).wait()

        def h_copy(u):
            ref = hf.at[:, pl.ds(mult(core * DH + u * CW, CW), CW)]
            return remote(ref, ref, h_s.at[u], h_r.at[u], partner, tp)

        def out_proj(u, c):
            base = wo_base + u * Q
            slab_wait(mult(base, 256), Q, w_sem.at[n_kv + n_q + u])
            acc = jnp.zeros((M2, CW), F32)
            for t in range(tp_size):
                acc = acc + jnp.dot(ctxr[t], slab[pl.ds(mult(base + t * qw, 256), qw), :], preferred_element_type=F32)
            res = xres[:, pl.ds(mult(u * CW, CW), CW)].astype(F32)
            hf[:, pl.ds(mult(core * DH + u * CW, CW), CW)] = (res + acc.astype(BF).astype(F32)).astype(BF)
            h_copy(u).start()
            return c

        lax.fori_loop(0, n_o, out_proj, 0)
        n_early = gu_base // F
        for n in range(1, n_early):
            d_copy(n).start()
        for u in range(n_o):
            ref = hf.at[:, pl.ds(mult(oc * DH + u * CW, CW), CW)]
            pltpu.make_async_copy(ref, ref, h_r.at[u]).wait()

        def norm_h(i, c):
            r = pl.ds(mult(i * 32, 32), 32)
            hn[r, :] = norm(hf[r, :])
            return c

        lax.fori_loop(0, M2 // 32, norm_h, 0)

        def a_copy(j):
            ref = act.at[:, pl.ds(mult(core * FH + j * CW, CW), CW)]
            return remote(ref, ref, a_s.at[j], a_r.at[j], partner, tp)

        def last_slot(n):
            top = (n + 1) * F - gu_base
            slot = (top - 1) // (2 * D)
            return slot + ((n_g - 1 - slot) // GU_SLOTS) * GU_SLOTS

        def gate_up(j, c):
            slot = lax.rem(j, GU_SLOTS)
            base = mult(gu_base + slot * (2 * D), 256)
            slab_wait(base, 2 * D, g_sem.at[slot])
            g = jnp.dot(hn[...], slab[pl.ds(base, D), :], preferred_element_type=F32)
            u = jnp.dot(hn[...], slab[pl.ds(mult(base + D, 256), D), :], preferred_element_type=F32)
            g = g.astype(BF).astype(F32)
            u = u.astype(BF).astype(F32)
            act[:, pl.ds(mult(core * FH + j * CW, CW), CW)] = (g * jax.nn.sigmoid(g) * u).astype(BF)
            a_copy(j).start()

            @pl.when(j + GU_SLOTS < n_g)
            def _():
                start_gu(j + GU_SLOTS, slot)

            for n in range(n_early, n_d):
                @pl.when(j == last_slot(n))
                def _(n=n):
                    d_copy(n).start()
            return c

        lax.fori_loop(0, n_g, gate_up, 0)

        def a_got(j, c):
            ref = act.at[:, pl.ds(mult(oc * FH + j * CW, CW), CW)]
            pltpu.make_async_copy(ref, ref, a_r.at[j]).wait()
            return c

        lax.fori_loop(0, n_g, a_got, 0)

        up, down = at(1), at(tp_size - 1)
        own_out = pl.ds(mult(core * RT, RT), RT)
        his_out = pl.ds(mult(oc * RT, RT), RT)
        own_dec = pl.ds(mult(2 * RT + core * B, B), B)
        his_dec = pl.ds(mult(2 * RT + oc * B, B), B)
        rows_of = lambda t: pl.ds(mult(t * RT, RT), RT)

        def f_copies(n):
            cols = pl.ds(mult(core * DH + n * CW, CW), CW)
            there = hid.at[rows_of(tp), cols]
            mine, his = outst.at[n, own_out, :], outst.at[n, his_out, :]
            return [remote(mine, there, f_s.at[0, n], f_r.at[0, n], side, up),
                    remote(mine, there, f_s.at[1, n], f_r.at[1, n], side, down),
                    remote(his, there, f_s.at[2, n], f_r.at[2, n], partner, up),
                    remote(his, there, f_s.at[3, n], f_r.at[3, n], partner, down),
                    remote(his, there, f_s.at[4, n], f_r.at[4, n], partner, tp),
                    remote(outst.at[n, his_dec, :], decb.at[:, cols], f_s.at[5, n], f_r.at[5, n], partner, tp)]

        def down_proj(n, c):
            d_copy(n).wait()
            acc = jnp.dot(act[...], slab[pl.ds(mult(n * F, 256), F), :], preferred_element_type=F32)
            cols = pl.ds(mult(core * DH + n * CW, CW), CW)
            outst[n] = (hf[:, cols].astype(F32) + acc.astype(BF).astype(F32)).astype(BF)
            for cp in f_copies(n):
                cp.start()
            hid[rows_of(tp), cols] = outst[n, own_out, :]
            decb[:, cols] = outst[n, own_dec, :]
            return c

        lax.fori_loop(0, n_d, down_proj, 0)

        def piece(t, c_from, n):
            return hid.at[rows_of(t), pl.ds(mult(c_from * DH + n * CW, CW), CW)]

        def arrived(ref, sem):
            pltpu.make_async_copy(ref, ref, sem).wait()

        kind = {(0, 1): 0, (1, 1): 1, (0, 0): 2, (1, 0): 3}
        relays = []
        for n in range(n_d):
            for same in (1, 0):
                c_from = core if same else oc
                if n % 2 == 0:
                    ref = piece(down, c_from, n)
                    arrived(ref, f_r.at[kind[(0, same)], n])
                    cp = remote(ref, ref, r_s.at[same, n], r_r.at[same, n], side, up)
                else:
                    ref = piece(up, c_from, n)
                    arrived(ref, f_r.at[kind[(1, same)], n])
                    cp = remote(ref, ref, r_s.at[same, n], r_r.at[same, n], side, down)
                cp.start()
                relays.append(cp)

        for i in (6, 7, 8):
            got(i)
        start, length, total = jnp.int32(0), jnp.int32(0), jnp.int32(0)
        for r in range(nblk):
            mine = dst[r] == side
            start = start + jnp.where(mine, total, 0)
            length = length + jnp.where(mine, rl[r], 0)
            total = total + rl[r]
        o_row = lax.broadcasted_iota(jnp.int32, (PR, 1), 0)
        want = jnp.where(o_row // 2 < length, o_row // 2 + start, -1)
        col = lax.broadcasted_iota(jnp.int32, (1, 2 * R), 1)
        col_slot, col_row = col // R, lax.rem(col, R)
        code = want * 2 + lax.rem(o_row, 2)

        def install(b, c):
            kacc, vacc = c
            pick = jnp.where(code == (col_row + b * R) * 2 + col_slot, 1.0, 0.0).astype(BF)
            kk = kva[b, pl.ds(0, 2)].reshape(2 * R, HD)
            vv = kva[b, pl.ds(2, 2)].reshape(2 * R, HD)
            kps[...] = kps[...] + jnp.dot(pick, kk, preferred_element_type=F32).astype(BF)
            vps[...] = vps[...] + jnp.dot(pick, vv, preferred_element_type=F32).astype(BF)
            return c

        kps[...] = jnp.zeros((PR, HD), BF)
        vps[...] = jnp.zeros((PR, HD), BF)
        lax.fori_loop(0, nblk, install, (0, 0))
        outs = [pltpu.make_async_copy(kps, kp_o, o_sem.at[2]), pltpu.make_async_copy(vps, vp_o, o_sem.at[3])]
        for cp in outs:
            cp.start()

        def flush(t, i):
            r = rows_of(t)
            cp = pltpu.make_async_copy(hid.at[r, :], hid_o.at[r, :], o_sem.at[4 + i])
            cp.start()
            outs.append(cp)

        for n in range(n_d):
            arrived(piece(tp, oc, n), f_r.at[4, n])
            arrived(decb.at[:, pl.ds(mult(oc * DH + n * CW, CW), CW)], f_r.at[5, n])
        flush(tp, 0)
        cp = pltpu.make_async_copy(decb, dec_o, o_sem.at[8])
        cp.start()
        outs.append(cp)
        for n in range(n_d):
            for same in (1, 0):
                c_from = core if same else oc
                if n % 2 == 0:
                    arrived(piece(up, c_from, n), f_r.at[kind[(1, same)], n])
                else:
                    arrived(piece(down, c_from, n), f_r.at[kind[(0, same)], n])
        flush(up, 1)
        flush(down, 2)
        for n in range(n_d):
            for same in (1, 0):
                arrived(piece(at(2), core if same else oc, n), r_r.at[same, n])
        flush(at(2), 3)

        for cp in kx + dx + df + [df_own] + cx + cf + relays:
            cp.wait_send()

        def h_done(u, c):
            h_copy(u).wait_send()
            return c

        def a_done(j, c):
            a_copy(j).wait_send()
            return c

        def f_done(n, c):
            for cp in f_copies(n):
                cp.wait_send()
            return c

        lax.fori_loop(0, n_o, h_done, 0)
        lax.fori_loop(0, n_g, a_done, 0)
        lax.fori_loop(0, n_d, f_done, 0)
        kn_out.wait()
        vn_out.wait()
        for cp in outs:
            cp.wait()

    dma = lambda *s: pltpu.SemaphoreType.DMA(s)
    scratch = [
        pltpu.VMEM((slab_rows, CW), BF),
        pltpu.VMEM((R, D), BF), pltpu.VMEM((B, D), BF), pltpu.VMEM((M1, D), BF),
        pltpu.VMEM((n_kv + n_q, M1, CW), BF), pltpu.VMEM((heads_local, M1, HD), BF),
        pltpu.VMEM((nblk, 4, R, HD), BF), pltpu.VMEM((2 * B, 3 * HD), BF),
        pltpu.VMEM((CK, HD), BF), pltpu.VMEM((CK, HD), BF),
        pltpu.VMEM((M1, HD), F32), pltpu.VMEM((M1, HD), F32),
        pltpu.VMEM((B, qw), BF), pltpu.VMEM((4, RT, qw), BF), pltpu.VMEM((tp_size, M2, qw), BF),
        pltpu.VMEM((M2, DH), BF), pltpu.VMEM((M2, D), BF), pltpu.VMEM((M2, D), BF), pltpu.VMEM((M2, F), BF),
        pltpu.VMEM((n_d, M2, CW), BF), pltpu.VMEM((R, D), BF), pltpu.VMEM((B, D), BF),
        pltpu.VMEM((PR, HD), BF), pltpu.VMEM((PR, HD), BF),
        dma(6), dma(n_kv + n_q + n_o), dma(GU_SLOTS), dma(n_d),
        dma(2), dma(2), dma(9), dma(9), dma(3), dma(3), dma(4), dma(4),
        dma(3), dma(3), dma(4), dma(4), dma(n_o), dma(n_o), dma(n_g), dma(n_g),
        dma(6, n_d), dma(6, n_d), dma(2, n_d), dma(2, n_d), dma(9),
    ]
    return kernel, scratch, (R, D, B, PR, HD, CK)


def solution(mesh):
    tp_size = mesh.shape['tp']
    side_size = mesh.shape['side']
    rows_spec = P(('pair', 'side'), None)
    batch_spec = P(('pair', 'side'), None, None)
    cache_spec = P(('pair', 'side'), None, None, None, 'tp', None)
    prompt_spec = P(('pair', 'side'), None, None, 'tp', None)

    def local_step(x_loc, req_len, dest, w_qkv, w_out, w_gate, w_up, w_down, y_loc, kc_loc, vc_loc, clen_loc):
        R, D = x_loc.shape
        B, T, slots, HD = kc_loc.shape[2:]
        Q, F = w_out.shape[1], w_gate.shape[2]
        KV = (w_qkv.shape[2] - Q) // 2
        max_req = 2 * R - R // 4
        kernel, scratch, _ = make_kernel(tp_size, side_size, R, D, B, T, Q, KV, HD, F, max_req)
        half = HD // 2
        inv_freq = ROPE_BASE ** (-jnp.arange(half, dtype=F32) / half)
        one = jnp.ones((half,), F32)
        fq = jnp.zeros((8, HD), F32).at[0].set(jnp.concatenate([inv_freq, inv_freq])).at[1].set(jnp.concatenate([-one, one]))
        any_spec = pl.BlockSpec(memory_space=pl.ANY)
        smem = pl.BlockSpec(memory_space=pltpu.SMEM)
        CK = B * T * slots
        hid, dec, kp, vp, kn, vn = pl.pallas_call(
            kernel,
            name='prefill_decode',
            out_shape=[jax.ShapeDtypeStruct(s, BF) for s in
                       ((R, D), (B, D), (max_req * 2, HD), (max_req * 2, HD), (CK, HD), (CK, HD))],
            in_specs=[any_spec] * 9 + [smem] * 3 + [pl.BlockSpec(memory_space=pltpu.VMEM)],
            out_specs=[any_spec] * 6,
            scratch_shapes=scratch,
            compiler_params=pltpu.CompilerParams(collective_id=0, has_side_effects=True, vmem_limit_bytes=67043328),
        )(x_loc, y_loc[0], w_qkv[0], w_out[0], w_gate[0], w_up[0], w_down[0],
          kc_loc.reshape(CK, HD), vc_loc.reshape(CK, HD), req_len, dest, clen_loc[0], fq)
        cache = (1, 1, B, T, slots, HD)
        prompt = (1, 1, max_req, slots, HD)
        return hid, dec[None], kp.reshape(prompt), vp.reshape(prompt), kn.reshape(cache), vn.reshape(cache)

    return jax.shard_map(local_step, mesh=mesh,
                         in_specs=(rows_spec, P('pair'), P('pair'), P(), P(), P(), P(), P(), batch_spec, cache_spec, cache_spec, rows_spec),
                         out_specs=(rows_spec, batch_spec, prompt_spec, prompt_spec, cache_spec, cache_spec),
                         check_vma=False)
```

```python
import jax
import jax.numpy as jnp
import numpy as np
from jax import lax
from jax.experimental import pallas as pl
from jax.experimental.pallas import tpu as pltpu
from jax.sharding import PartitionSpec as P

ROPE_BASE = 10000.0
NORM_EPS = 1e-5
BF = jnp.bfloat16
F32 = jnp.float32
CW = 256
GU_SLOTS = 9
MESH = pl.DeviceIdType.MESH


def mult(v, m):
    return pl.multiple_of(v, m)


def make_kernel(tp_size, side_size, R, D, B, T, Q, KV, HD, F, max_req):
    heads_local = Q // HD // tp_size
    rep = heads_local // 2
    hw = rep * HD
    qw = 2 * hw
    RT = R // tp_size
    DH = D // 2
    FH = F // 2
    M1 = R + B
    M2 = 2 * RT + 2 * B
    n_kv, n_q = 2 * 2 * HD // CW, qw // CW
    n_o, n_g, n_d = DH // CW, FH // CW, DH // CW
    wo_base = -(-(n_kv + n_q) * D // F) * F
    gu_base = wo_base + n_o * Q
    slab_rows = gu_base + GU_SLOTS * 2 * D
    CK = B * T * 2
    PR = max_req * 2
    scale = HD ** -0.5
    n_first = wo_base // F
    AB = D // CW
    nblk = side_size

    def kernel(x_h, y_h, wqkv_h, wo_h, wg_h, wu_h, wd_h, kc_h, vc_h, rl, dst, cl, fq,
               hid_o, dec_o, kp_o, vp_o, kn_o, vn_o,
               slab, ub, ys, raw, qs, kva, knv, kcs, vcs, cos_s, sin_s,
               dcs, cst, ctxr, xres, hf, hn, outst, hid, decb, kps, vps,
               in_sem, w_sem, g_sem, d_sem, xr_s, xr_r, kx_s, kx_r, cx_s, cx_r, cf_s, cf_r,
               dx_s, dx_r, df_s, df_r, h_s, h_r, a_s, a_r, f_s, f_r, r_s, r_r, o_sem):
        xs, xn = ub.at[pl.ds(0, R), :], ub.at[pl.ds(R, M1), :]
        side = lax.axis_index('side')
        tp = lax.axis_index('tp')
        core = lax.rem(side, 2)
        oc = 1 - core
        partner = side + 1 - 2 * core
        left = lax.rem(side + side_size - 2, side_size)
        right = lax.rem(side + 2, side_size)
        far = lax.rem(side + 4, side_size)
        p_left = lax.rem(partner + side_size - 2, side_size)
        p_right = lax.rem(partner + 2, side_size)
        p_far = lax.rem(partner + 4, side_size)

        def at(d):
            return lax.rem(tp + d, tp_size)

        def dev(s, t):
            return {'side': s, 'tp': t}

        q_cols0, k_cols0, v_cols0 = 0, Q, Q + KV
        hcol = [tp * hw, (tp + tp_size) * hw]
        kcol = [k_cols0 + tp * HD, k_cols0 + (tp + tp_size) * HD]
        vcol = [v_cols0 + tp * HD, v_cols0 + (tp + tp_size) * HD]

        def pieces(u):
            if u < 2:
                return [(kcol[u], 0, HD), (vcol[u], HD, HD)]
            lo, hi = (u - 2) * CW, (u - 1) * CW
            out = []
            for j in range(2):
                a, b = max(lo, j * hw), min(hi, (j + 1) * hw)
                if a < b:
                    out.append((hcol[j] + (a - j * hw), a - lo, b - a))
            return out

        def start_qkv(u):
            for src, d0, w in pieces(u):
                pltpu.make_async_copy(wqkv_h.at[:, pl.ds(mult(src, 128), w)],
                                      slab.at[pl.ds(u * D, D), pl.ds(d0, w)], w_sem.at[u]).start()

        def slab_wait(base, rows, sem):
            pltpu.make_async_copy(slab.at[pl.ds(base, rows), :], slab.at[pl.ds(base, rows), :], sem).wait()

        def start_wo(u):
            col = mult(core * DH + u * CW, 128)
            for t in range(tp_size):
                for j in range(2):
                    pltpu.make_async_copy(wo_h.at[pl.ds((t + j * tp_size) * hw, hw), pl.ds(col, CW)],
                                          slab.at[pl.ds(wo_base + u * Q + t * qw + j * hw, hw), :],
                                          w_sem.at[n_kv + n_q + u]).start()

        def start_gu(j, slot):
            col = mult(core * FH + j * CW, 128)
            base = mult(gu_base + slot * (2 * D), 256)
            pltpu.make_async_copy(wg_h.at[:, pl.ds(col, CW)], slab.at[pl.ds(base, D), :], g_sem.at[slot]).start()
            pltpu.make_async_copy(wu_h.at[:, pl.ds(col, CW)], slab.at[pl.ds(mult(base + D, 256), D), :], g_sem.at[slot]).start()

        def d_copy(n):
            return pltpu.make_async_copy(wd_h.at[:, pl.ds(mult(core * DH + n * CW, 128), CW)],
                                         slab.at[pl.ds(mult(n * F, 256), F), :], d_sem.at[n])

        x_in = pltpu.make_async_copy(x_h, xs, in_sem.at[0])
        y_in = pltpu.make_async_copy(y_h, ys, in_sem.at[1])
        x_in.start()
        y_in.start()
        for u in range(n_kv + n_q):
            start_qkv(u)

        peers = [(partner, tp), (left, tp), (right, tp), (side, at(1)), (side, at(tp_size - 1)), (side, at(2)),
                 (partner, at(1)), (partner, at(tp_size - 1))]
        barrier = pltpu.get_barrier_semaphore()
        for s, t in peers:
            pl.semaphore_signal(barrier, inc=1, device_id=dev(s, t), device_id_type=MESH)

        kc_in = pltpu.make_async_copy(kc_h, kcs, in_sem.at[2])
        vc_in = pltpu.make_async_copy(vc_h, vcs, in_sem.at[3])
        kc_in.start()
        vc_in.start()
        row_t = mult(tp * RT, RT)
        my_cols = mult(core * DH, 128)
        xres_l = [pltpu.make_async_copy(x_h.at[pl.ds(row_t, RT), pl.ds(my_cols, DH)],
                                        xres.at[pl.ds(mult(core * RT, RT), RT), :], in_sem.at[4]),
                  pltpu.make_async_copy(y_h.at[:, pl.ds(my_cols, DH)],
                                        xres.at[pl.ds(mult(2 * RT + core * B, B), B), :], in_sem.at[5])]
        for cp in xres_l:
            cp.start()

        def seg_of(rows):
            seg = jnp.zeros_like(rows)
            total = jnp.int32(0)
            for r in range(nblk):
                total = total + rl[r]
                seg = jnp.where(rows >= total, total, seg)
            return seg

        idx = lax.broadcasted_iota(jnp.int32, (M1, 1), 0)
        rows = idx + side * R
        pos = rows - seg_of(rows)
        for b in range(B):
            pos = jnp.where(idx == R + b, cl[b], pos)
        ang = pos.astype(F32) * fq[0:1, :]
        cos_s[...] = jnp.cos(ang)
        sin_s[...] = jnp.sin(ang) * fq[1:2, :]

        def norm(v):
            w = v.astype(F32)
            sc = lax.rsqrt(jnp.sum(w * w, axis=-1, keepdims=True) / D + NORM_EPS)
            return (w * sc).astype(BF)

        x_in.wait()

        def norm_x(i, c):
            r = pl.ds(mult(i * 32, 32), 32)
            xn[r, :] = norm(xs[r, :])
            return c

        lax.fori_loop(0, R // 32, norm_x, 0)
        y_in.wait()
        xn[pl.ds(R, B), :] = norm(ys[...])

        def remote(src, dst_ref, ss, rs, s, t):
            return pltpu.make_async_remote_copy(src_ref=src, dst_ref=dst_ref, send_sem=ss, recv_sem=rs,
                                                device_id=dev(s, t), device_id_type=MESH)

        his_cols = mult(oc * DH, 128)
        xres_r = [remote(x_h.at[pl.ds(row_t, RT), pl.ds(his_cols, DH)], xres.at[pl.ds(mult(core * RT, RT), RT), :],
                         xr_s.at[0], xr_r.at[0], partner, tp),
                  remote(y_h.at[:, pl.ds(his_cols, DH)], xres.at[pl.ds(mult(2 * RT + core * B, B), B), :],
                         xr_s.at[1], xr_r.at[1], partner, tp)]

        def project(u):
            w = slab[pl.ds(mult(u * D, 256), D), :]
            raw[u] = jnp.dot(xn[...], w, preferred_element_type=F32).astype(BF)

        def rope(v):
            w = v.astype(F32)
            return (w * cos_s[...] + pltpu.roll(w, HD // 2, 1) * sin_s[...]).astype(BF)

        def project_loop(i, c):
            slab_wait(mult(i * D, 256), D, w_sem.at[i])
            project(i)
            return c

        for u in range(n_o):
            start_wo(u)

        def blk(b, i0, n):
            return kva.at[pl.ds(i0, n), pl.ds(mult(b * R, R), R), :]

        plan = [(side, 0, 1, right, left), (side, 1, 1, right, left),
                (side, 0, 1, partner, partner), (side, 1, 1, partner, partner),
                (side, 0, 2, left, right),
                (left, 0, 1, partner, p_left), (left, 1, 1, partner, p_left),
                (left, 0, 1, right, far),
                (right, 0, 2, partner, p_right), (right, 1, 1, left, far),
                (far, 0, 1, partner, p_far), (far, 1, 1, partner, p_far)]
        kx = [remote(blk(b, i0, n), blk(b, i0, n), kx_s.at[i], kx_r.at[i], to, tp)
              for i, (b, i0, n, to, _) in enumerate(plan)]

        def got(i):
            ref = blk(plan[i][4], plan[i][1], plan[i][2])
            pltpu.make_async_copy(ref, ref, kx_r.at[i]).wait()

        own_rows = pl.ds(mult(side * R, R), R)
        for j in range(2):
            slab_wait(j * D, D, w_sem.at[j])
            project(j)
            k_j = rope(raw[j, :, pl.ds(0, HD)])
            v_j = raw[j, :, pl.ds(HD, HD)]
            kva[j, own_rows, pl.ds(0, HD)] = k_j[:R]
            kva[j, own_rows, pl.ds(HD, HD)] = v_j[:R]
            if j == 0:
                pl.semaphore_wait(barrier, len(peers))
            kx[j].start()
            kx[2 + j].start()
            knv[pl.ds(j * B, B), pl.ds(0, HD)] = k_j[R:]
            knv[pl.ds(j * B, B), pl.ds(HD, HD)] = v_j[R:]
        kx[4].start()
        for cp in xres_r:
            cp.start()
        knv[:, pl.ds(2 * HD, HD)] = jnp.ones((2 * B, HD), BF)

        lax.fori_loop(n_kv, n_kv + n_q, project_loop, 0)
        for slot in range(GU_SLOTS):
            start_gu(slot, slot)
        for n in range(n_first):
            d_copy(n).start()
        for h in range(heads_local):
            u, off = divmod(h * HD, CW)
            qs[h] = rope(raw[2 + u, :, pl.ds(off, HD)])

        kc_in.wait()
        vc_in.wait()
        lane2 = lax.broadcasted_iota(jnp.int32, (1, 2 * B), 1)
        len2 = jnp.zeros((1, 2 * B), jnp.int32)
        for b in range(B):
            len2 = jnp.where(lax.rem(lane2, B) == b, cl[b], len2)
        code2 = (lax.rem(lane2, B) * T + len2) * 2 + lane2 // B
        CH = 256

        def insert(i, c):
            r0 = mult(i * CH, CH)
            rr = lax.broadcasted_iota(jnp.int32, (CH, 1), 0) + r0
            pick = jnp.where(rr == code2, 1.0, 0.0).astype(BF)
            new = jnp.dot(pick, knv[...], preferred_element_type=F32)
            hit = new[:, 2 * HD:] > 0.5
            sl = pl.ds(r0, CH)
            kcs[sl, :] = jnp.where(hit, new[:, :HD], kcs[sl, :].astype(F32)).astype(BF)
            vcs[sl, :] = jnp.where(hit, new[:, HD:2 * HD], vcs[sl, :].astype(F32)).astype(BF)
            return c

        lax.fori_loop(0, CK // CH, insert, 0)
        kn_out = pltpu.make_async_copy(kcs, kn_o, o_sem.at[0])
        vn_out = pltpu.make_async_copy(vcs, vn_o, o_sem.at[1])
        kn_out.start()
        vn_out.start()

        HB = heads_local * B
        q_dec = qs[:, pl.ds(R, B), :].reshape(HB, HD)
        s_dec = lax.dot_general(q_dec, kcs[...], (((1,), (1,)), ((), ())), preferred_element_type=F32) * scale
        qi = lax.broadcasted_iota(jnp.int32, (HB, 1), 0)
        ki = lax.broadcasted_iota(jnp.int32, (1, CK), 1)
        q_len = jnp.zeros((HB, 1), jnp.int32)
        for b in range(B):
            q_len = jnp.where(lax.rem(qi, B) == b, cl[b], q_len)
        q_code = lax.rem(qi, B) * 2 + qi // (rep * B)
        k_code = (ki // (2 * T)) * 2 + lax.rem(ki, 2)
        k_pos = lax.rem(ki // 2, T)
        s_dec = jnp.where((q_code == k_code) & (k_pos <= q_len), s_dec, -1e30)
        e_dec = jnp.exp(s_dec - jnp.max(s_dec, axis=-1, keepdims=True))
        p_dec = (e_dec / jnp.sum(e_dec, axis=-1, keepdims=True)).astype(BF)
        c_dec = jnp.dot(p_dec, vcs[...], preferred_element_type=F32).astype(BF)
        for h in range(heads_local):
            dcs[:, pl.ds(h * HD, HD)] = c_dec[h * B:(h + 1) * B]
        dec_rows = pl.ds(mult(2 * RT + core * B, B), B)
        hops = (2, 1, 3, 0)
        srcs = (2, 3, 1)
        dx = [remote(dcs, ctxr.at[tp, dec_rows, :], dx_s.at[k], dx_r.at[k], side, at(hops[k])) for k in range(3)]
        for cp in dx:
            cp.start()
        ctxr[tp, dec_rows, :] = dcs[...]
        df_own = remote(dcs, ctxr.at[tp, dec_rows, :], df_s.at[3], df_r.at[3], partner, tp)
        df_own.start()

        got(0)
        kx[5].start()
        kx[7].start()

        got(2)
        got(5)

        blks = [lax.rem(side + side_size - 2, side_size), lax.rem(side + side_size - 1, side_size), side]
        pre_rows = pl.ds(mult(core * RT, RT), RT)
        key_row = (side - 2) * R + lax.broadcasted_iota(jnp.int32, (1, 3 * R), 1)
        QR = rep * RT
        q_off = lax.rem(lax.broadcasted_iota(jnp.int32, (QR, 1), 0), RT)

        def attend(j, k):
            r0 = mult(at(hops[k]) * RT, RT)
            q_row = side * R + r0 + q_off
            q_seg = seg_of(q_row)
            q = qs[pl.ds(j * rep, rep), pl.ds(r0, RT), :].reshape(QR, HD)
            held = lambda i, b: kva[j, pl.ds(mult(b * R, R), R), pl.ds(i * HD, HD)]
            s = jnp.concatenate([lax.dot_general(q, held(0, b), (((1,), (1,)), ((), ())), preferred_element_type=F32)
                                 for b in blks], axis=-1) * scale
            s = jnp.where((key_row >= q_seg) & (key_row <= q_row), s, -1e30)
            e = jnp.exp(s - jnp.max(s, axis=-1, keepdims=True))
            p = (e * (1.0 / jnp.sum(e, axis=-1, keepdims=True))).astype(BF)
            o = jnp.zeros((QR, HD), F32)
            for i, b in enumerate(blks):
                o = o + jnp.dot(p[:, i * R:(i + 1) * R], held(1, b), preferred_element_type=F32)
            o = o.astype(BF)
            for h in range(rep):
                cst[j, k, :, pl.ds(h * HD, HD)] = o[h * RT:(h + 1) * RT]

        def ctx_at(t, rows_, j):
            return ctxr.at[t, rows_, pl.ds(j * hw, hw)]

        cx = [[remote(cst.at[j, k], ctx_at(tp, pre_rows, j), cx_s.at[j, k], cx_r.at[j, k], side, at(hops[k]))
               for k in range(3)] for j in range(2)]
        cf = [[remote(ctx_at(at(srcs[k]), pre_rows, j), ctx_at(at(srcs[k]), pre_rows, j), cf_s.at[j, k], cf_r.at[j, k], partner, tp)
               for k in range(3)] + [remote(cst.at[j, 3], ctx_at(tp, pre_rows, j), cf_s.at[j, 3], cf_r.at[j, 3], partner, tp)]
              for j in range(2)]

        def pass_ctx(j, k):
            ref = ctx_at(at(srcs[k]), pre_rows, j)
            pltpu.make_async_copy(ref, ref, cx_r.at[j, k]).wait()
            cf[j][k].start()

        df = []
        for j in range(2):
            for k in range(4):
                attend(j, k)
                if k < 3:
                    cx[j][k].start()
                else:
                    ctxr[tp, pre_rows, pl.ds(j * hw, hw)] = cst[j, 3]
                    cf[j][3].start()
                if j == 0 and k == 2:
                    got(1)
                    kx[6].start()
                if j == 1 and k > 0:
                    pass_ctx(0, k - 1)
            if j == 0:
                for k in range(3):
                    ref = ctxr.at[at(srcs[k]), dec_rows, :]
                    pltpu.make_async_copy(ref, ref, dx_r.at[k]).wait()
                    df.append(remote(ref, ref, df_s.at[k], df_r.at[k], partner, tp))
                    df[k].start()
                got(3)
                got(6)
                got(4)
                kx[8].start()
                kx[9].start()

        for k in range(3):
            pass_ctx(1, k)
        p_pre = pl.ds(mult(oc * RT, RT), RT)
        p_dec_rows = pl.ds(mult(2 * RT + oc * B, B), B)
        for k in range(4):
            t = at(srcs[k]) if k < 3 else tp
            for j in range(2):
                ref = ctx_at(t, p_pre, j)
                pltpu.make_async_copy(ref, ref, cf_r.at[j, k]).wait()
            ref = ctxr.at[t, p_dec_rows, :]
            pltpu.make_async_copy(ref, ref, df_r.at[k]).wait()
        for cp in xres_l:
            cp.wait()
        for i, cp in enumerate(xres_r):
            cp.wait_send()
        ref = xres.at[p_pre, :]
        pltpu.make_async_copy(ref, ref, xr_r.at[0]).wait()
        ref = xres.at[p_dec_rows, :]
        pltpu.make_async_copy(ref, ref, xr_r.at[1]).wait()

        def h_copy(u):
            ref = hf.at[:, pl.ds(mult(core * DH + u * CW, CW), CW)]
            return remote(ref, ref, h_s.at[u], h_r.at[u], partner, tp)

        def out_proj(u, c):
            base = wo_base + u * Q
            slab_wait(mult(base, 256), Q, w_sem.at[n_kv + n_q + u])
            acc = jnp.zeros((M2, CW), F32)
            for t in range(tp_size):
                acc = acc + jnp.dot(ctxr[t], slab[pl.ds(mult(base + t * qw, 256), qw), :], preferred_element_type=F32)
            res = xres[:, pl.ds(mult(u * CW, CW), CW)].astype(F32)
            hf[:, pl.ds(mult(core * DH + u * CW, CW), CW)] = (res + acc.astype(BF).astype(F32)).astype(BF)
            h_copy(u).start()
            return c

        lax.fori_loop(0, n_o, out_proj, 0)
        for i in (7, 9):
            got(i)
        kx[10].start()
        kx[11].start()
        for u in range(n_o):
            ref = hf.at[:, pl.ds(mult(oc * DH + u * CW, CW), CW)]
            pltpu.make_async_copy(ref, ref, h_r.at[u]).wait()

        def norm_h(i, c):
            r = pl.ds(mult(i * 32, 32), 32)
            hn[r, :] = norm(hf[r, :])
            return c

        lax.fori_loop(0, M2 // 32, norm_h, 0)

        def act_at(c_of, j):
            g = c_of * n_g + j
            return ub.at[pl.ds(mult((g // AB) * M2, 16), M2), pl.ds(mult(lax.rem(g, AB) * CW, CW), CW)]

        def a_copy(j):
            ref = act_at(core, j)
            return remote(ref, ref, a_s.at[j], a_r.at[j], partner, tp)

        def last_slot(n):
            top = (n + 1) * F - gu_base
            if top <= 0:
                return 2 * (n - n_first) + 2
            slot = (top - 1) // (2 * D)
            return slot + ((n_g - 1 - slot) // GU_SLOTS) * GU_SLOTS

        def gate_up(j, c):
            slot = lax.rem(j, GU_SLOTS)
            base = mult(gu_base + slot * (2 * D), 256)
            slab_wait(base, 2 * D, g_sem.at[slot])
            g = jnp.dot(hn[...], slab[pl.ds(base, D), :], preferred_element_type=F32)
            u = jnp.dot(hn[...], slab[pl.ds(mult(base + D, 256), D), :], preferred_element_type=F32)
            g = g.astype(BF).astype(F32)
            u = u.astype(BF).astype(F32)
            act_at(core, j)[...] = (g * jax.nn.sigmoid(g) * u).astype(BF)
            a_copy(j).start()

            @pl.when(j + GU_SLOTS < n_g)
            def _():
                start_gu(j + GU_SLOTS, slot)

            for n in range(n_first, n_d):
                @pl.when(j == last_slot(n))
                def _(n=n):
                    d_copy(n).start()
            return c

        lax.fori_loop(0, n_g, gate_up, 0)

        def a_got(j, c):
            ref = act_at(oc, j)
            pltpu.make_async_copy(ref, ref, a_r.at[j]).wait()
            return c

        lax.fori_loop(0, n_g, a_got, 0)

        up, down = at(1), at(tp_size - 1)
        own_out = pl.ds(mult(core * RT, RT), RT)
        his_out = pl.ds(mult(oc * RT, RT), RT)
        own_dec = pl.ds(mult(2 * RT + core * B, B), B)
        his_dec = pl.ds(mult(2 * RT + oc * B, B), B)
        rows_of = lambda t: pl.ds(mult(t * RT, RT), RT)

        def f_copies(n):
            cols = pl.ds(mult(core * DH + n * CW, CW), CW)
            there = hid.at[rows_of(tp), cols]
            mine, his = outst.at[n, own_out, :], outst.at[n, his_out, :]
            return [remote(mine, there, f_s.at[0, n], f_r.at[0, n], side, up),
                    remote(mine, there, f_s.at[1, n], f_r.at[1, n], side, down),
                    remote(his, there, f_s.at[2, n], f_r.at[2, n], partner, up),
                    remote(his, there, f_s.at[3, n], f_r.at[3, n], partner, down),
                    remote(his, there, f_s.at[4, n], f_r.at[4, n], partner, tp),
                    remote(outst.at[n, his_dec, :], decb.at[:, cols], f_s.at[5, n], f_r.at[5, n], partner, tp)]

        def down_proj(n, c):
            d_copy(n).wait()
            acc = jnp.zeros((M2, CW), F32)
            for i in range(-(-F // D)):
                w = min(D, F - i * D)
                acc = acc + jnp.dot(ub[pl.ds(i * M2, M2), pl.ds(0, w)], slab[pl.ds(mult(n * F + i * D, 256), w), :],
                                    preferred_element_type=F32)
            cols = pl.ds(mult(core * DH + n * CW, CW), CW)
            outst[n] = (hf[:, cols].astype(F32) + acc.astype(BF).astype(F32)).astype(BF)
            for cp in f_copies(n):
                cp.start()
            hid[rows_of(tp), cols] = outst[n, own_out, :]
            decb[:, cols] = outst[n, own_dec, :]
            return c

        lax.fori_loop(0, n_d, down_proj, 0)

        def piece(t, c_from, n):
            return hid.at[rows_of(t), pl.ds(mult(c_from * DH + n * CW, CW), CW)]

        def arrived(ref, sem):
            pltpu.make_async_copy(ref, ref, sem).wait()

        kind = {(0, 1): 0, (1, 1): 1, (0, 0): 2, (1, 0): 3}
        relays = []
        for n in range(n_d):
            for same in (1, 0):
                c_from = core if same else oc
                if n % 2 == 0:
                    ref = piece(down, c_from, n)
                    arrived(ref, f_r.at[kind[(0, same)], n])
                    cp = remote(ref, ref, r_s.at[same, n], r_r.at[same, n], side, up)
                else:
                    ref = piece(up, c_from, n)
                    arrived(ref, f_r.at[kind[(1, same)], n])
                    cp = remote(ref, ref, r_s.at[same, n], r_r.at[same, n], side, down)
                cp.start()
                relays.append(cp)

        for i in (8, 10, 11):
            got(i)
        start, length, total = jnp.int32(0), jnp.int32(0), jnp.int32(0)
        for r in range(nblk):
            mine = dst[r] == side
            start = start + jnp.where(mine, total, 0)
            length = length + jnp.where(mine, rl[r], 0)
            total = total + rl[r]
        IR = 128
        col = lax.broadcasted_iota(jnp.int32, (1, 2 * nblk * R), 1)

        def install(i, c):
            r = pl.ds(mult(i * IR, IR), IR)
            o_row = lax.broadcasted_iota(jnp.int32, (IR, 1), 0) + i * IR
            code = jnp.where(o_row // 2 < length, o_row // 2 + start + lax.rem(o_row, 2) * (nblk * R), -1)
            pick = jnp.where(code == col, 1.0, 0.0).astype(BF)
            out = jnp.dot(pick, kva[...].reshape(2 * nblk * R, 2 * HD), preferred_element_type=F32).astype(BF)
            kps[r, :] = out[:, :HD]
            vps[r, :] = out[:, HD:]
            return c

        lax.fori_loop(0, PR // IR, install, 0)
        outs = [pltpu.make_async_copy(kps, kp_o, o_sem.at[2]), pltpu.make_async_copy(vps, vp_o, o_sem.at[3])]
        for cp in outs:
            cp.start()

        def flush(t, i):
            r = rows_of(t)
            cp = pltpu.make_async_copy(hid.at[r, :], hid_o.at[r, :], o_sem.at[4 + i])
            cp.start()
            outs.append(cp)

        for n in range(n_d):
            arrived(piece(tp, oc, n), f_r.at[4, n])
            arrived(decb.at[:, pl.ds(mult(oc * DH + n * CW, CW), CW)], f_r.at[5, n])
        flush(tp, 0)
        cp = pltpu.make_async_copy(decb, dec_o, o_sem.at[8])
        cp.start()
        outs.append(cp)
        for n in range(n_d):
            for same in (1, 0):
                c_from = core if same else oc
                if n % 2 == 0:
                    arrived(piece(up, c_from, n), f_r.at[kind[(1, same)], n])
                else:
                    arrived(piece(down, c_from, n), f_r.at[kind[(0, same)], n])
        flush(up, 1)
        flush(down, 2)
        for n in range(n_d):
            for same in (1, 0):
                arrived(piece(at(2), core if same else oc, n), r_r.at[same, n])
        flush(at(2), 3)

        for cp in kx + dx + df + [df_own] + cx[0] + cx[1] + cf[0] + cf[1] + relays:
            cp.wait_send()

        def h_done(u, c):
            h_copy(u).wait_send()
            return c

        def a_done(j, c):
            a_copy(j).wait_send()
            return c

        def f_done(n, c):
            for cp in f_copies(n):
                cp.wait_send()
            return c

        lax.fori_loop(0, n_o, h_done, 0)
        lax.fori_loop(0, n_g, a_done, 0)
        lax.fori_loop(0, n_d, f_done, 0)
        kn_out.wait()
        vn_out.wait()
        for cp in outs:
            cp.wait()

    dma = lambda *s: pltpu.SemaphoreType.DMA(s)
    scratch = [
        pltpu.VMEM((slab_rows, CW), BF),
        pltpu.VMEM((max(R + M1, -(-F // D) * M2), D), BF), pltpu.VMEM((B, D), BF),
        pltpu.VMEM((n_kv + n_q, M1, CW), BF), pltpu.VMEM((heads_local, M1, HD), BF),
        pltpu.VMEM((2, nblk * R, 2 * HD), BF), pltpu.VMEM((2 * B, 3 * HD), BF),
        pltpu.VMEM((CK, HD), BF), pltpu.VMEM((CK, HD), BF),
        pltpu.VMEM((M1, HD), F32), pltpu.VMEM((M1, HD), F32),
        pltpu.VMEM((B, qw), BF), pltpu.VMEM((2, 4, RT, hw), BF), pltpu.VMEM((tp_size, M2, qw), BF),
        pltpu.VMEM((M2, DH), BF), pltpu.VMEM((M2, D), BF), pltpu.VMEM((M2, D), BF),
        pltpu.VMEM((n_d, M2, CW), BF), pltpu.VMEM((R, D), BF), pltpu.VMEM((B, D), BF),
        pltpu.VMEM((PR, HD), BF), pltpu.VMEM((PR, HD), BF),
        dma(6), dma(n_kv + n_q + n_o), dma(GU_SLOTS), dma(n_d),
        dma(2), dma(2), dma(12), dma(12), dma(2, 3), dma(2, 3), dma(2, 4), dma(2, 4),
        dma(3), dma(3), dma(4), dma(4), dma(n_o), dma(n_o), dma(n_g), dma(n_g),
        dma(6, n_d), dma(6, n_d), dma(2, n_d), dma(2, n_d), dma(9),
    ]
    return kernel, scratch, (R, D, B, PR, HD, CK)


def write_out(*arrays):
    n = len(arrays)
    cuts = []
    for i, a in enumerate(arrays):
        parts = 4 if i == 0 else 1
        step = a.shape[0] // parts
        cuts += [(i, p * step, step) for p in range(parts)]

    def kernel(*refs):
        ins, outs, bufs, sem_in, sem_out = refs[:n], refs[n:2 * n], refs[2 * n:3 * n], refs[3 * n], refs[3 * n + 1]
        reads = [pltpu.make_async_copy(ins[i].at[pl.ds(r, w), :], bufs[i].at[pl.ds(r, w), :], sem_in.at[k])
                 for k, (i, r, w) in enumerate(cuts)]
        writes = [pltpu.make_async_copy(bufs[i].at[pl.ds(r, w), :], outs[i].at[pl.ds(r, w), :], sem_out.at[k])
                  for k, (i, r, w) in enumerate(cuts)]
        for cp in reads:
            cp.start()
        for rd, wr in zip(reads, writes):
            rd.wait()
            wr.start()
        for wr in writes:
            wr.wait()

    any_spec = pl.BlockSpec(memory_space=pl.ANY)
    return pl.pallas_call(
        kernel,
        name='write_out',
        out_shape=[jax.ShapeDtypeStruct(a.shape, a.dtype) for a in arrays],
        in_specs=[any_spec] * n,
        out_specs=[any_spec] * n,
        scratch_shapes=[pltpu.VMEM(a.shape, a.dtype) for a in arrays]
        + [pltpu.SemaphoreType.DMA((len(cuts),)), pltpu.SemaphoreType.DMA((len(cuts),))],
        compiler_params=pltpu.CompilerParams(vmem_limit_bytes=67043328),
    )(*arrays)


def solution(mesh):
    tp_size = mesh.shape['tp']
    side_size = mesh.shape['side']
    rows_spec = P(('pair', 'side'), None)
    batch_spec = P(('pair', 'side'), None, None)
    cache_spec = P(('pair', 'side'), None, None, None, 'tp', None)
    prompt_spec = P(('pair', 'side'), None, None, 'tp', None)

    def local_step(x_loc, req_len, dest, w_qkv, w_out, w_gate, w_up, w_down, y_loc, kc_loc, vc_loc, clen_loc):
        R, D = x_loc.shape
        B, T, slots, HD = kc_loc.shape[2:]
        Q, F = w_out.shape[1], w_gate.shape[2]
        KV = (w_qkv.shape[2] - Q) // 2
        max_req = 2 * R - R // 4
        kernel, scratch, _ = make_kernel(tp_size, side_size, R, D, B, T, Q, KV, HD, F, max_req)
        half = HD // 2
        inv_freq = np.float32(ROPE_BASE) ** (-np.arange(half, dtype=np.float32) / np.float32(half))
        table = np.zeros((8, HD), np.float32)
        table[0] = np.concatenate([inv_freq, inv_freq])
        table[1] = np.concatenate([-np.ones(half), np.ones(half)])
        fq = jnp.asarray(table)
        any_spec = pl.BlockSpec(memory_space=pl.ANY)
        smem = pl.BlockSpec(memory_space=pltpu.SMEM)
        CK = B * T * slots
        hid, dec, kp, vp, kn, vn = pl.pallas_call(
            kernel,
            name='prefill_decode',
            out_shape=[jax.ShapeDtypeStruct(s, BF) for s in
                       ((R, D), (B, D), (max_req * 2, HD), (max_req * 2, HD), (CK, HD), (CK, HD))],
            in_specs=[any_spec] * 9 + [smem] * 3 + [pl.BlockSpec(memory_space=pltpu.VMEM)],
            out_specs=[any_spec] * 6,
            scratch_shapes=scratch,
            compiler_params=pltpu.CompilerParams(collective_id=0, has_side_effects=True, vmem_limit_bytes=67043328),
        )(x_loc, y_loc[0], w_qkv[0], w_out[0], w_gate[0], w_up[0], w_down[0],
          kc_loc.reshape(CK, HD), vc_loc.reshape(CK, HD), req_len, dest, clen_loc[0], fq)
        hid, dec, kp, vp, kn, vn = write_out(hid, dec, kp, vp, kn, vn)
        cache = (1, 1, B, T, slots, HD)
        prompt = (1, 1, max_req, slots, HD)
        return hid, dec[None], kp.reshape(prompt), vp.reshape(prompt), kn.reshape(cache), vn.reshape(cache)

    return jax.shard_map(local_step, mesh=mesh,
                         in_specs=(rows_spec, P('pair'), P('pair'), P(), P(), P(), P(), P(), batch_spec, cache_spec, cache_spec, rows_spec),
                         out_specs=(rows_spec, batch_spec, prompt_spec, prompt_spec, cache_spec, cache_spec),
                         check_vma=False)
```

```python
import jax
import jax.numpy as jnp
import numpy as np
from jax import lax
from jax.experimental import pallas as pl
from jax.experimental.pallas import tpu as pltpu
from jax.sharding import PartitionSpec as P

ROPE_BASE = 10000.0
NORM_EPS = 1e-5
BF = jnp.bfloat16
F32 = jnp.float32
CW = 256
GU_SLOTS = 9
MESH = pl.DeviceIdType.MESH


def mult(v, m):
    return pl.multiple_of(v, m)


def make_kernel(tp_size, side_size, R, D, B, T, Q, KV, HD, F, max_req):
    heads_local = Q // HD // tp_size
    rep = heads_local // 2
    hw = rep * HD
    qw = 2 * hw
    RT = R // tp_size
    DH = D // 2
    FH = F // 2
    M1 = R + B
    M2 = 2 * RT + 2 * B
    n_kv, n_q = 2 * 2 * HD // CW, qw // CW
    n_o, n_g, n_d = DH // CW, FH // CW, DH // CW
    wo_base = -(-(n_kv + n_q) * D // F) * F
    gu_base = wo_base + n_o * Q
    slab_rows = gu_base + GU_SLOTS * 2 * D
    CK = B * T * 2
    PR = max_req * 2
    scale = HD ** -0.5
    WK = max_req + RT
    n_first = wo_base // F
    AB = D // CW
    nblk = side_size

    def kernel(x_h, y_h, wqkv_h, wo_h, wg_h, wu_h, wd_h, kc_h, vc_h, rl_h, dst_h, cl_h, fq_h,
               hid_o, dec_o, kp_o, vp_o, kn_o, vn_o,
               rl, dst, cl, fq, slab, ub, ys, raw, qs, kva, knv, kcs, vcs, cos_s, sin_s, bias_s,
               dcs, cst, ctxr, xres, hf, hn, outst, hid, decb, kps, vps,
               in_sem, w_sem, g_sem, d_sem, xr_s, xr_r, kx_s, kx_r, cx_s, cx_r, cf_s, cf_r,
               dx_s, dx_r, df_s, df_r, h_s, h_r, a_s, a_r, f_s, f_r, r_s, r_r, o_sem):
        xs, xn = ub.at[pl.ds(0, R), :], ub.at[pl.ds(R, M1), :]
        side = lax.axis_index('side')
        tp = lax.axis_index('tp')
        core = lax.rem(side, 2)
        oc = 1 - core
        partner = side + 1 - 2 * core
        left = lax.rem(side + side_size - 2, side_size)
        right = lax.rem(side + 2, side_size)
        far = lax.rem(side + 4, side_size)
        p_left = lax.rem(partner + side_size - 2, side_size)
        p_right = lax.rem(partner + 2, side_size)
        p_far = lax.rem(partner + 4, side_size)

        def at(d):
            return lax.rem(tp + d, tp_size)

        def dev(s, t):
            return {'side': s, 'tp': t}

        q_cols0, k_cols0, v_cols0 = 0, Q, Q + KV
        hcol = [tp * hw, (tp + tp_size) * hw]
        kcol = [k_cols0 + tp * HD, k_cols0 + (tp + tp_size) * HD]
        vcol = [v_cols0 + tp * HD, v_cols0 + (tp + tp_size) * HD]

        def pieces(u):
            if u < 2:
                return [(kcol[u], 0, HD), (vcol[u], HD, HD)]
            lo, hi = (u - 2) * CW, (u - 1) * CW
            out = []
            for j in range(2):
                a, b = max(lo, j * hw), min(hi, (j + 1) * hw)
                if a < b:
                    out.append((hcol[j] + (a - j * hw), a - lo, b - a))
            return out

        def start_qkv(u):
            for src, d0, w in pieces(u):
                pltpu.make_async_copy(wqkv_h.at[:, pl.ds(mult(src, 128), w)],
                                      slab.at[pl.ds(u * D, D), pl.ds(d0, w)], w_sem.at[u]).start()

        def slab_wait(base, rows, sem):
            pltpu.make_async_copy(slab.at[pl.ds(base, rows), :], slab.at[pl.ds(base, rows), :], sem).wait()

        def start_wo(u):
            col = mult(core * DH + u * CW, 128)
            pltpu.make_async_copy(wo_h.at[:, pl.ds(col, CW)], slab.at[pl.ds(wo_base + u * Q, Q), :],
                                  w_sem.at[n_kv + n_q + u]).start()

        def start_gu(j, slot):
            col = mult(core * FH + j * CW, 128)
            base = mult(gu_base + slot * (2 * D), 256)
            pltpu.make_async_copy(wg_h.at[:, pl.ds(col, CW)], slab.at[pl.ds(base, D), :], g_sem.at[slot]).start()
            pltpu.make_async_copy(wu_h.at[:, pl.ds(col, CW)], slab.at[pl.ds(mult(base + D, 256), D), :], g_sem.at[slot]).start()

        def d_copy(n):
            return pltpu.make_async_copy(wd_h.at[:, pl.ds(mult(core * DH + n * CW, 128), CW)],
                                         slab.at[pl.ds(mult(n * F, 256), F), :], d_sem.at[n])

        small = [pltpu.make_async_copy(a, b, in_sem.at[6 + i])
                 for i, (a, b) in enumerate(((rl_h, rl), (dst_h, dst), (cl_h, cl), (fq_h, fq)))]
        XC = 4
        x_in = [pltpu.make_async_copy(x_h.at[pl.ds(i * (R // XC), R // XC), :], xs.at[pl.ds(i * (R // XC), R // XC), :],
                                      in_sem.at[10 + i]) for i in range(XC)]
        y_in = pltpu.make_async_copy(y_h, ys, in_sem.at[1])
        for cp in small + x_in + [y_in]:
            cp.start()
        for u in range(n_kv + n_q):
            start_qkv(u)

        peers = [(partner, tp), (left, tp), (right, tp), (side, at(1)), (side, at(tp_size - 1)), (side, at(2)),
                 (partner, at(1)), (partner, at(tp_size - 1))]
        barrier = pltpu.get_barrier_semaphore()
        for s, t in peers:
            pl.semaphore_signal(barrier, inc=1, device_id=dev(s, t), device_id_type=MESH)

        kc_in = pltpu.make_async_copy(kc_h, kcs, in_sem.at[2])
        vc_in = pltpu.make_async_copy(vc_h, vcs, in_sem.at[3])
        kc_in.start()
        vc_in.start()
        row_t = mult(tp * RT, RT)
        my_cols = mult(core * DH, 128)
        xres_l = [pltpu.make_async_copy(x_h.at[pl.ds(row_t, RT), pl.ds(my_cols, DH)],
                                        xres.at[pl.ds(mult(core * RT, RT), RT), :], in_sem.at[4]),
                  pltpu.make_async_copy(y_h.at[:, pl.ds(my_cols, DH)],
                                        xres.at[pl.ds(mult(2 * RT + core * B, B), B), :], in_sem.at[5])]
        for cp in xres_l:
            cp.start()

        def seg_of(rows):
            seg = jnp.zeros_like(rows)
            total = jnp.int32(0)
            for r in range(nblk):
                total = total + rl[r]
                seg = jnp.where(rows >= total, total, seg)
            return seg

        for cp in small:
            cp.wait()
        idx = lax.broadcasted_iota(jnp.int32, (M1, 1), 0)
        rows = idx + side * R
        pos = rows - seg_of(rows)
        for b in range(B):
            pos = jnp.where(idx == R + b, cl[b], pos)
        ang = pos.astype(F32) * fq[0:1, :]
        cos_s[...] = jnp.cos(ang)
        sin_s[...] = jnp.sin(ang) * fq[1:2, :]

        def norm(v):
            w = v.astype(F32)
            sc = lax.rsqrt(jnp.sum(w * w, axis=-1, keepdims=True) / D + NORM_EPS)
            return (w * sc).astype(BF)

        for i in range(XC):
            x_in[i].wait()

            def norm_x(k, c, i=i):
                r = pl.ds(mult(i * (R // XC) + k * 32, 32), 32)
                xn[r, :] = norm(xs[r, :])
                return c

            lax.fori_loop(0, R // XC // 32, norm_x, 0, unroll=True)
        y_in.wait()
        xn[pl.ds(R, B), :] = norm(ys[...])

        def remote(src, dst_ref, ss, rs, s, t):
            return pltpu.make_async_remote_copy(src_ref=src, dst_ref=dst_ref, send_sem=ss, recv_sem=rs,
                                                device_id=dev(s, t), device_id_type=MESH)

        his_cols = mult(oc * DH, 128)
        xres_r = [remote(x_h.at[pl.ds(row_t, RT), pl.ds(his_cols, DH)], xres.at[pl.ds(mult(core * RT, RT), RT), :],
                         xr_s.at[0], xr_r.at[0], partner, tp),
                  remote(y_h.at[:, pl.ds(his_cols, DH)], xres.at[pl.ds(mult(2 * RT + core * B, B), B), :],
                         xr_s.at[1], xr_r.at[1], partner, tp)]

        def project(u):
            w = slab[pl.ds(mult(u * D, 256), D), :]
            raw[u] = jnp.dot(xn[...], w, preferred_element_type=F32).astype(BF)

        def rope(v):
            w = v.astype(F32)
            return (w * cos_s[...] + pltpu.roll(w, HD // 2, 1) * sin_s[...]).astype(BF)

        for u in range(n_o):
            start_wo(u)

        def blk(b, i0, n):
            return kva.at[pl.ds(i0, n), pl.ds(mult(b * R, R), R), :]

        plan = [(side, 0, 1, right, left), (side, 1, 1, right, left),
                (side, 0, 1, partner, partner), (side, 1, 1, partner, partner),
                (side, 0, 2, left, right),
                (left, 0, 1, partner, p_left), (left, 1, 1, partner, p_left),
                (left, 0, 1, right, far),
                (right, 0, 2, partner, p_right), (right, 1, 1, left, far),
                (far, 0, 1, partner, p_far), (far, 1, 1, partner, p_far)]
        kx = [remote(blk(b, i0, n), blk(b, i0, n), kx_s.at[i], kx_r.at[i], to, tp)
              for i, (b, i0, n, to, _) in enumerate(plan)]

        def got(i):
            ref = blk(plan[i][4], plan[i][1], plan[i][2])
            pltpu.make_async_copy(ref, ref, kx_r.at[i]).wait()

        own_rows = pl.ds(mult(side * R, R), R)
        pl.semaphore_wait(barrier, len(peers))

        def keys_values(j, c):
            slab_wait(mult(j * D, 256), D, w_sem.at[j])
            project(j)
            k_j = rope(raw[j, :, pl.ds(0, HD)])
            v_j = raw[j, :, pl.ds(HD, HD)]
            kva[j, own_rows, pl.ds(0, HD)] = k_j[:R]
            kva[j, own_rows, pl.ds(HD, HD)] = v_j[:R]
            ref = blk(side, j, 1)
            remote(ref, ref, kx_s.at[j], kx_r.at[j], right, tp).start()
            remote(ref, ref, kx_s.at[2 + j], kx_r.at[2 + j], partner, tp).start()
            knv[pl.ds(mult(j * B, B), B), pl.ds(0, HD)] = k_j[R:]
            knv[pl.ds(mult(j * B, B), B), pl.ds(HD, HD)] = v_j[R:]
            return c

        lax.fori_loop(0, 2, keys_values, 0)
        kx[4].start()
        for cp in xres_r:
            cp.start()
        knv[:, pl.ds(2 * HD, HD)] = jnp.ones((2 * B, HD), BF)

        for u in range(n_kv, n_kv + n_q):
            slab_wait(u * D, D, w_sem.at[u])

        def queries(i, c):
            for u in range(n_q):
                raw[n_kv + u] = jnp.dot(xn[...], slab[pl.ds(mult((n_kv + u + i) * D, 256), D), :], preferred_element_type=F32).astype(BF)
            return c

        lax.fori_loop(0, tp // tp_size + 1, queries, 0)
        for slot in range(GU_SLOTS):
            start_gu(slot, slot)
        for n in range(n_first):
            d_copy(n).start()
        for h in range(heads_local):
            u, off = divmod(h * HD, CW)
            qs[h] = rope(raw[2 + u, :, pl.ds(off, HD)])

        kc_in.wait()
        vc_in.wait()
        lane2 = lax.broadcasted_iota(jnp.int32, (1, 2 * B), 1)
        len2 = jnp.zeros((1, 2 * B), jnp.int32)
        for b in range(B):
            len2 = jnp.where(lax.rem(lane2, B) == b, cl[b], len2)
        code2 = (lax.rem(lane2, B) * T + len2) * 2 + lane2 // B
        CH = 256

        def insert(i, c):
            r0 = mult(i * CH, CH)
            rr = lax.broadcasted_iota(jnp.int32, (CH, 1), 0) + r0
            pick = jnp.where(rr == code2, 1.0, 0.0).astype(BF)
            new = jnp.dot(pick, knv[...], preferred_element_type=F32)
            hit = new[:, 2 * HD:] > 0.5
            sl = pl.ds(r0, CH)
            kcs[sl, :] = jnp.where(hit, new[:, :HD], kcs[sl, :].astype(F32)).astype(BF)
            vcs[sl, :] = jnp.where(hit, new[:, HD:2 * HD], vcs[sl, :].astype(F32)).astype(BF)
            return c

        lax.fori_loop(0, CK // CH, insert, 0)
        inner = side >= 2

        @pl.when(inner)
        def _():
            got(0)
            kx[5].start()
            kx[7].start()

        kn_out = pltpu.make_async_copy(kcs, kn_o, o_sem.at[0])
        vn_out = pltpu.make_async_copy(vcs, vn_o, o_sem.at[1])
        kn_out.start()
        vn_out.start()

        HB = heads_local * B
        q_dec = qs[:, pl.ds(R, B), :].reshape(HB, HD)
        s_dec = lax.dot_general(q_dec, kcs[...], (((1,), (1,)), ((), ())), preferred_element_type=F32) * scale
        qi = lax.broadcasted_iota(jnp.int32, (HB, 1), 0)
        ki = lax.broadcasted_iota(jnp.int32, (1, CK), 1)
        q_len = jnp.zeros((HB, 1), jnp.int32)
        for b in range(B):
            q_len = jnp.where(lax.rem(qi, B) == b, cl[b], q_len)
        q_code = lax.rem(qi, B) * 2 + qi // (rep * B)
        k_code = (ki // (2 * T)) * 2 + lax.rem(ki, 2)
        k_pos = lax.rem(ki // 2, T)
        s_dec = jnp.where((q_code == k_code) & (k_pos <= q_len), s_dec, -1e30)
        e_dec = jnp.exp(s_dec - jnp.max(s_dec, axis=-1, keepdims=True))
        p_dec = (e_dec / jnp.sum(e_dec, axis=-1, keepdims=True)).astype(BF)
        c_dec = jnp.dot(p_dec, vcs[...], preferred_element_type=F32).astype(BF)
        for h in range(heads_local):
            dcs[h // rep, :, pl.ds((h % rep) * HD, HD)] = c_dec[h * B:(h + 1) * B]
        dec_rows = pl.ds(mult(2 * RT + core * B, B), B)
        hops = (2, 1, 3, 0)
        srcs = (2, 3, 1)
        dec_at = lambda t, rows_: ctxr.at[:, rows_, pl.ds(mult(t * hw, 128), hw)]
        dx = [remote(dcs, dec_at(tp, dec_rows), dx_s.at[k], dx_r.at[k], side, at(hops[k])) for k in range(3)]
        for cp in dx:
            cp.start()
        dec_at(tp, dec_rows)[...] = dcs[...]
        df_own = remote(dcs, dec_at(tp, dec_rows), df_s.at[3], df_r.at[3], partner, tp)
        df_own.start()

        win = []
        for k in range(4):
            r0 = mult(at(hops[k]) * RT, RT)
            lead = side * R + r0 - max_req
            lead = lead * ((lead + 2 * nblk * R) // (2 * nblk * R))
            win.append((r0, mult(lead, RT)))
            q_row = side * R + r0 + lax.broadcasted_iota(jnp.int32, (RT, 1), 0)
            key_row = lead + lax.broadcasted_iota(jnp.int32, (1, WK), 1)
            bias_s[k] = jnp.where((key_row >= seg_of(q_row)) & (key_row <= q_row), 0.0, -1e30)
        got(2)

        @pl.when(inner)
        def _():
            got(5)

        pre_rows = pl.ds(mult(core * RT, RT), RT)
        QR = rep * RT

        def attend(j, k):
            r0, lead = win[k]
            q = qs[pl.ds(j * rep, rep), pl.ds(r0, RT), :].reshape(QR, HD)
            held = lambda i: kva[j, pl.ds(lead, WK), pl.ds(i * HD, HD)]
            s = lax.dot_general(q, held(0), (((1,), (1,)), ((), ())), preferred_element_type=F32)
            s = s.reshape(rep, RT, WK) * scale + bias_s[k][None]
            e = jnp.exp(s - jnp.max(s, axis=-1, keepdims=True))
            p = (e * (1.0 / jnp.sum(e, axis=-1, keepdims=True))).astype(BF).reshape(QR, WK)
            o = jnp.dot(p, held(1), preferred_element_type=F32)
            o = o.astype(BF)
            for h in range(rep):
                cst[j, k, :, pl.ds(h * HD, HD)] = o[h * RT:(h + 1) * RT]

        def ctx_at(t, rows_, j):
            return ctxr.at[j, rows_, pl.ds(mult(t * hw, 128), hw)]

        cx = [[remote(cst.at[j, k], ctx_at(tp, pre_rows, j), cx_s.at[j, k], cx_r.at[j, k], side, at(hops[k]))
               for k in range(3)] for j in range(2)]
        cf = [[remote(ctx_at(at(srcs[k]), pre_rows, j), ctx_at(at(srcs[k]), pre_rows, j), cf_s.at[j, k], cf_r.at[j, k], partner, tp)
               for k in range(3)] + [remote(cst.at[j, 3], ctx_at(tp, pre_rows, j), cf_s.at[j, 3], cf_r.at[j, 3], partner, tp)]
              for j in range(2)]

        def pass_ctx(j, k):
            ref = ctx_at(at(srcs[k]), pre_rows, j)
            pltpu.make_async_copy(ref, ref, cx_r.at[j, k]).wait()
            cf[j][k].start()

        df = []
        for j in range(2):
            for k in range(4):
                attend(j, k)
                if k < 3:
                    cx[j][k].start()
                else:
                    ctx_at(tp, pre_rows, j)[...] = cst[j, 3]
                    cf[j][3].start()
                if j == 0 and k == 2:
                    @pl.when(inner)
                    def _():
                        got(1)
                        kx[6].start()
            if j == 0:
                got(3)

                @pl.when(inner)
                def _():
                    got(6)

        for k in range(3):
            pass_ctx(0, k)
        for k in range(3):
            ref = dec_at(at(srcs[k]), dec_rows)
            pltpu.make_async_copy(ref, ref, dx_r.at[k]).wait()
            df.append(remote(ref, ref, df_s.at[k], df_r.at[k], partner, tp))
            df[k].start()
        for k in range(3):
            pass_ctx(1, k)
        p_pre = pl.ds(mult(oc * RT, RT), RT)
        p_dec_rows = pl.ds(mult(2 * RT + oc * B, B), B)
        for k in range(4):
            t = at(srcs[k]) if k < 3 else tp
            for j in range(2):
                ref = ctx_at(t, p_pre, j)
                pltpu.make_async_copy(ref, ref, cf_r.at[j, k]).wait()
            ref = dec_at(t, p_dec_rows)
            pltpu.make_async_copy(ref, ref, df_r.at[k]).wait()
        for cp in xres_l:
            cp.wait()
        for i, cp in enumerate(xres_r):
            cp.wait_send()
        ref = xres.at[p_pre, :]
        pltpu.make_async_copy(ref, ref, xr_r.at[0]).wait()
        ref = xres.at[p_dec_rows, :]
        pltpu.make_async_copy(ref, ref, xr_r.at[1]).wait()

        def h_copy(u):
            ref = hf.at[:, pl.ds(mult(core * DH + u * CW, CW), CW)]
            return remote(ref, ref, h_s.at[u], h_r.at[u], partner, tp)

        OU = 2

        def out_proj(i, c):
            for k in range(OU):
                u = i * OU + k
                slab_wait(mult(wo_base + u * Q, 256), Q, w_sem.at[n_kv + n_q + u])
            for k in range(OU):
                u = i * OU + k
                acc = jnp.zeros((M2, CW), F32)
                for j in range(2):
                    acc = acc + jnp.dot(ctxr[j], slab[pl.ds(mult(wo_base + u * Q + j * (Q // 2), 256), Q // 2), :],
                                        preferred_element_type=F32)
                res = xres[:, pl.ds(mult(u * CW, CW), CW)].astype(F32)
                hf[:, pl.ds(mult(core * DH + u * CW, CW), CW)] = (res + acc.astype(BF).astype(F32)).astype(BF)
            for k in range(OU):
                h_copy(i * OU + k).start()
            return c

        lax.fori_loop(0, n_o // OU, out_proj, 0)
        @pl.when(side < 2)
        def _():
            for i in (0, 1):
                got(i)
            for i in (5, 6, 7):
                kx[i].start()
            for i in (5, 6):
                got(i)

        got(4)
        kx[8].start()
        kx[9].start()
        for u in range(n_o):
            ref = hf.at[:, pl.ds(mult(oc * DH + u * CW, CW), CW)]
            pltpu.make_async_copy(ref, ref, h_r.at[u]).wait()

        def norm_h(i, c):
            r = pl.ds(mult(i * 32, 32), 32)
            hn[r, :] = norm(hf[r, :])
            return c

        lax.fori_loop(0, M2 // 32, norm_h, 0, unroll=True)

        def act_at(c_of, j):
            g = c_of * n_g + j
            return ub.at[pl.ds(mult((g // AB) * M2, 16), M2), pl.ds(mult(lax.rem(g, AB) * CW, CW), CW)]

        def a_copy(j):
            ref = act_at(core, j)
            return remote(ref, ref, a_s.at[j], a_r.at[j], partner, tp)

        def last_slot(n):
            top = (n + 1) * F - gu_base
            if top <= 0:
                return 2 * (n - n_first) + 2
            slot = (top - 1) // (2 * D)
            return slot + ((n_g - 1 - slot) // GU_SLOTS) * GU_SLOTS

        def gu_base_of(j):
            return mult(gu_base + lax.rem(j, GU_SLOTS) * (2 * D), 256)

        def gu_next(j):
            @pl.when(j + GU_SLOTS < n_g)
            def _():
                start_gu(j + GU_SLOTS, lax.rem(j, GU_SLOTS))

            for n in range(n_first, n_d):
                @pl.when(j == last_slot(n))
                def _(n=n):
                    d_copy(n).start()

        GU = 2

        def gate_up(i, c):
            for k in range(GU):
                j = i * GU + k
                slab_wait(gu_base_of(j), 2 * D, g_sem.at[lax.rem(j, GU_SLOTS)])
            for k in range(GU):
                j = i * GU + k
                base = gu_base_of(j)
                g = jnp.dot(hn[...], slab[pl.ds(base, D), :], preferred_element_type=F32)
                u = jnp.dot(hn[...], slab[pl.ds(mult(base + D, 256), D), :], preferred_element_type=F32)
                g = g.astype(BF).astype(F32)
                u = u.astype(BF).astype(F32)
                act_at(core, j)[...] = (g * jax.nn.sigmoid(g) * u).astype(BF)
            for k in range(GU):
                a_copy(i * GU + k).start()
            for k in range(GU):
                gu_next(i * GU + k)
            return c

        lax.fori_loop(0, n_g // GU, gate_up, 0)

        def a_got(j, c):
            ref = act_at(oc, j)
            pltpu.make_async_copy(ref, ref, a_r.at[j]).wait()
            return c

        lax.fori_loop(0, n_g, a_got, 0)

        for i in (7, 9):
            got(i)
        kx[10].start()
        kx[11].start()

        up, down = at(1), at(tp_size - 1)
        own_out = pl.ds(mult(core * RT, RT), RT)
        his_out = pl.ds(mult(oc * RT, RT), RT)
        own_dec = pl.ds(mult(2 * RT + core * B, B), B)
        his_dec = pl.ds(mult(2 * RT + oc * B, B), B)
        rows_of = lambda t: pl.ds(mult(t * RT, RT), RT)

        def f_copies(n):
            cols = pl.ds(mult(core * DH + n * CW, CW), CW)
            there = hid.at[rows_of(tp), cols]
            mine, his = outst.at[n, own_out, :], outst.at[n, his_out, :]
            return [remote(mine, there, f_s.at[0, n], f_r.at[0, n], side, up),
                    remote(mine, there, f_s.at[1, n], f_r.at[1, n], side, down),
                    remote(his, there, f_s.at[2, n], f_r.at[2, n], partner, up),
                    remote(his, there, f_s.at[3, n], f_r.at[3, n], partner, down),
                    remote(his, there, f_s.at[4, n], f_r.at[4, n], partner, tp),
                    remote(outst.at[n, his_dec, :], decb.at[:, cols], f_s.at[5, n], f_r.at[5, n], partner, tp)]

        def down_proj(n, c):
            d_copy(n).wait()
            acc = jnp.zeros((M2, CW), F32)
            for i in range(-(-F // D)):
                w = min(D, F - i * D)
                acc = acc + jnp.dot(ub[pl.ds(i * M2, M2), pl.ds(0, w)], slab[pl.ds(mult(n * F + i * D, 256), w), :],
                                    preferred_element_type=F32)
            cols = pl.ds(mult(core * DH + n * CW, CW), CW)
            outst[n] = (hf[:, cols].astype(F32) + acc.astype(BF).astype(F32)).astype(BF)
            for cp in f_copies(n):
                cp.start()
            hid[rows_of(tp), cols] = outst[n, own_out, :]
            decb[:, cols] = outst[n, own_dec, :]
            return c

        lax.fori_loop(0, n_d, down_proj, 0)

        def piece(t, c_from, n, of=hid):
            return of.at[rows_of(t), pl.ds(mult(c_from * DH + n * CW, CW), CW)]

        def arrived(ref, sem):
            pltpu.make_async_copy(ref, ref, sem).wait()

        kind = {(0, 1): 0, (1, 1): 1, (0, 0): 2, (1, 0): 3}
        relays = []
        for n in range(n_d):
            for same in (1, 0):
                c_from = core if same else oc
                if n % 2 == 0:
                    ref = piece(down, c_from, n)
                    arrived(ref, f_r.at[kind[(0, same)], n])
                    cp = remote(ref, piece(down, c_from, n, hid_o), r_s.at[same, n], r_r.at[same, n], side, up)
                else:
                    ref = piece(up, c_from, n)
                    arrived(ref, f_r.at[kind[(1, same)], n])
                    cp = remote(ref, piece(up, c_from, n, hid_o), r_s.at[same, n], r_r.at[same, n], side, down)
                cp.start()
                relays.append(cp)

        for i in (8, 10, 11):
            got(i)
        start, length, total = jnp.int32(0), jnp.int32(0), jnp.int32(0)
        for r in range(nblk):
            mine = dst[r] == side
            start = start + jnp.where(mine, total, 0)
            length = length + jnp.where(mine, rl[r], 0)
            total = total + rl[r]
        IR = 128
        col = lax.broadcasted_iota(jnp.int32, (1, 2 * nblk * R), 1)

        def install(i, c):
            r = pl.ds(mult(i * IR, IR), IR)
            o_row = lax.broadcasted_iota(jnp.int32, (IR, 1), 0) + i * IR
            code = jnp.where(o_row // 2 < length, o_row // 2 + start + lax.rem(o_row, 2) * (nblk * R), -1)
            pick = jnp.where(code == col, 1.0, 0.0).astype(BF)
            out = jnp.dot(pick, kva[...].reshape(2 * nblk * R, 2 * HD), preferred_element_type=F32).astype(BF)
            kps[r, :] = out[:, :HD]
            vps[r, :] = out[:, HD:]
            return c

        lax.fori_loop(0, PR // IR, install, 0)
        outs = [pltpu.make_async_copy(kps, kp_o, o_sem.at[2]), pltpu.make_async_copy(vps, vp_o, o_sem.at[3])]
        for cp in outs:
            cp.start()

        def flush(t, i):
            r = rows_of(t)
            cp = pltpu.make_async_copy(hid.at[r, :], hid_o.at[r, :], o_sem.at[4 + i])
            cp.start()
            outs.append(cp)

        for n in range(n_d):
            arrived(piece(tp, oc, n), f_r.at[4, n])
            arrived(decb.at[:, pl.ds(mult(oc * DH + n * CW, CW), CW)], f_r.at[5, n])
        flush(tp, 0)
        cp = pltpu.make_async_copy(decb, dec_o, o_sem.at[8])
        cp.start()
        outs.append(cp)
        for n in range(n_d):
            for same in (1, 0):
                c_from = core if same else oc
                if n % 2 == 0:
                    arrived(piece(up, c_from, n), f_r.at[kind[(1, same)], n])
                else:
                    arrived(piece(down, c_from, n), f_r.at[kind[(0, same)], n])
        flush(up, 1)
        flush(down, 2)
        for n in range(n_d):
            for same in (1, 0):
                arrived(piece(at(2), core if same else oc, n, hid_o), r_r.at[same, n])

        for cp in kx + dx + df + [df_own] + cx[0] + cx[1] + cf[0] + cf[1] + relays:
            cp.wait_send()

        def h_done(u, c):
            h_copy(u).wait_send()
            return c

        def a_done(j, c):
            a_copy(j).wait_send()
            return c

        def f_done(n, c):
            for cp in f_copies(n):
                cp.wait_send()
            return c

        lax.fori_loop(0, n_o, h_done, 0)
        lax.fori_loop(0, n_g, a_done, 0)
        lax.fori_loop(0, n_d, f_done, 0)
        kn_out.wait()
        vn_out.wait()
        for cp in outs:
            cp.wait()

    dma = lambda *s: pltpu.SemaphoreType.DMA(s)
    scratch = [
        pltpu.SMEM((side_size,), jnp.int32), pltpu.SMEM((side_size,), jnp.int32), pltpu.SMEM((B,), jnp.int32), pltpu.VMEM((8, HD), F32),
        pltpu.VMEM((slab_rows, CW), BF),
        pltpu.VMEM((max(R + M1, -(-F // D) * M2), D), BF), pltpu.VMEM((B, D), BF),
        pltpu.VMEM((n_kv + n_q, M1, CW), BF), pltpu.VMEM((heads_local, M1, HD), BF),
        pltpu.VMEM((2, nblk * R, 2 * HD), BF), pltpu.VMEM((2 * B, 3 * HD), BF),
        pltpu.VMEM((CK, HD), BF), pltpu.VMEM((CK, HD), BF),
        pltpu.VMEM((M1, HD), F32), pltpu.VMEM((M1, HD), F32), pltpu.VMEM((4, RT, max_req + RT), F32),
        pltpu.VMEM((2, B, hw), BF), pltpu.VMEM((2, 4, RT, hw), BF), pltpu.VMEM((2, M2, Q // 2), BF),
        pltpu.VMEM((M2, DH), BF), pltpu.VMEM((M2, D), BF), pltpu.VMEM((M2, D), BF),
        pltpu.VMEM((n_d, M2, CW), BF), pltpu.VMEM((R, D), BF), pltpu.VMEM((B, D), BF),
        pltpu.VMEM((PR, HD), BF), pltpu.VMEM((PR, HD), BF),
        dma(14), dma(n_kv + n_q + n_o), dma(GU_SLOTS), dma(n_d),
        dma(2), dma(2), dma(12), dma(12), dma(2, 3), dma(2, 3), dma(2, 4), dma(2, 4),
        dma(3), dma(3), dma(4), dma(4), dma(n_o), dma(n_o), dma(n_g), dma(n_g),
        dma(6, n_d), dma(6, n_d), dma(2, n_d), dma(2, n_d), dma(9),
    ]
    return kernel, scratch, (R, D, B, PR, HD, CK)


def write_out(*arrays):
    n = len(arrays)
    cuts = []
    for i, a in enumerate(arrays):
        parts = 4 if i == 0 else 1
        step = a.shape[0] // parts
        cuts += [(i, p * step, step) for p in range(parts)]

    def kernel(*refs):
        ins, outs, bufs, sem_in, sem_out = refs[:n], refs[n:2 * n], refs[2 * n:3 * n], refs[3 * n], refs[3 * n + 1]
        reads = [pltpu.make_async_copy(ins[i].at[pl.ds(r, w), :], bufs[i].at[pl.ds(r, w), :], sem_in.at[k])
                 for k, (i, r, w) in enumerate(cuts)]
        writes = [pltpu.make_async_copy(bufs[i].at[pl.ds(r, w), :], outs[i].at[pl.ds(r, w), :], sem_out.at[k])
                  for k, (i, r, w) in enumerate(cuts)]
        for cp in reads:
            cp.start()
        for rd, wr in zip(reads, writes):
            rd.wait()
            wr.start()
        for wr in writes:
            wr.wait()

    any_spec = pl.BlockSpec(memory_space=pl.ANY)
    return pl.pallas_call(
        kernel,
        name='write_out',
        out_shape=[jax.ShapeDtypeStruct(a.shape, a.dtype) for a in arrays],
        in_specs=[any_spec] * n,
        out_specs=[any_spec] * n,
        scratch_shapes=[pltpu.VMEM(a.shape, a.dtype) for a in arrays]
        + [pltpu.SemaphoreType.DMA((len(cuts),)), pltpu.SemaphoreType.DMA((len(cuts),))],
        compiler_params=pltpu.CompilerParams(vmem_limit_bytes=67043328),
    )(*arrays)


def solution(mesh):
    tp_size = mesh.shape['tp']
    side_size = mesh.shape['side']
    rows_spec = P(('pair', 'side'), None)
    batch_spec = P(('pair', 'side'), None, None)
    cache_spec = P(('pair', 'side'), None, None, None, 'tp', None)
    prompt_spec = P(('pair', 'side'), None, None, 'tp', None)

    def local_step(x_loc, req_len, dest, w_qkv, w_out, w_gate, w_up, w_down, y_loc, kc_loc, vc_loc, clen_loc):
        R, D = x_loc.shape
        B, T, slots, HD = kc_loc.shape[2:]
        Q, F = w_out.shape[1], w_gate.shape[2]
        KV = (w_qkv.shape[2] - Q) // 2
        max_req = 2 * R - R // 4
        kernel, scratch, _ = make_kernel(tp_size, side_size, R, D, B, T, Q, KV, HD, F, max_req)
        half = HD // 2
        inv_freq = np.float32(ROPE_BASE) ** (-np.arange(half, dtype=np.float32) / np.float32(half))
        table = np.zeros((8, HD), np.float32)
        table[0] = np.concatenate([inv_freq, inv_freq])
        table[1] = np.concatenate([-np.ones(half), np.ones(half)])
        fq = jnp.asarray(table)
        any_spec = pl.BlockSpec(memory_space=pl.ANY)
        CK = B * T * slots
        hid, dec, kp, vp, kn, vn = pl.pallas_call(
            kernel,
            name='prefill_decode',
            out_shape=[jax.ShapeDtypeStruct(s, BF) for s in
                       ((R, D), (B, D), (max_req * 2, HD), (max_req * 2, HD), (CK, HD), (CK, HD))],
            in_specs=[any_spec] * 13,
            out_specs=[any_spec] * 6,
            scratch_shapes=scratch,
            compiler_params=pltpu.CompilerParams(collective_id=0, has_side_effects=True, vmem_limit_bytes=67043328),
        )(x_loc, y_loc[0], w_qkv[0], w_out[0], w_gate[0], w_up[0], w_down[0],
          kc_loc.reshape(CK, HD), vc_loc.reshape(CK, HD), req_len, dest, clen_loc[0], fq)
        hid, dec, kp, vp, kn, vn = write_out(hid, dec, kp, vp, kn, vn)
        cache = (1, 1, B, T, slots, HD)
        prompt = (1, 1, max_req, slots, HD)
        return hid, dec[None], kp.reshape(prompt), vp.reshape(prompt), kn.reshape(cache), vn.reshape(cache)

    return jax.shard_map(local_step, mesh=mesh,
                         in_specs=(rows_spec, P('pair'), P('pair'), P(), P(), P(), P(), P(), batch_spec, cache_spec, cache_spec, rows_spec),
                         out_specs=(rows_spec, batch_spec, prompt_spec, prompt_spec, cache_spec, cache_spec),
                         check_vma=False)
```

```python
import jax
import jax.numpy as jnp
import numpy as np
from jax import lax
from jax.experimental import pallas as pl
from jax.experimental.pallas import tpu as pltpu
from jax.sharding import PartitionSpec as P

ROPE_BASE = 10000.0
NORM_EPS = 1e-5
BF = jnp.bfloat16
F32 = jnp.float32
CW = 256
GU_SLOTS = 10
MESH = pl.DeviceIdType.MESH


def mult(v, m):
    return pl.multiple_of(v, m)


def make_kernel(tp_size, side_size, R, D, B, T, Q, KV, HD, F, max_req):
    heads_local = Q // HD // tp_size
    rep = heads_local // 2
    hw = rep * HD
    qw = 2 * hw
    RT = R // tp_size
    DH = D // 2
    FH = F // 2
    M1 = R + B
    M2 = 2 * RT + 2 * B
    n_kv, n_q = 2 * 2 * HD // CW, qw // CW
    n_o, n_g, n_d = DH // CW, FH // CW, DH // CW
    wo_base = -(-(n_kv + n_q) * D // F) * F
    gu_base = wo_base + n_o * Q
    slab_rows = gu_base + GU_SLOTS * 2 * D
    CK = B * T * 2
    PR = max_req * 2
    scale = HD ** -0.5
    WK = max_req + RT
    n_first = wo_base // F
    AW = max(w for w in range(CW, D + 1, CW) if FH % w == 0)
    AB, AN = AW // CW, FH // AW
    nblk = side_size

    def kernel(x_h, y_h, wqkv_h, wo_h, wg_h, wu_h, wd_h, kc_h, vc_h, rl_h, dst_h, cl_h, fq_h,
               hid_o, dec_o, kp_o, vp_o, kn_o, vn_o,
               rl, dst, cl, fq, slab, ub, ys, raw, qs, kva, knv, kcs, vcs, cos_s, sin_s, bias_s,
               dcs, cst, ctxr, xres, hf, outst, hid, decb,
               in_sem, w_sem, g_sem, d_sem, xr_s, xr_r, kx_s, kx_r, cx_s, cx_r, cf_s, cf_r,
               dx_s, dx_r, df_s, df_r, h_s, h_r, a_s, a_r, f_s, f_r, r_s, r_r, o_sem):
        xs, xn = ub.at[pl.ds(0, R), :], ub.at[pl.ds(R, M1), :]
        side = lax.axis_index('side')
        tp = lax.axis_index('tp')
        core = lax.rem(side, 2)
        oc = 1 - core
        partner = side + 1 - 2 * core
        left = lax.rem(side + side_size - 2, side_size)
        right = lax.rem(side + 2, side_size)
        far = lax.rem(side + 4, side_size)
        p_left = lax.rem(partner + side_size - 2, side_size)
        p_right = lax.rem(partner + 2, side_size)
        p_far = lax.rem(partner + 4, side_size)

        def at(d):
            return lax.rem(tp + d, tp_size)

        def dev(s, t):
            return {'side': s, 'tp': t}

        q_cols0, k_cols0, v_cols0 = 0, Q, Q + KV
        hcol = [tp * hw, (tp + tp_size) * hw]
        kcol = [k_cols0 + tp * HD, k_cols0 + (tp + tp_size) * HD]
        vcol = [v_cols0 + tp * HD, v_cols0 + (tp + tp_size) * HD]

        def pieces(u):
            if u < 2:
                return [(kcol[u], 0, HD), (vcol[u], HD, HD)]
            lo, hi = (u - 2) * CW, (u - 1) * CW
            out = []
            for j in range(2):
                a, b = max(lo, j * hw), min(hi, (j + 1) * hw)
                if a < b:
                    out.append((hcol[j] + (a - j * hw), a - lo, b - a))
            return out

        def start_qkv(u):
            for src, d0, w in pieces(u):
                pltpu.make_async_copy(wqkv_h.at[:, pl.ds(mult(src, 128), w)],
                                      slab.at[pl.ds(u * D, D), pl.ds(d0, w)], w_sem.at[u]).start()

        def slab_wait(base, rows, sem):
            pltpu.make_async_copy(slab.at[pl.ds(base, rows), :], slab.at[pl.ds(base, rows), :], sem).wait()

        def start_wo(u):
            col = mult(core * DH + u * CW, 128)
            pltpu.make_async_copy(wo_h.at[:, pl.ds(col, CW)], slab.at[pl.ds(wo_base + u * Q, Q), :],
                                  w_sem.at[n_kv + n_q + u]).start()

        def start_gu(j, slot):
            col = mult(core * FH + j * CW, 128)
            base = mult(gu_base + slot * (2 * D), 256)
            pltpu.make_async_copy(wg_h.at[:, pl.ds(col, CW)], slab.at[pl.ds(base, D), :], g_sem.at[slot]).start()
            pltpu.make_async_copy(wu_h.at[:, pl.ds(col, CW)], slab.at[pl.ds(mult(base + D, 256), D), :], g_sem.at[slot]).start()

        def d_copy(n):
            return pltpu.make_async_copy(wd_h.at[:, pl.ds(mult(core * DH + n * CW, 128), CW)],
                                         slab.at[pl.ds(mult(n * F, 256), F), :], d_sem.at[n])

        small = [pltpu.make_async_copy(a, b, in_sem.at[6 + i])
                 for i, (a, b) in enumerate(((rl_h, rl), (dst_h, dst), (cl_h, cl), (fq_h, fq)))]
        XC = 4
        x_in = [pltpu.make_async_copy(x_h.at[pl.ds(i * (R // XC), R // XC), :], xs.at[pl.ds(i * (R // XC), R // XC), :],
                                      in_sem.at[10 + i]) for i in range(XC)]
        y_in = pltpu.make_async_copy(y_h, ys, in_sem.at[1])
        for cp in small + x_in + [y_in]:
            cp.start()

        peers = [(partner, tp), (left, tp), (right, tp), (side, at(1)), (side, at(tp_size - 1)), (side, at(2)),
                 (partner, at(1)), (partner, at(tp_size - 1))]
        barrier = pltpu.get_barrier_semaphore()
        for s, t in peers:
            pl.semaphore_signal(barrier, inc=1, device_id=dev(s, t), device_id_type=MESH)

        kc_in = pltpu.make_async_copy(kc_h, kcs, in_sem.at[2])
        vc_in = pltpu.make_async_copy(vc_h, vcs, in_sem.at[3])
        row_t = mult(tp * RT, RT)
        my_cols = mult(core * DH, 128)
        xres_l = [pltpu.make_async_copy(x_h.at[pl.ds(row_t, RT), pl.ds(my_cols, DH)],
                                        xres.at[pl.ds(mult(core * RT, RT), RT), :], in_sem.at[4]),
                  pltpu.make_async_copy(y_h.at[:, pl.ds(my_cols, DH)],
                                        xres.at[pl.ds(mult(2 * RT + core * B, B), B), :], in_sem.at[5])]

        def seg_of(rows):
            seg = jnp.zeros_like(rows)
            total = jnp.int32(0)
            for r in range(nblk):
                total = total + rl[r]
                seg = jnp.where(rows >= total, total, seg)
            return seg

        for cp in small:
            cp.wait()
        idx = lax.broadcasted_iota(jnp.int32, (M1, 1), 0)
        rows = idx + side * R
        pos = rows - seg_of(rows)
        for b in range(B):
            pos = jnp.where(idx == R + b, cl[b], pos)
        ang = pos.astype(F32) * fq[0:1, :]
        cos_s[...] = jnp.cos(ang)
        sin_s[...] = jnp.sin(ang) * fq[1:2, :]

        def norm(v):
            w = v.astype(F32)
            sc = lax.rsqrt(jnp.sum(w * w, axis=-1, keepdims=True) / D + NORM_EPS)
            return (w * sc).astype(BF)

        for i in range(XC):
            x_in[i].wait()
            start_qkv(i)

            def norm_x(k, c, i=i):
                r = pl.ds(mult(i * (R // XC) + k * 32, 32), 32)
                xn[r, :] = norm(xs[r, :])
                return c

            lax.fori_loop(0, R // XC // 32, norm_x, 0, unroll=True)
        for u in range(XC, n_kv + n_q):
            start_qkv(u)
        y_in.wait()
        xn[pl.ds(R, B), :] = norm(ys[...])

        def remote(src, dst_ref, ss, rs, s, t):
            return pltpu.make_async_remote_copy(src_ref=src, dst_ref=dst_ref, send_sem=ss, recv_sem=rs,
                                                device_id=dev(s, t), device_id_type=MESH)

        his_cols = mult(oc * DH, 128)
        xres_r = [remote(x_h.at[pl.ds(row_t, RT), pl.ds(his_cols, DH)], xres.at[pl.ds(mult(core * RT, RT), RT), :],
                         xr_s.at[0], xr_r.at[0], partner, tp),
                  remote(y_h.at[:, pl.ds(his_cols, DH)], xres.at[pl.ds(mult(2 * RT + core * B, B), B), :],
                         xr_s.at[1], xr_r.at[1], partner, tp)]

        def project(u):
            w = slab[pl.ds(mult(u * D, 256), D), :]
            raw[pl.ds(mult(u * M1, 16), M1), :] = jnp.dot(xn[...], w, preferred_element_type=F32).astype(BF)

        def rope(v):
            w = v.astype(F32)
            return (w * cos_s[...] + pltpu.roll(w, HD // 2, 1) * sin_s[...]).astype(BF)


        def blk(b, i0, n):
            return kva.at[pl.ds(i0, n), pl.ds(mult(b * R, R), R), :]

        plan = [(side, 0, 1, right, left), (side, 1, 1, right, left),
                (side, 0, 1, partner, partner), (side, 1, 1, partner, partner),
                (side, 0, 2, left, right),
                (left, 0, 1, partner, p_left), (left, 1, 1, partner, p_left),
                (left, 0, 1, right, far),
                (right, 0, 2, partner, p_right), (right, 1, 1, left, far),
                (far, 0, 1, partner, p_far), (far, 1, 1, partner, p_far)]
        kx = [remote(blk(b, i0, n), blk(b, i0, n), kx_s.at[i], kx_r.at[i], to, tp)
              for i, (b, i0, n, to, _) in enumerate(plan)]

        def got(i):
            ref = blk(plan[i][4], plan[i][1], plan[i][2])
            pltpu.make_async_copy(ref, ref, kx_r.at[i]).wait()

        own_rows = pl.ds(mult(side * R, R), R)
        pl.semaphore_wait(barrier, len(peers))

        def keys_values(j, c):
            slab_wait(mult(j * D, 256), D, w_sem.at[j])
            project(j)
            k_j = rope(raw[pl.ds(mult(j * M1, 16), M1), pl.ds(0, HD)])
            v_j = raw[pl.ds(mult(j * M1, 16), M1), pl.ds(HD, HD)]
            kva[j, own_rows, pl.ds(0, HD)] = k_j[:R]
            kva[j, own_rows, pl.ds(HD, HD)] = v_j[:R]
            ref = blk(side, j, 1)
            remote(ref, ref, kx_s.at[j], kx_r.at[j], right, tp).start()
            remote(ref, ref, kx_s.at[2 + j], kx_r.at[2 + j], partner, tp).start()
            knv[pl.ds(mult(j * B, B), B), pl.ds(0, HD)] = k_j[R:]
            knv[pl.ds(mult(j * B, B), B), pl.ds(HD, HD)] = v_j[R:]
            return c

        lax.fori_loop(0, 2, keys_values, 0)
        kx[4].start()
        for cp in xres_r:
            cp.start()
        knv[:, pl.ds(2 * HD, HD)] = jnp.ones((2 * B, HD), BF)

        for cp in [kc_in, vc_in] + xres_l:
            cp.start()
        for u in range(n_o):
            start_wo(u)
        for u in range(n_kv, n_kv + n_q):
            slab_wait(u * D, D, w_sem.at[u])

        def queries(i, c):
            for u in range(n_q):
                raw[pl.ds((n_kv + u) * M1, M1), :] = jnp.dot(xn[...], slab[pl.ds(mult((n_kv + u + i) * D, 256), D), :], preferred_element_type=F32).astype(BF)
            return c

        lax.fori_loop(0, tp // tp_size + 1, queries, 0)
        for slot in range(GU_SLOTS):
            start_gu(slot, slot)
        for n in range(n_first):
            d_copy(n).start()
        for h in range(heads_local):
            u, off = divmod(h * HD, CW)
            qs[h] = rope(raw[pl.ds((n_kv + u) * M1, M1), pl.ds(off, HD)])

        kc_in.wait()
        vc_in.wait()
        lane2 = lax.broadcasted_iota(jnp.int32, (1, 2 * B), 1)
        len2 = jnp.zeros((1, 2 * B), jnp.int32)
        for b in range(B):
            len2 = jnp.where(lax.rem(lane2, B) == b, cl[b], len2)
        code2 = (lax.rem(lane2, B) * T + len2) * 2 + lane2 // B
        CH = 256

        def insert(i, c):
            r0 = mult(i * CH, CH)
            rr = lax.broadcasted_iota(jnp.int32, (CH, 1), 0) + r0
            pick = jnp.where(rr == code2, 1.0, 0.0).astype(BF)
            new = jnp.dot(pick, knv[...], preferred_element_type=F32)
            hit = new[:, 2 * HD:] > 0.5
            sl = pl.ds(r0, CH)
            kcs[sl, :] = jnp.where(hit, new[:, :HD], kcs[sl, :].astype(F32)).astype(BF)
            vcs[sl, :] = jnp.where(hit, new[:, HD:2 * HD], vcs[sl, :].astype(F32)).astype(BF)
            return c

        lax.fori_loop(0, CK // CH, insert, 0)
        inner = side >= 2

        @pl.when(inner)
        def _():
            got(0)
            kx[5].start()
            kx[7].start()

        kn_out = pltpu.make_async_copy(kcs, kn_o, o_sem.at[0])
        vn_out = pltpu.make_async_copy(vcs, vn_o, o_sem.at[1])
        kn_out.start()
        vn_out.start()

        HB = heads_local * B
        q_dec = qs[:, pl.ds(R, B), :].reshape(HB, HD)
        s_dec = lax.dot_general(q_dec, kcs[...], (((1,), (1,)), ((), ())), preferred_element_type=F32) * scale
        qi = lax.broadcasted_iota(jnp.int32, (HB, 1), 0)
        ki = lax.broadcasted_iota(jnp.int32, (1, CK), 1)
        q_len = jnp.zeros((HB, 1), jnp.int32)
        for b in range(B):
            q_len = jnp.where(lax.rem(qi, B) == b, cl[b], q_len)
        q_code = lax.rem(qi, B) * 2 + qi // (rep * B)
        k_code = (ki // (2 * T)) * 2 + lax.rem(ki, 2)
        k_pos = lax.rem(ki // 2, T)
        s_dec = jnp.where((q_code == k_code) & (k_pos <= q_len), s_dec, -1e30)
        e_dec = jnp.exp(s_dec - jnp.max(s_dec, axis=-1, keepdims=True))
        p_dec = (e_dec / jnp.sum(e_dec, axis=-1, keepdims=True)).astype(BF)
        c_dec = jnp.dot(p_dec, vcs[...], preferred_element_type=F32).astype(BF)
        for h in range(heads_local):
            dcs[h // rep, :, pl.ds((h % rep) * HD, HD)] = c_dec[h * B:(h + 1) * B]
        dec_rows = pl.ds(mult(2 * RT + core * B, B), B)
        hops = (2, 1, 3, 0)
        srcs = (2, 3, 1)
        dec_at = lambda t, rows_: ctxr.at[:, rows_, pl.ds(mult(t * hw, 128), hw)]
        dx = [remote(dcs, dec_at(tp, dec_rows), dx_s.at[k], dx_r.at[k], side, at(hops[k])) for k in range(3)]
        for cp in dx:
            cp.start()
        dec_at(tp, dec_rows)[...] = dcs[...]
        df_own = remote(dcs, dec_at(tp, dec_rows), df_s.at[3], df_r.at[3], partner, tp)
        df_own.start()

        win = []
        for k in range(4):
            r0 = mult(at(hops[k]) * RT, RT)
            lead = side * R + r0 - max_req
            lead = lead * ((lead + 2 * nblk * R) // (2 * nblk * R))
            win.append((r0, mult(lead, RT)))
            q_row = side * R + r0 + lax.broadcasted_iota(jnp.int32, (RT, 1), 0)
            key_row = lead + lax.broadcasted_iota(jnp.int32, (1, WK), 1)
            bias = jnp.where((key_row >= seg_of(q_row)) & (key_row <= q_row), 0.0, -1e30)
            for i in range(WK // CW):
                bias_s[i, pl.ds(k * RT, RT), :] = bias[:, i * CW:(i + 1) * CW]
        got(2)

        @pl.when(inner)
        def _():
            got(5)

        pre_rows = pl.ds(mult(core * RT, RT), RT)
        QR = rep * RT

        def attend(j, k):
            r0, lead = win[k]
            q = qs[pl.ds(j * rep, rep), pl.ds(r0, RT), :].reshape(QR, HD)
            held = lambda i: kva[j, pl.ds(lead, WK), pl.ds(i * HD, HD)]
            s = lax.dot_general(q, held(0), (((1,), (1,)), ((), ())), preferred_element_type=F32)
            s = s.reshape(rep, RT, WK) * scale + jnp.concatenate([bias_s[i, pl.ds(k * RT, RT), :] for i in range(WK // CW)], axis=-1)[None]
            e = jnp.exp(s - jnp.max(s, axis=-1, keepdims=True))
            p = (e * (1.0 / jnp.sum(e, axis=-1, keepdims=True))).astype(BF).reshape(QR, WK)
            o = jnp.dot(p, held(1), preferred_element_type=F32)
            o = o.astype(BF)
            for h in range(rep):
                cst[j, k, :, pl.ds(h * HD, HD)] = o[h * RT:(h + 1) * RT]

        def ctx_at(t, rows_, j):
            return ctxr.at[j, rows_, pl.ds(mult(t * hw, 128), hw)]

        cx = [[remote(cst.at[j, k], ctx_at(tp, pre_rows, j), cx_s.at[j, k], cx_r.at[j, k], side, at(hops[k]))
               for k in range(3)] for j in range(2)]
        cf = [[remote(ctx_at(at(srcs[k]), pre_rows, j), ctx_at(at(srcs[k]), pre_rows, j), cf_s.at[j, k], cf_r.at[j, k], partner, tp)
               for k in range(3)] + [remote(cst.at[j, 3], ctx_at(tp, pre_rows, j), cf_s.at[j, 3], cf_r.at[j, 3], partner, tp)]
              for j in range(2)]

        def pass_ctx(j, k):
            ref = ctx_at(at(srcs[k]), pre_rows, j)
            pltpu.make_async_copy(ref, ref, cx_r.at[j, k]).wait()
            cf[j][k].start()

        df = []
        for j in range(2):
            for k in range(4):
                if k % 2 == 0:
                    attend(j, k)
                    attend(j, k + 1)
                if k < 3:
                    cx[j][k].start()
                else:
                    ctx_at(tp, pre_rows, j)[...] = cst[j, 3]
                    cf[j][3].start()
                if j == 0 and k == 2:
                    @pl.when(inner)
                    def _():
                        got(1)
                        kx[6].start()
            if j == 0:
                got(3)

                @pl.when(inner)
                def _():
                    got(6)

        for k in range(3):
            pass_ctx(0, k)
        for k in range(3):
            ref = dec_at(at(srcs[k]), dec_rows)
            pltpu.make_async_copy(ref, ref, dx_r.at[k]).wait()
            df.append(remote(ref, ref, df_s.at[k], df_r.at[k], partner, tp))
            df[k].start()
        for k in range(3):
            pass_ctx(1, k)
        p_pre = pl.ds(mult(oc * RT, RT), RT)
        p_dec_rows = pl.ds(mult(2 * RT + oc * B, B), B)
        for k in range(4):
            t = at(srcs[k]) if k < 3 else tp
            for j in range(2):
                ref = ctx_at(t, p_pre, j)
                pltpu.make_async_copy(ref, ref, cf_r.at[j, k]).wait()
            ref = dec_at(t, p_dec_rows)
            pltpu.make_async_copy(ref, ref, df_r.at[k]).wait()
        for cp in xres_l:
            cp.wait()
        for i, cp in enumerate(xres_r):
            cp.wait_send()
        ref = xres.at[p_pre, :]
        pltpu.make_async_copy(ref, ref, xr_r.at[0]).wait()
        ref = xres.at[p_dec_rows, :]
        pltpu.make_async_copy(ref, ref, xr_r.at[1]).wait()

        def h_copy(u):
            ref = hf.at[:, pl.ds(mult(core * DH + u * CW, CW), CW)]
            return remote(ref, ref, h_s.at[u], h_r.at[u], partner, tp)

        OU = 2

        def out_proj(i, c):
            for k in range(OU):
                u = i * OU + k
                slab_wait(mult(wo_base + u * Q, 256), Q, w_sem.at[n_kv + n_q + u])
            for k in range(OU):
                u = i * OU + k
                acc = jnp.zeros((M2, CW), F32)
                for j in range(2):
                    acc = acc + jnp.dot(ctxr[j], slab[pl.ds(mult(wo_base + u * Q + j * (Q // 2), 256), Q // 2), :],
                                        preferred_element_type=F32)
                res = xres[:, pl.ds(mult(u * CW, CW), CW)].astype(F32)
                hf[:, pl.ds(mult(core * DH + u * CW, CW), CW)] = (res + acc.astype(BF).astype(F32)).astype(BF)
            for k in range(OU):
                h_copy(i * OU + k).start()
            for n in range(n_first, n_d):
                if (n + 1) * F <= gu_base:
                    @pl.when(i == (min((n + 1) * F - wo_base, n_o * Q) - 1) // (OU * Q))
                    def _(n=n):
                        d_copy(n).start()
            return c

        lax.fori_loop(0, n_o // OU, out_proj, 0)
        @pl.when(side < 2)
        def _():
            for i in (0, 1):
                got(i)
            for i in (5, 6, 7):
                kx[i].start()
            for i in (5, 6):
                got(i)

        got(4)
        kx[8].start()
        kx[9].start()
        for u in range(n_o):
            ref = hf.at[:, pl.ds(mult(oc * DH + u * CW, CW), CW)]
            pltpu.make_async_copy(ref, ref, h_r.at[u]).wait()

        for cp in df + [df_own] + cf[0] + cf[1]:
            cp.wait_send()

        def norm_h(i, c):
            r = pl.ds(mult(i * 32, 32), 32)
            v = norm(hf[r, :])
            for j in range(2):
                ctxr[j, r, :] = v[:, j * DH:(j + 1) * DH]
            return c

        lax.fori_loop(0, M2 // 32, norm_h, 0, unroll=True)

        def act_at(c_of, j):
            g = c_of * n_g + j
            return ub.at[pl.ds(mult((g // AB) * M2, 16), M2), pl.ds(mult(lax.rem(g, AB) * CW, CW), CW)]

        def a_copy(j):
            ref = act_at(core, j)
            return remote(ref, ref, a_s.at[j], a_r.at[j], partner, tp)

        def last_slot(n):
            top = (n + 1) * F - gu_base
            slot = (top - 1) // (2 * D)
            return slot + ((n_g - 1 - slot) // GU_SLOTS) * GU_SLOTS

        def gu_base_of(j):
            return mult(gu_base + lax.rem(j, GU_SLOTS) * (2 * D), 256)

        def gu_next(j):
            @pl.when(j + GU_SLOTS < n_g)
            def _():
                start_gu(j + GU_SLOTS, lax.rem(j, GU_SLOTS))

            for n in range(gu_base // F, n_d):
                @pl.when(j == last_slot(n))
                def _(n=n):
                    d_copy(n).start()

        GU = 2

        def gate_up(i, c):
            for k in range(GU):
                j = i * GU + k
                slab_wait(gu_base_of(j), 2 * D, g_sem.at[lax.rem(j, GU_SLOTS)])
            for k in range(GU):
                j = i * GU + k
                base = gu_base_of(j)
                half = lambda i: slab[pl.ds(mult(base + i * DH, 256), DH), :]
                g = jnp.dot(ctxr[0], half(0), preferred_element_type=F32) + jnp.dot(ctxr[1], half(1), preferred_element_type=F32)
                u = jnp.dot(ctxr[0], half(2), preferred_element_type=F32) + jnp.dot(ctxr[1], half(3), preferred_element_type=F32)
                g = g.astype(BF).astype(F32)
                u = u.astype(BF).astype(F32)
                act_at(core, j)[...] = (g * jax.nn.sigmoid(g) * u).astype(BF)
            for k in range(GU):
                a_copy(i * GU + k).start()
            for k in range(GU):
                gu_next(i * GU + k)
            return c

        lax.fori_loop(0, n_g // GU, gate_up, 0)

        def a_got(j, c):
            ref = act_at(oc, j)
            pltpu.make_async_copy(ref, ref, a_r.at[j]).wait()
            return c

        for i in (7, 9):
            got(i)
        kx[10].start()
        kx[11].start()

        up, down = at(1), at(tp_size - 1)
        own_out = pl.ds(mult(core * RT, RT), RT)
        his_out = pl.ds(mult(oc * RT, RT), RT)
        own_dec = pl.ds(mult(2 * RT + core * B, B), B)
        his_dec = pl.ds(mult(2 * RT + oc * B, B), B)
        rows_of = lambda t: pl.ds(mult(t * RT, RT), RT)

        def f_copies(n):
            cols = pl.ds(mult(core * DH + n * CW, CW), CW)
            there = hid.at[rows_of(tp), cols]
            mine, his = outst.at[n, own_out, :], outst.at[n, his_out, :]
            return [remote(mine, there, f_s.at[0, n], f_r.at[0, n], side, up),
                    remote(mine, there, f_s.at[1, n], f_r.at[1, n], side, down),
                    remote(his, there, f_s.at[2, n], f_r.at[2, n], partner, up),
                    remote(his, there, f_s.at[3, n], f_r.at[3, n], partner, down),
                    remote(his, there, f_s.at[4, n], f_r.at[4, n], partner, tp),
                    remote(outst.at[n, his_dec, :], decb.at[:, cols], f_s.at[5, n], f_r.at[5, n], partner, tp)]

        def down_part(n, c_of):
            acc = None
            for i in range(AN):
                g = c_of * AN + i
                part = jnp.dot(ub[pl.ds(mult(g * M2, 16), M2), pl.ds(0, AW)],
                               slab[pl.ds(mult(n * F + g * AW, 256), AW), :], preferred_element_type=F32)
                acc = part if acc is None else acc + part
            return acc

        def down_end(n, acc):
            cols = pl.ds(mult(core * DH + n * CW, CW), CW)
            outst[n] = (hf[:, cols].astype(F32) + acc.astype(BF).astype(F32)).astype(BF)
            for cp in f_copies(n):
                cp.start()
            hid[rows_of(tp), cols] = outst[n, own_out, :]
            decb[:, cols] = outst[n, own_dec, :]

        EARLY = 2

        def down_first(n, c):
            d_copy(n).wait()
            bias_s[n, pl.ds(0, M2), :] = down_part(n, core)
            return c

        lax.fori_loop(0, EARLY, down_first, 0)
        lax.fori_loop(0, n_g, a_got, 0)

        def down_second(n, c):
            down_end(n, bias_s[n, pl.ds(0, M2), :] + down_part(n, oc))
            return c

        lax.fori_loop(0, EARLY, down_second, 0)

        def down_proj(n, c):
            d_copy(n).wait()
            down_end(n, down_part(n, core) + down_part(n, oc))
            return c

        lax.fori_loop(EARLY, n_d, down_proj, 0)

        def piece(t, c_from, n, of=hid):
            return of.at[rows_of(t), pl.ds(mult(c_from * DH + n * CW, CW), CW)]

        def arrived(ref, sem):
            pltpu.make_async_copy(ref, ref, sem).wait()

        kind = {(0, 1): 0, (1, 1): 1, (0, 0): 2, (1, 0): 3}
        relays = []
        for n in range(n_d):
            for same in (1, 0):
                c_from = core if same else oc
                if n % 2 == 0:
                    ref = piece(down, c_from, n)
                    arrived(ref, f_r.at[kind[(0, same)], n])
                    cp = remote(ref, piece(down, c_from, n, hid_o), r_s.at[same, n], r_r.at[same, n], side, up)
                else:
                    ref = piece(up, c_from, n)
                    arrived(ref, f_r.at[kind[(1, same)], n])
                    cp = remote(ref, piece(up, c_from, n, hid_o), r_s.at[same, n], r_r.at[same, n], side, down)
                cp.start()
                relays.append(cp)

        for i in (8, 10, 11):
            got(i)
        start, length, total = jnp.int32(0), jnp.int32(0), jnp.int32(0)
        for r in range(nblk):
            mine = dst[r] == side
            start = start + jnp.where(mine, total, 0)
            length = length + jnp.where(mine, rl[r], 0)
            total = total + rl[r]
        IR = 128
        col = lax.broadcasted_iota(jnp.int32, (1, 2 * nblk * R), 1)

        def install(i, c):
            r = pl.ds(mult(i * IR, IR), IR)
            o_row = lax.broadcasted_iota(jnp.int32, (IR, 1), 0) + i * IR
            code = jnp.where(o_row // 2 < length, o_row // 2 + start + lax.rem(o_row, 2) * (nblk * R), -1)
            pick = jnp.where(code == col, 1.0, 0.0).astype(BF)
            out = jnp.dot(pick, kva[...].reshape(2 * nblk * R, 2 * HD), preferred_element_type=F32).astype(BF)
            raw[r, :] = out
            return c

        lax.fori_loop(0, PR // IR, install, 0)
        outs = [pltpu.make_async_copy(raw.at[pl.ds(0, PR), pl.ds(i * HD, HD)], o, o_sem.at[2 + i]) for i, o in enumerate((kp_o, vp_o))]
        for cp in outs:
            cp.start()

        def flush(t, i):
            r = rows_of(t)
            cp = pltpu.make_async_copy(hid.at[r, :], hid_o.at[r, :], o_sem.at[4 + i])
            cp.start()
            outs.append(cp)

        for n in range(n_d):
            arrived(piece(tp, oc, n), f_r.at[4, n])
            arrived(decb.at[:, pl.ds(mult(oc * DH + n * CW, CW), CW)], f_r.at[5, n])
        flush(tp, 0)
        cp = pltpu.make_async_copy(decb, dec_o, o_sem.at[8])
        cp.start()
        outs.append(cp)
        for n in range(n_d):
            for same in (1, 0):
                c_from = core if same else oc
                if n % 2 == 0:
                    arrived(piece(up, c_from, n), f_r.at[kind[(1, same)], n])
                else:
                    arrived(piece(down, c_from, n), f_r.at[kind[(0, same)], n])
        flush(up, 1)
        flush(down, 2)
        for n in range(n_d):
            for same in (1, 0):
                arrived(piece(at(2), core if same else oc, n, hid_o), r_r.at[same, n])

        for cp in kx + dx + cx[0] + cx[1] + relays:
            cp.wait_send()

        def h_done(u, c):
            h_copy(u).wait_send()
            return c

        def a_done(j, c):
            a_copy(j).wait_send()
            return c

        def f_done(n, c):
            for cp in f_copies(n):
                cp.wait_send()
            return c

        lax.fori_loop(0, n_o, h_done, 0)
        lax.fori_loop(0, n_g, a_done, 0)
        lax.fori_loop(0, n_d, f_done, 0)
        kn_out.wait()
        vn_out.wait()
        for cp in outs:
            cp.wait()

    dma = lambda *s: pltpu.SemaphoreType.DMA(s)
    scratch = [
        pltpu.SMEM((side_size,), jnp.int32), pltpu.SMEM((side_size,), jnp.int32), pltpu.SMEM((B,), jnp.int32), pltpu.VMEM((8, HD), F32),
        pltpu.VMEM((slab_rows, CW), BF),
        pltpu.VMEM((max(R + M1, 2 * AN * M2), D), BF), pltpu.VMEM((B, D), BF),
        pltpu.VMEM((max((n_kv + n_q) * M1, PR), CW), BF), pltpu.VMEM((heads_local, M1, HD), BF),
        pltpu.VMEM((2, nblk * R, 2 * HD), BF), pltpu.VMEM((2 * B, 3 * HD), BF),
        pltpu.VMEM((CK, HD), BF), pltpu.VMEM((CK, HD), BF),
        pltpu.VMEM((M1, HD), F32), pltpu.VMEM((M1, HD), F32), pltpu.VMEM((WK // CW, max(4 * RT, M2), CW), F32),
        pltpu.VMEM((2, B, hw), BF), pltpu.VMEM((2, 4, RT, hw), BF), pltpu.VMEM((2, M2, Q // 2), BF),
        pltpu.VMEM((M2, DH), BF), pltpu.VMEM((M2, D), BF),
        pltpu.VMEM((n_d, M2, CW), BF), pltpu.VMEM((R, D), BF), pltpu.VMEM((B, D), BF),
        dma(14), dma(n_kv + n_q + n_o), dma(GU_SLOTS), dma(n_d),
        dma(2), dma(2), dma(12), dma(12), dma(2, 3), dma(2, 3), dma(2, 4), dma(2, 4),
        dma(3), dma(3), dma(4), dma(4), dma(n_o), dma(n_o), dma(n_g), dma(n_g),
        dma(6, n_d), dma(6, n_d), dma(2, n_d), dma(2, n_d), dma(9),
    ]
    return kernel, scratch, (R, D, B, PR, HD, CK)


def write_out(*arrays):
    n = len(arrays)
    cuts = []
    for i, a in enumerate(arrays):
        parts = 4 if i == 0 else 1
        step = a.shape[0] // parts
        cuts += [(i, p * step, step) for p in range(parts)]

    def kernel(*refs):
        ins, outs, bufs, sem_in, sem_out = refs[:n], refs[n:2 * n], refs[2 * n:3 * n], refs[3 * n], refs[3 * n + 1]
        reads = [pltpu.make_async_copy(ins[i].at[pl.ds(r, w), :], bufs[i].at[pl.ds(r, w), :], sem_in.at[k])
                 for k, (i, r, w) in enumerate(cuts)]
        writes = [pltpu.make_async_copy(bufs[i].at[pl.ds(r, w), :], outs[i].at[pl.ds(r, w), :], sem_out.at[k])
                  for k, (i, r, w) in enumerate(cuts)]
        for cp in reads:
            cp.start()
        for rd, wr in zip(reads, writes):
            rd.wait()
            wr.start()
        for wr in writes:
            wr.wait()

    any_spec = pl.BlockSpec(memory_space=pl.ANY)
    return pl.pallas_call(
        kernel,
        name='write_out',
        out_shape=[jax.ShapeDtypeStruct(a.shape, a.dtype) for a in arrays],
        in_specs=[any_spec] * n,
        out_specs=[any_spec] * n,
        scratch_shapes=[pltpu.VMEM(a.shape, a.dtype) for a in arrays]
        + [pltpu.SemaphoreType.DMA((len(cuts),)), pltpu.SemaphoreType.DMA((len(cuts),))],
        compiler_params=pltpu.CompilerParams(vmem_limit_bytes=67043328),
    )(*arrays)


def solution(mesh):
    tp_size = mesh.shape['tp']
    side_size = mesh.shape['side']
    rows_spec = P(('pair', 'side'), None)
    batch_spec = P(('pair', 'side'), None, None)
    cache_spec = P(('pair', 'side'), None, None, None, 'tp', None)
    prompt_spec = P(('pair', 'side'), None, None, 'tp', None)

    def local_step(x_loc, req_len, dest, w_qkv, w_out, w_gate, w_up, w_down, y_loc, kc_loc, vc_loc, clen_loc):
        R, D = x_loc.shape
        B, T, slots, HD = kc_loc.shape[2:]
        Q, F = w_out.shape[1], w_gate.shape[2]
        KV = (w_qkv.shape[2] - Q) // 2
        max_req = 2 * R - R // 4
        kernel, scratch, _ = make_kernel(tp_size, side_size, R, D, B, T, Q, KV, HD, F, max_req)
        half = HD // 2
        inv_freq = np.float32(ROPE_BASE) ** (-np.arange(half, dtype=np.float32) / np.float32(half))
        table = np.zeros((8, HD), np.float32)
        table[0] = np.concatenate([inv_freq, inv_freq])
        table[1] = np.concatenate([-np.ones(half), np.ones(half)])
        fq = jnp.asarray(table)
        any_spec = pl.BlockSpec(memory_space=pl.ANY)
        CK = B * T * slots
        hid, dec, kp, vp, kn, vn = pl.pallas_call(
            kernel,
            name='prefill_decode',
            out_shape=[jax.ShapeDtypeStruct(s, BF) for s in
                       ((R, D), (B, D), (max_req * 2, HD), (max_req * 2, HD), (CK, HD), (CK, HD))],
            in_specs=[any_spec] * 13,
            out_specs=[any_spec] * 6,
            scratch_shapes=scratch,
            compiler_params=pltpu.CompilerParams(collective_id=0, has_side_effects=True, vmem_limit_bytes=67043328),
        )(x_loc, y_loc[0], w_qkv[0], w_out[0], w_gate[0], w_up[0], w_down[0],
          kc_loc.reshape(CK, HD), vc_loc.reshape(CK, HD), req_len, dest, clen_loc[0], fq)
        hid, dec, kp, vp, kn, vn = write_out(hid, dec, kp, vp, kn, vn)
        cache = (1, 1, B, T, slots, HD)
        prompt = (1, 1, max_req, slots, HD)
        return hid, dec[None], kp.reshape(prompt), vp.reshape(prompt), kn.reshape(cache), vn.reshape(cache)

    return jax.shard_map(local_step, mesh=mesh,
                         in_specs=(rows_spec, P('pair'), P('pair'), P(), P(), P(), P(), P(), batch_spec, cache_spec, cache_spec, rows_spec),
                         out_specs=(rows_spec, batch_spec, prompt_spec, prompt_spec, cache_spec, cache_spec),
                         check_vma=False)
```

```python
import jax
import jax.numpy as jnp
import numpy as np
from jax import lax
from jax.experimental import pallas as pl
from jax.experimental.pallas import tpu as pltpu
from jax.sharding import PartitionSpec as P

ROPE_BASE = 10000.0
NORM_EPS = 1e-5
BF = jnp.bfloat16
F32 = jnp.float32
CW = 256
GU_SLOTS = 10
MESH = pl.DeviceIdType.MESH


def mult(v, m):
    return pl.multiple_of(v, m)


def make_kernel(tp_size, side_size, R, D, B, T, Q, KV, HD, F, max_req):
    heads_local = Q // HD // tp_size
    rep = heads_local // 2
    hw = rep * HD
    qw = 2 * hw
    RT = R // tp_size
    DH = D // 2
    FH = F // 2
    M1 = R + B
    M2 = 2 * RT + 2 * B
    n_kv, n_q = 2 * 2 * HD // CW, qw // CW
    n_o, n_g, n_d = DH // CW, FH // CW, DH // CW
    wo_base = -(-(n_kv + n_q) * D // F) * F
    gu_base = wo_base + n_o * Q
    slab_rows = gu_base + GU_SLOTS * 2 * D
    CK = B * T * 2
    PR = max_req * 2
    scale = HD ** -0.5
    WK = max_req + RT
    n_first = wo_base // F
    AW = max(w for w in range(CW, D + 1, CW) if FH % w == 0)
    AB, AN = AW // CW, FH // AW
    nblk = side_size

    def kernel(x_h, y_h, wqkv_h, wo_h, wg_h, wu_h, wd_h, kc_h, vc_h, rl_h, dst_h, cl_h, fq_h,
               hid_o, dec_o, kp_o, vp_o, kn_o, vn_o,
               rl, dst, cl, fq, slab, ub, ys, raw, qs, kva, knv, kcs, vcs, cos_s, sin_s, bias_s,
               dcs, cst, ctxr, xres, hf, outst, hid, decb,
               in_sem, w_sem, g_sem, d_sem, xr_s, xr_r, kx_s, kx_r, cx_s, cx_r, cf_s, cf_r,
               dx_s, dx_r, df_s, df_r, h_s, h_r, a_s, a_r, f_s, f_r, r_s, r_r, o_sem):
        xs, xn = ub.at[pl.ds(0, R), :], ub.at[pl.ds(R, M1), :]
        side = lax.axis_index('side')
        tp = lax.axis_index('tp')
        core = lax.rem(side, 2)
        oc = 1 - core
        partner = side + 1 - 2 * core
        left = lax.rem(side + side_size - 2, side_size)
        right = lax.rem(side + 2, side_size)
        far = lax.rem(side + 4, side_size)
        p_left = lax.rem(partner + side_size - 2, side_size)
        p_right = lax.rem(partner + 2, side_size)
        p_far = lax.rem(partner + 4, side_size)

        def at(d):
            return lax.rem(tp + d, tp_size)

        def dev(s, t):
            return {'side': s, 'tp': t}

        q_cols0, k_cols0, v_cols0 = 0, Q, Q + KV
        hcol = [tp * hw, (tp + tp_size) * hw]
        kcol = [k_cols0 + tp * HD, k_cols0 + (tp + tp_size) * HD]
        vcol = [v_cols0 + tp * HD, v_cols0 + (tp + tp_size) * HD]

        def pieces(u):
            if u < 2:
                return [(kcol[u], 0, HD), (vcol[u], HD, HD)]
            lo, hi = (u - 2) * CW, (u - 1) * CW
            out = []
            for j in range(2):
                a, b = max(lo, j * hw), min(hi, (j + 1) * hw)
                if a < b:
                    out.append((hcol[j] + (a - j * hw), a - lo, b - a))
            return out

        def start_qkv(u):
            for src, d0, w in pieces(u):
                pltpu.make_async_copy(wqkv_h.at[:, pl.ds(mult(src, 128), w)],
                                      slab.at[pl.ds(u * D, D), pl.ds(d0, w)], w_sem.at[u]).start()

        def slab_wait(base, rows, sem):
            pltpu.make_async_copy(slab.at[pl.ds(base, rows), :], slab.at[pl.ds(base, rows), :], sem).wait()

        def start_wo(u):
            col = mult(core * DH + u * CW, 128)
            pltpu.make_async_copy(wo_h.at[:, pl.ds(col, CW)], slab.at[pl.ds(wo_base + u * Q, Q), :],
                                  w_sem.at[n_kv + n_q + u]).start()

        def start_gu(j, slot):
            col = mult(core * FH + j * CW, 128)
            base = mult(gu_base + slot * (2 * D), 256)
            pltpu.make_async_copy(wg_h.at[:, pl.ds(col, CW)], slab.at[pl.ds(base, D), :], g_sem.at[slot]).start()
            pltpu.make_async_copy(wu_h.at[:, pl.ds(col, CW)], slab.at[pl.ds(mult(base + D, 256), D), :], g_sem.at[slot]).start()

        def d_copy(n):
            return pltpu.make_async_copy(wd_h.at[:, pl.ds(mult(core * DH + n * CW, 128), CW)],
                                         slab.at[pl.ds(mult(n * F, 256), F), :], d_sem.at[n])

        small = [pltpu.make_async_copy(a, b, in_sem.at[6 + i])
                 for i, (a, b) in enumerate(((rl_h, rl), (dst_h, dst), (cl_h, cl), (fq_h, fq)))]
        XC = 4
        x_in = [pltpu.make_async_copy(x_h.at[pl.ds(i * (R // XC), R // XC), :], xs.at[pl.ds(i * (R // XC), R // XC), :],
                                      in_sem.at[10 + i]) for i in range(XC)]
        y_in = pltpu.make_async_copy(y_h, ys, in_sem.at[1])
        for cp in small + x_in + [y_in]:
            cp.start()
        start_qkv(0)

        peers = [(partner, tp), (left, tp), (right, tp), (side, at(1)), (side, at(tp_size - 1)), (side, at(2)),
                 (partner, at(1)), (partner, at(tp_size - 1))]
        barrier = pltpu.get_barrier_semaphore()
        for s, t in peers:
            pl.semaphore_signal(barrier, inc=1, device_id=dev(s, t), device_id_type=MESH)

        kc_in = pltpu.make_async_copy(kc_h, kcs, in_sem.at[2])
        vc_in = pltpu.make_async_copy(vc_h, vcs, in_sem.at[3])
        row_t = mult(tp * RT, RT)
        my_cols = mult(core * DH, 128)
        xres_l = [pltpu.make_async_copy(x_h.at[pl.ds(row_t, RT), pl.ds(my_cols, DH)],
                                        xres.at[pl.ds(mult(core * RT, RT), RT), :], in_sem.at[4]),
                  pltpu.make_async_copy(y_h.at[:, pl.ds(my_cols, DH)],
                                        xres.at[pl.ds(mult(2 * RT + core * B, B), B), :], in_sem.at[5])]

        def seg_of(rows):
            seg = jnp.zeros_like(rows)
            total = jnp.int32(0)
            for r in range(nblk):
                total = total + rl[r]
                seg = jnp.where(rows >= total, total, seg)
            return seg

        for cp in small:
            cp.wait()
        idx = lax.broadcasted_iota(jnp.int32, (M1, 1), 0)
        rows = idx + side * R
        pos = rows - seg_of(rows)
        for b in range(B):
            pos = jnp.where(idx == R + b, cl[b], pos)
        ang = pos.astype(F32) * fq[0:1, :]
        cos_s[...] = jnp.cos(ang)
        sin_s[...] = jnp.sin(ang) * fq[1:2, :]

        def norm(v):
            w = v.astype(F32)
            sc = lax.rsqrt(jnp.sum(w * w, axis=-1, keepdims=True) / D + NORM_EPS)
            return (w * sc).astype(BF)

        for i in range(XC):
            x_in[i].wait()
            start_qkv(i + 1)

            def norm_x(k, c, i=i):
                r = pl.ds(mult(i * (R // XC) + k * 32, 32), 32)
                xn[r, :] = norm(xs[r, :])
                return c

            lax.fori_loop(0, R // XC // 32, norm_x, 0, unroll=True)
        for u in range(XC + 1, n_kv + n_q):
            start_qkv(u)
        y_in.wait()
        xn[pl.ds(R, B), :] = norm(ys[...])

        def remote(src, dst_ref, ss, rs, s, t):
            return pltpu.make_async_remote_copy(src_ref=src, dst_ref=dst_ref, send_sem=ss, recv_sem=rs,
                                                device_id=dev(s, t), device_id_type=MESH)

        his_cols = mult(oc * DH, 128)
        xres_r = [remote(x_h.at[pl.ds(row_t, RT), pl.ds(his_cols, DH)], xres.at[pl.ds(mult(core * RT, RT), RT), :],
                         xr_s.at[0], xr_r.at[0], partner, tp),
                  remote(y_h.at[:, pl.ds(his_cols, DH)], xres.at[pl.ds(mult(2 * RT + core * B, B), B), :],
                         xr_s.at[1], xr_r.at[1], partner, tp)]

        def project(u):
            w = slab[pl.ds(mult(u * D, 256), D), :]
            raw[pl.ds(mult(u * M1, 16), M1), :] = jnp.dot(xn[...], w, preferred_element_type=F32).astype(BF)

        def rope(v):
            w = v.astype(F32)
            return (w * cos_s[...] + pltpu.roll(w, HD // 2, 1) * sin_s[...]).astype(BF)


        def blk(b, i0, n):
            return kva.at[pl.ds(i0, n), pl.ds(mult(b * R, R), R), :]

        plan = [(side, 0, 1, right, left), (side, 1, 1, right, left),
                (side, 0, 1, partner, partner), (side, 1, 1, partner, partner),
                (side, 0, 2, left, right),
                (left, 0, 1, partner, p_left), (left, 1, 1, partner, p_left),
                (left, 0, 1, right, far),
                (right, 0, 2, partner, p_right), (right, 1, 1, left, far),
                (far, 0, 1, partner, p_far), (far, 1, 1, partner, p_far)]
        kx = [remote(blk(b, i0, n), blk(b, i0, n), kx_s.at[i], kx_r.at[i], to, tp)
              for i, (b, i0, n, to, _) in enumerate(plan)]

        def got(i):
            ref = blk(plan[i][4], plan[i][1], plan[i][2])
            pltpu.make_async_copy(ref, ref, kx_r.at[i]).wait()

        own_rows = pl.ds(mult(side * R, R), R)
        pl.semaphore_wait(barrier, len(peers))

        def keys_values(j, c):
            slab_wait(mult(j * D, 256), D, w_sem.at[j])
            project(j)
            k_j = rope(raw[pl.ds(mult(j * M1, 16), M1), pl.ds(0, HD)])
            v_j = raw[pl.ds(mult(j * M1, 16), M1), pl.ds(HD, HD)]
            kva[j, own_rows, pl.ds(0, HD)] = k_j[:R]
            kva[j, own_rows, pl.ds(HD, HD)] = v_j[:R]
            ref = blk(side, j, 1)
            remote(ref, ref, kx_s.at[j], kx_r.at[j], right, tp).start()
            remote(ref, ref, kx_s.at[2 + j], kx_r.at[2 + j], partner, tp).start()
            knv[pl.ds(mult(j * B, B), B), pl.ds(0, HD)] = k_j[R:]
            knv[pl.ds(mult(j * B, B), B), pl.ds(HD, HD)] = v_j[R:]
            return c

        lax.fori_loop(0, 2, keys_values, 0)
        kx[4].start()
        for cp in xres_r:
            cp.start()
        knv[:, pl.ds(2 * HD, HD)] = jnp.ones((2 * B, HD), BF)

        for cp in [kc_in, vc_in] + xres_l:
            cp.start()
        for u in range(n_o):
            start_wo(u)
        for u in range(n_kv, n_kv + n_q):
            slab_wait(u * D, D, w_sem.at[u])

        def queries(i, c):
            for u in range(n_q):
                raw[pl.ds((n_kv + u) * M1, M1), :] = jnp.dot(xn[...], slab[pl.ds(mult((n_kv + u + i) * D, 256), D), :], preferred_element_type=F32).astype(BF)
            return c

        lax.fori_loop(0, tp // tp_size + 1, queries, 0)
        for slot in range(GU_SLOTS):
            start_gu(slot, slot)
        for n in range(n_first):
            d_copy(n).start()
        for h in range(heads_local):
            u, off = divmod(h * HD, CW)
            qs[h] = rope(raw[pl.ds((n_kv + u) * M1, M1), pl.ds(off, HD)])

        kc_in.wait()
        vc_in.wait()
        lane2 = lax.broadcasted_iota(jnp.int32, (1, 2 * B), 1)
        len2 = jnp.zeros((1, 2 * B), jnp.int32)
        for b in range(B):
            len2 = jnp.where(lax.rem(lane2, B) == b, cl[b], len2)
        code2 = (lax.rem(lane2, B) * T + len2) * 2 + lane2 // B
        CH = 256

        def insert(i, c):
            r0 = mult(i * CH, CH)
            rr = lax.broadcasted_iota(jnp.int32, (CH, 1), 0) + r0
            pick = jnp.where(rr == code2, 1.0, 0.0).astype(BF)
            new = jnp.dot(pick, knv[...], preferred_element_type=F32)
            hit = new[:, 2 * HD:] > 0.5
            sl = pl.ds(r0, CH)
            kcs[sl, :] = jnp.where(hit, new[:, :HD], kcs[sl, :].astype(F32)).astype(BF)
            vcs[sl, :] = jnp.where(hit, new[:, HD:2 * HD], vcs[sl, :].astype(F32)).astype(BF)
            return c

        lax.fori_loop(0, CK // CH, insert, 0)
        inner = side >= 2

        @pl.when(inner)
        def _():
            got(0)
            kx[5].start()
            kx[7].start()

        kn_out = pltpu.make_async_copy(kcs, kn_o, o_sem.at[0])
        vn_out = pltpu.make_async_copy(vcs, vn_o, o_sem.at[1])
        kn_out.start()
        vn_out.start()

        HB = heads_local * B
        q_dec = qs[:, pl.ds(R, B), :].reshape(HB, HD)
        s_dec = lax.dot_general(q_dec, kcs[...], (((1,), (1,)), ((), ())), preferred_element_type=F32) * scale
        qi = lax.broadcasted_iota(jnp.int32, (HB, 1), 0)
        ki = lax.broadcasted_iota(jnp.int32, (1, CK), 1)
        q_len = jnp.zeros((HB, 1), jnp.int32)
        for b in range(B):
            q_len = jnp.where(lax.rem(qi, B) == b, cl[b], q_len)
        q_code = lax.rem(qi, B) * 2 + qi // (rep * B)
        k_code = (ki // (2 * T)) * 2 + lax.rem(ki, 2)
        k_pos = lax.rem(ki // 2, T)
        s_dec = jnp.where((q_code == k_code) & (k_pos <= q_len), s_dec, -1e30)
        e_dec = jnp.exp(s_dec - jnp.max(s_dec, axis=-1, keepdims=True))
        p_dec = (e_dec / jnp.sum(e_dec, axis=-1, keepdims=True)).astype(BF)
        c_dec = jnp.dot(p_dec, vcs[...], preferred_element_type=F32).astype(BF)
        for h in range(heads_local):
            dcs[h // rep, :, pl.ds((h % rep) * HD, HD)] = c_dec[h * B:(h + 1) * B]
        dec_rows = pl.ds(mult(2 * RT + core * B, B), B)
        hops = (2, 1, 3, 0)
        srcs = (2, 3, 1)
        dec_at = lambda t, rows_: ctxr.at[:, rows_, pl.ds(mult(t * hw, 128), hw)]
        dx = [remote(dcs, dec_at(tp, dec_rows), dx_s.at[k], dx_r.at[k], side, at(hops[k])) for k in range(3)]
        for cp in dx:
            cp.start()
        dec_at(tp, dec_rows)[...] = dcs[...]
        df_own = remote(dcs, dec_at(tp, dec_rows), df_s.at[3], df_r.at[3], partner, tp)
        df_own.start()

        win = []
        for k in range(4):
            r0 = mult(at(hops[k]) * RT, RT)
            lead = side * R + r0 - max_req
            lead = lead * ((lead + 2 * nblk * R) // (2 * nblk * R))
            win.append((r0, mult(lead, RT)))
            q_row = side * R + r0 + lax.broadcasted_iota(jnp.int32, (RT, 1), 0)
            key_row = lead + lax.broadcasted_iota(jnp.int32, (1, WK), 1)
            bias = jnp.where((key_row >= seg_of(q_row)) & (key_row <= q_row), 0.0, -1e30)
            for i in range(WK // CW):
                bias_s[i, pl.ds(k * RT, RT), :] = bias[:, i * CW:(i + 1) * CW]
        got(2)

        @pl.when(inner)
        def _():
            got(5)

        pre_rows = pl.ds(mult(core * RT, RT), RT)
        QR = rep * RT

        def attend(j, k):
            r0, lead = win[k]
            q = qs[pl.ds(j * rep, rep), pl.ds(r0, RT), :].reshape(QR, HD)
            held = lambda i: kva[j, pl.ds(lead, WK), pl.ds(i * HD, HD)]
            s = lax.dot_general(q, held(0), (((1,), (1,)), ((), ())), preferred_element_type=F32)
            s = s.reshape(rep, RT, WK) * scale + jnp.concatenate([bias_s[i, pl.ds(k * RT, RT), :] for i in range(WK // CW)], axis=-1)[None]
            e = jnp.exp(s - jnp.max(s, axis=-1, keepdims=True))
            p = (e * (1.0 / jnp.sum(e, axis=-1, keepdims=True))).astype(BF).reshape(QR, WK)
            o = jnp.dot(p, held(1), preferred_element_type=F32)
            o = o.astype(BF)
            for h in range(rep):
                cst[j, k, :, pl.ds(h * HD, HD)] = o[h * RT:(h + 1) * RT]

        def ctx_at(t, rows_, j):
            return ctxr.at[j, rows_, pl.ds(mult(t * hw, 128), hw)]

        cx = [[remote(cst.at[j, k], ctx_at(tp, pre_rows, j), cx_s.at[j, k], cx_r.at[j, k], side, at(hops[k]))
               for k in range(3)] for j in range(2)]
        cf = [[remote(ctx_at(at(srcs[k]), pre_rows, j), ctx_at(at(srcs[k]), pre_rows, j), cf_s.at[j, k], cf_r.at[j, k], partner, tp)
               for k in range(3)] + [remote(cst.at[j, 3], ctx_at(tp, pre_rows, j), cf_s.at[j, 3], cf_r.at[j, 3], partner, tp)]
              for j in range(2)]

        def pass_ctx(j, k):
            ref = ctx_at(at(srcs[k]), pre_rows, j)
            pltpu.make_async_copy(ref, ref, cx_r.at[j, k]).wait()
            cf[j][k].start()

        df = []
        for j in range(2):
            for k in range(4):
                if k % 2 == 0:
                    attend(j, k)
                    attend(j, k + 1)
                if k < 3:
                    cx[j][k].start()
                else:
                    ctx_at(tp, pre_rows, j)[...] = cst[j, 3]
                    cf[j][3].start()
                if j == 0 and k == 2:
                    @pl.when(inner)
                    def _():
                        got(1)
                        kx[6].start()
            if j == 0:
                got(3)

                @pl.when(inner)
                def _():
                    got(6)

        for k in range(3):
            pass_ctx(0, k)
        for k in range(3):
            ref = dec_at(at(srcs[k]), dec_rows)
            pltpu.make_async_copy(ref, ref, dx_r.at[k]).wait()
            df.append(remote(ref, ref, df_s.at[k], df_r.at[k], partner, tp))
            df[k].start()
        for k in range(3):
            pass_ctx(1, k)
        p_pre = pl.ds(mult(oc * RT, RT), RT)
        p_dec_rows = pl.ds(mult(2 * RT + oc * B, B), B)
        for k in range(4):
            t = at(srcs[k]) if k < 3 else tp
            for j in range(2):
                ref = ctx_at(t, p_pre, j)
                pltpu.make_async_copy(ref, ref, cf_r.at[j, k]).wait()
            ref = dec_at(t, p_dec_rows)
            pltpu.make_async_copy(ref, ref, df_r.at[k]).wait()
        for cp in xres_l:
            cp.wait()
        for i, cp in enumerate(xres_r):
            cp.wait_send()
        ref = xres.at[p_pre, :]
        pltpu.make_async_copy(ref, ref, xr_r.at[0]).wait()
        ref = xres.at[p_dec_rows, :]
        pltpu.make_async_copy(ref, ref, xr_r.at[1]).wait()

        def h_copy(u):
            ref = hf.at[:, pl.ds(mult(core * DH + u * CW, CW), CW)]
            return remote(ref, ref, h_s.at[u], h_r.at[u], partner, tp)

        OU = 2

        def out_proj(i, c):
            for k in range(OU):
                u = i * OU + k
                slab_wait(mult(wo_base + u * Q, 256), Q, w_sem.at[n_kv + n_q + u])
            for k in range(OU):
                u = i * OU + k
                acc = jnp.zeros((M2, CW), F32)
                for j in range(2):
                    acc = acc + jnp.dot(ctxr[j], slab[pl.ds(mult(wo_base + u * Q + j * (Q // 2), 256), Q // 2), :],
                                        preferred_element_type=F32)
                res = xres[:, pl.ds(mult(u * CW, CW), CW)].astype(F32)
                hf[:, pl.ds(mult(core * DH + u * CW, CW), CW)] = (res + acc.astype(BF).astype(F32)).astype(BF)
            for k in range(OU):
                h_copy(i * OU + k).start()
            for n in range(n_first, n_d):
                if (n + 1) * F <= gu_base:
                    @pl.when(i == (min((n + 1) * F - wo_base, n_o * Q) - 1) // (OU * Q))
                    def _(n=n):
                        d_copy(n).start()
            return c

        lax.fori_loop(0, n_o // OU, out_proj, 0)
        @pl.when(side < 2)
        def _():
            for i in (0, 1):
                got(i)
            for i in (5, 6, 7):
                kx[i].start()

        got(4)
        kx[8].start()
        kx[9].start()
        for u in range(n_o):
            ref = hf.at[:, pl.ds(mult(oc * DH + u * CW, CW), CW)]
            pltpu.make_async_copy(ref, ref, h_r.at[u]).wait()

        for cp in df + [df_own] + cf[0] + cf[1]:
            cp.wait_send()

        def norm_h(i, c):
            r = pl.ds(mult(i * 32, 32), 32)
            v = norm(hf[r, :])
            for j in range(2):
                ctxr[j, r, :] = v[:, j * DH:(j + 1) * DH]
            return c

        lax.fori_loop(0, M2 // 32, norm_h, 0, unroll=True)

        def act_at(c_of, j):
            g = c_of * n_g + j
            return ub.at[pl.ds(mult((g // AB) * M2, 16), M2), pl.ds(mult(lax.rem(g, AB) * CW, CW), CW)]

        def a_copy(j):
            ref = act_at(core, j)
            return remote(ref, ref, a_s.at[j], a_r.at[j], partner, tp)

        def last_slot(n):
            top = (n + 1) * F - gu_base
            slot = (top - 1) // (2 * D)
            return slot + ((n_g - 1 - slot) // GU_SLOTS) * GU_SLOTS

        def gu_base_of(j):
            return mult(gu_base + lax.rem(j, GU_SLOTS) * (2 * D), 256)

        def gu_next(j):
            @pl.when(j + GU_SLOTS < n_g)
            def _():
                start_gu(j + GU_SLOTS, lax.rem(j, GU_SLOTS))

            for n in range(gu_base // F, n_d):
                @pl.when(j == last_slot(n))
                def _(n=n):
                    d_copy(n).start()

        GU = 2

        def gate_up(i, c):
            for k in range(GU):
                j = i * GU + k
                slab_wait(gu_base_of(j), 2 * D, g_sem.at[lax.rem(j, GU_SLOTS)])
            for k in range(GU):
                j = i * GU + k
                base = gu_base_of(j)
                half = lambda i: slab[pl.ds(mult(base + i * DH, 256), DH), :]
                g = jnp.dot(ctxr[0], half(0), preferred_element_type=F32) + jnp.dot(ctxr[1], half(1), preferred_element_type=F32)
                u = jnp.dot(ctxr[0], half(2), preferred_element_type=F32) + jnp.dot(ctxr[1], half(3), preferred_element_type=F32)
                g = g.astype(BF).astype(F32)
                u = u.astype(BF).astype(F32)
                act_at(core, j)[...] = (g * jax.nn.sigmoid(g) * u).astype(BF)
            for k in range(GU):
                a_copy(i * GU + k).start()
            for k in range(GU):
                gu_next(i * GU + k)
            return c

        lax.fori_loop(0, n_g // GU, gate_up, 0)

        def a_got(j, c):
            ref = act_at(oc, j)
            pltpu.make_async_copy(ref, ref, a_r.at[j]).wait()
            return c

        for i in (7, 9):
            got(i)
        kx[10].start()
        kx[11].start()

        up, down = at(1), at(tp_size - 1)
        own_out = pl.ds(mult(core * RT, RT), RT)
        his_out = pl.ds(mult(oc * RT, RT), RT)
        own_dec = pl.ds(mult(2 * RT + core * B, B), B)
        his_dec = pl.ds(mult(2 * RT + oc * B, B), B)
        rows_of = lambda t: pl.ds(mult(t * RT, RT), RT)

        def f_copies(n):
            cols = pl.ds(mult(core * DH + n * CW, CW), CW)
            there = hid.at[rows_of(tp), cols]
            mine, his = outst.at[n, own_out, :], outst.at[n, his_out, :]
            return [remote(mine, there, f_s.at[0, n], f_r.at[0, n], side, up),
                    remote(mine, there, f_s.at[1, n], f_r.at[1, n], side, down),
                    remote(his, there, f_s.at[2, n], f_r.at[2, n], partner, up),
                    remote(his, there, f_s.at[3, n], f_r.at[3, n], partner, down),
                    remote(his, there, f_s.at[4, n], f_r.at[4, n], partner, tp),
                    remote(outst.at[n, his_dec, :], decb.at[:, cols], f_s.at[5, n], f_r.at[5, n], partner, tp)]

        def down_part(n, c_of):
            acc = None
            for i in range(AN):
                g = c_of * AN + i
                part = jnp.dot(ub[pl.ds(mult(g * M2, 16), M2), pl.ds(0, AW)],
                               slab[pl.ds(mult(n * F + g * AW, 256), AW), :], preferred_element_type=F32)
                acc = part if acc is None else acc + part
            return acc

        def down_end(n, acc):
            cols = pl.ds(mult(core * DH + n * CW, CW), CW)
            outst[n] = (hf[:, cols].astype(F32) + acc.astype(BF).astype(F32)).astype(BF)
            for cp in f_copies(n):
                cp.start()
            hid[rows_of(tp), cols] = outst[n, own_out, :]
            decb[:, cols] = outst[n, own_dec, :]

        EARLY = 2

        def down_first(n, c):
            d_copy(n).wait()
            bias_s[n, pl.ds(0, M2), :] = down_part(n, core)
            return c

        lax.fori_loop(0, EARLY, down_first, 0)
        lax.fori_loop(0, n_g, a_got, 0)

        def down_second(n, c):
            down_end(n, bias_s[n, pl.ds(0, M2), :] + down_part(n, oc))
            return c

        lax.fori_loop(0, EARLY, down_second, 0)

        def down_proj(n, c):
            d_copy(n).wait()
            down_end(n, down_part(n, core) + down_part(n, oc))
            return c

        lax.fori_loop(EARLY, n_d, down_proj, 0)

        def piece(t, c_from, n, of=hid):
            return of.at[rows_of(t), pl.ds(mult(c_from * DH + n * CW, CW), CW)]

        def arrived(ref, sem):
            pltpu.make_async_copy(ref, ref, sem).wait()

        kind = {(0, 1): 0, (1, 1): 1, (0, 0): 2, (1, 0): 3}
        relays = []
        for n in range(n_d):
            for same in (1, 0):
                c_from = core if same else oc
                if n % 2 == 0:
                    ref = piece(down, c_from, n)
                    arrived(ref, f_r.at[kind[(0, same)], n])
                    cp = remote(ref, piece(down, c_from, n, hid_o), r_s.at[same, n], r_r.at[same, n], side, up)
                else:
                    ref = piece(up, c_from, n)
                    arrived(ref, f_r.at[kind[(1, same)], n])
                    cp = remote(ref, piece(up, c_from, n, hid_o), r_s.at[same, n], r_r.at[same, n], side, down)
                cp.start()
                relays.append(cp)

        @pl.when(side < 2)
        def _():
            for i in (5, 6):
                got(i)

        for i in (8, 10, 11):
            got(i)
        start, length, total = jnp.int32(0), jnp.int32(0), jnp.int32(0)
        for r in range(nblk):
            mine = dst[r] == side
            start = start + jnp.where(mine, total, 0)
            length = length + jnp.where(mine, rl[r], 0)
            total = total + rl[r]
        IR = 128
        col = lax.broadcasted_iota(jnp.int32, (1, 2 * nblk * R), 1)

        def install(i, c):
            r = pl.ds(mult(i * IR, IR), IR)
            o_row = lax.broadcasted_iota(jnp.int32, (IR, 1), 0) + i * IR
            code = jnp.where(o_row // 2 < length, o_row // 2 + start + lax.rem(o_row, 2) * (nblk * R), -1)
            pick = jnp.where(code == col, 1.0, 0.0).astype(BF)
            out = jnp.dot(pick, kva[...].reshape(2 * nblk * R, 2 * HD), preferred_element_type=F32).astype(BF)
            raw[r, :] = out
            return c

        lax.fori_loop(0, PR // IR, install, 0)
        outs = [pltpu.make_async_copy(raw.at[pl.ds(0, PR), pl.ds(i * HD, HD)], o, o_sem.at[2 + i]) for i, o in enumerate((kp_o, vp_o))]
        for cp in outs:
            cp.start()

        def flush(t, i):
            r = rows_of(t)
            cp = pltpu.make_async_copy(hid.at[r, :], hid_o.at[r, :], o_sem.at[4 + i])
            cp.start()
            outs.append(cp)

        for n in range(n_d):
            arrived(piece(tp, oc, n), f_r.at[4, n])
            arrived(decb.at[:, pl.ds(mult(oc * DH + n * CW, CW), CW)], f_r.at[5, n])
        flush(tp, 0)
        cp = pltpu.make_async_copy(decb, dec_o, o_sem.at[8])
        cp.start()
        outs.append(cp)
        for n in range(n_d):
            for same in (1, 0):
                c_from = core if same else oc
                if n % 2 == 0:
                    arrived(piece(up, c_from, n), f_r.at[kind[(1, same)], n])
                else:
                    arrived(piece(down, c_from, n), f_r.at[kind[(0, same)], n])
        flush(up, 1)
        flush(down, 2)
        for n in range(n_d):
            for same in (1, 0):
                arrived(piece(at(2), core if same else oc, n, hid_o), r_r.at[same, n])

        for cp in kx + dx + cx[0] + cx[1] + relays:
            cp.wait_send()

        def h_done(u, c):
            h_copy(u).wait_send()
            return c

        def a_done(j, c):
            a_copy(j).wait_send()
            return c

        def f_done(n, c):
            for cp in f_copies(n):
                cp.wait_send()
            return c

        lax.fori_loop(0, n_o, h_done, 0)
        lax.fori_loop(0, n_g, a_done, 0)
        lax.fori_loop(0, n_d, f_done, 0)
        kn_out.wait()
        vn_out.wait()
        for cp in outs:
            cp.wait()

    dma = lambda *s: pltpu.SemaphoreType.DMA(s)
    scratch = [
        pltpu.SMEM((side_size,), jnp.int32), pltpu.SMEM((side_size,), jnp.int32), pltpu.SMEM((B,), jnp.int32), pltpu.VMEM((8, HD), F32),
        pltpu.VMEM((slab_rows, CW), BF),
        pltpu.VMEM((max(R + M1, 2 * AN * M2), D), BF), pltpu.VMEM((B, D), BF),
        pltpu.VMEM((max((n_kv + n_q) * M1, PR), CW), BF), pltpu.VMEM((heads_local, M1, HD), BF),
        pltpu.VMEM((2, nblk * R, 2 * HD), BF), pltpu.VMEM((2 * B, 3 * HD), BF),
        pltpu.VMEM((CK, HD), BF), pltpu.VMEM((CK, HD), BF),
        pltpu.VMEM((M1, HD), F32), pltpu.VMEM((M1, HD), F32), pltpu.VMEM((WK // CW, max(4 * RT, M2), CW), F32),
        pltpu.VMEM((2, B, hw), BF), pltpu.VMEM((2, 4, RT, hw), BF), pltpu.VMEM((2, M2, Q // 2), BF),
        pltpu.VMEM((M2, DH), BF), pltpu.VMEM((M2, D), BF),
        pltpu.VMEM((n_d, M2, CW), BF), pltpu.VMEM((R, D), BF), pltpu.VMEM((B, D), BF),
        dma(14), dma(n_kv + n_q + n_o), dma(GU_SLOTS), dma(n_d),
        dma(2), dma(2), dma(12), dma(12), dma(2, 3), dma(2, 3), dma(2, 4), dma(2, 4),
        dma(3), dma(3), dma(4), dma(4), dma(n_o), dma(n_o), dma(n_g), dma(n_g),
        dma(6, n_d), dma(6, n_d), dma(2, n_d), dma(2, n_d), dma(9),
    ]
    return kernel, scratch, (R, D, B, PR, HD, CK)


def write_out(*arrays):
    n = len(arrays)
    cuts = []
    for i, a in enumerate(arrays):
        parts = 4 if i == 0 else 1
        step = a.shape[0] // parts
        cuts += [(i, p * step, step) for p in range(parts)]

    def kernel(*refs):
        ins, outs, bufs, sem_in, sem_out = refs[:n], refs[n:2 * n], refs[2 * n:3 * n], refs[3 * n], refs[3 * n + 1]
        reads = [pltpu.make_async_copy(ins[i].at[pl.ds(r, w), :], bufs[i].at[pl.ds(r, w), :], sem_in.at[k])
                 for k, (i, r, w) in enumerate(cuts)]
        writes = [pltpu.make_async_copy(bufs[i].at[pl.ds(r, w), :], outs[i].at[pl.ds(r, w), :], sem_out.at[k])
                  for k, (i, r, w) in enumerate(cuts)]
        for cp in reads:
            cp.start()
        for rd, wr in zip(reads, writes):
            rd.wait()
            wr.start()
        for wr in writes:
            wr.wait()

    any_spec = pl.BlockSpec(memory_space=pl.ANY)
    return pl.pallas_call(
        kernel,
        name='write_out',
        out_shape=[jax.ShapeDtypeStruct(a.shape, a.dtype) for a in arrays],
        in_specs=[any_spec] * n,
        out_specs=[any_spec] * n,
        scratch_shapes=[pltpu.VMEM(a.shape, a.dtype) for a in arrays]
        + [pltpu.SemaphoreType.DMA((len(cuts),)), pltpu.SemaphoreType.DMA((len(cuts),))],
        compiler_params=pltpu.CompilerParams(vmem_limit_bytes=67043328),
    )(*arrays)


def solution(mesh):
    tp_size = mesh.shape['tp']
    side_size = mesh.shape['side']
    rows_spec = P(('pair', 'side'), None)
    batch_spec = P(('pair', 'side'), None, None)
    cache_spec = P(('pair', 'side'), None, None, None, 'tp', None)
    prompt_spec = P(('pair', 'side'), None, None, 'tp', None)

    def local_step(x_loc, req_len, dest, w_qkv, w_out, w_gate, w_up, w_down, y_loc, kc_loc, vc_loc, clen_loc):
        R, D = x_loc.shape
        B, T, slots, HD = kc_loc.shape[2:]
        Q, F = w_out.shape[1], w_gate.shape[2]
        KV = (w_qkv.shape[2] - Q) // 2
        max_req = 2 * R - R // 4
        kernel, scratch, _ = make_kernel(tp_size, side_size, R, D, B, T, Q, KV, HD, F, max_req)
        half = HD // 2
        inv_freq = np.float32(ROPE_BASE) ** (-np.arange(half, dtype=np.float32) / np.float32(half))
        table = np.zeros((8, HD), np.float32)
        table[0] = np.concatenate([inv_freq, inv_freq])
        table[1] = np.concatenate([-np.ones(half), np.ones(half)])
        fq = jnp.asarray(table)
        any_spec = pl.BlockSpec(memory_space=pl.ANY)
        CK = B * T * slots
        hid, dec, kp, vp, kn, vn = pl.pallas_call(
            kernel,
            name='prefill_decode',
            out_shape=[jax.ShapeDtypeStruct(s, BF) for s in
                       ((R, D), (B, D), (max_req * 2, HD), (max_req * 2, HD), (CK, HD), (CK, HD))],
            in_specs=[any_spec] * 13,
            out_specs=[any_spec] * 6,
            scratch_shapes=scratch,
            compiler_params=pltpu.CompilerParams(collective_id=0, has_side_effects=True, vmem_limit_bytes=67043328),
        )(x_loc, y_loc[0], w_qkv[0], w_out[0], w_gate[0], w_up[0], w_down[0],
          kc_loc.reshape(CK, HD), vc_loc.reshape(CK, HD), req_len, dest, clen_loc[0], fq)
        hid, dec, kp, vp, kn, vn = write_out(hid, dec, kp, vp, kn, vn)
        cache = (1, 1, B, T, slots, HD)
        prompt = (1, 1, max_req, slots, HD)
        return hid, dec[None], kp.reshape(prompt), vp.reshape(prompt), kn.reshape(cache), vn.reshape(cache)

    return jax.shard_map(local_step, mesh=mesh,
                         in_specs=(rows_spec, P('pair'), P('pair'), P(), P(), P(), P(), P(), batch_spec, cache_spec, cache_spec, rows_spec),
                         out_specs=(rows_spec, batch_spec, prompt_spec, prompt_spec, cache_spec, cache_spec),
                         check_vma=False)
```

```python
import jax
import jax.numpy as jnp
import numpy as np
from jax import lax
from jax.experimental import pallas as pl
from jax.experimental.pallas import tpu as pltpu
from jax.sharding import PartitionSpec as P

ROPE_BASE = 10000.0
NORM_EPS = 1e-5
BF = jnp.bfloat16
F32 = jnp.float32
CW = 256
GU_SLOTS = 10
MESH = pl.DeviceIdType.MESH


def mult(v, m):
    return pl.multiple_of(v, m)


def make_kernel(tp_size, side_size, R, D, B, T, Q, KV, HD, F, max_req):
    heads_local = Q // HD // tp_size
    rep = heads_local // 2
    hw = rep * HD
    qw = 2 * hw
    RT = R // tp_size
    DH = D // 2
    FH = F // 2
    M1 = R + B
    M2 = 2 * RT + 2 * B
    n_kv, n_q = 2 * 2 * HD // CW, qw // CW
    n_o, n_g, n_d = DH // CW, FH // CW, DH // CW
    wo_base = -(-(n_kv + n_q) * D // F) * F
    gu_base = wo_base + n_o * Q
    slab_rows = gu_base + GU_SLOTS * 2 * D
    CK = B * T * 2
    PR = max_req * 2
    scale = HD ** -0.5
    WK = max_req + RT
    n_first = wo_base // F
    AW = max(w for w in range(CW, D + 1, CW) if FH % w == 0)
    AB, AN = AW // CW, FH // AW
    nblk = side_size

    def kernel(x_h, y_h, wqkv_h, wo_h, wg_h, wu_h, wd_h, kc_h, vc_h, rl_h, dst_h, cl_h, fq_h,
               hid_o, dec_o, kp_o, vp_o, kn_o, vn_o,
               rl, dst, cl, fq, slab, ub, ys, raw, qs, kva, knv, kcs, vcs, cos_s, sin_s, bias_s,
               dcs, cst, ctxr, xres, hf, outst, hid, decb,
               in_sem, w_sem, g_sem, d_sem, xr_s, xr_r, kx_s, kx_r, cx_s, cx_r, cf_s, cf_r,
               dx_s, dx_r, df_s, df_r, h_s, h_r, a_s, a_r, f_s, f_r, r_s, r_r, o_sem):
        xs, xn = ub.at[pl.ds(0, R), :], ub.at[pl.ds(R, M1), :]
        side = lax.axis_index('side')
        tp = lax.axis_index('tp')
        core = lax.rem(side, 2)
        oc = 1 - core
        partner = side + 1 - 2 * core
        left = lax.rem(side + side_size - 2, side_size)
        right = lax.rem(side + 2, side_size)
        far = lax.rem(side + 4, side_size)
        p_left = lax.rem(partner + side_size - 2, side_size)
        p_right = lax.rem(partner + 2, side_size)
        p_far = lax.rem(partner + 4, side_size)

        def at(d):
            return lax.rem(tp + d, tp_size)

        def dev(s, t):
            return {'side': s, 'tp': t}

        q_cols0, k_cols0, v_cols0 = 0, Q, Q + KV
        hcol = [tp * hw, (tp + tp_size) * hw]
        kcol = [k_cols0 + tp * HD, k_cols0 + (tp + tp_size) * HD]
        vcol = [v_cols0 + tp * HD, v_cols0 + (tp + tp_size) * HD]

        def pieces(u):
            if u < 2:
                return [(kcol[u], 0, HD), (vcol[u], HD, HD)]
            lo, hi = (u - 2) * CW, (u - 1) * CW
            out = []
            for j in range(2):
                a, b = max(lo, j * hw), min(hi, (j + 1) * hw)
                if a < b:
                    out.append((hcol[j] + (a - j * hw), a - lo, b - a))
            return out

        def start_qkv(u):
            for src, d0, w in pieces(u):
                pltpu.make_async_copy(wqkv_h.at[:, pl.ds(mult(src, 128), w)],
                                      slab.at[pl.ds(u * D, D), pl.ds(d0, w)], w_sem.at[u]).start()

        def slab_wait(base, rows, sem):
            pltpu.make_async_copy(slab.at[pl.ds(base, rows), :], slab.at[pl.ds(base, rows), :], sem).wait()

        def start_wo(u):
            col = mult(core * DH + u * CW, 128)
            pltpu.make_async_copy(wo_h.at[:, pl.ds(col, CW)], slab.at[pl.ds(wo_base + u * Q, Q), :],
                                  w_sem.at[n_kv + n_q + u]).start()

        def start_gu(j, slot):
            col = mult(core * FH + j * CW, 128)
            base = mult(gu_base + slot * (2 * D), 256)
            pltpu.make_async_copy(wg_h.at[:, pl.ds(col, CW)], slab.at[pl.ds(base, D), :], g_sem.at[slot]).start()
            pltpu.make_async_copy(wu_h.at[:, pl.ds(col, CW)], slab.at[pl.ds(mult(base + D, 256), D), :], g_sem.at[slot]).start()

        def d_copy(n):
            return pltpu.make_async_copy(wd_h.at[:, pl.ds(mult(core * DH + n * CW, 128), CW)],
                                         slab.at[pl.ds(mult(n * F, 256), F), :], d_sem.at[n])

        small = [pltpu.make_async_copy(a, b, in_sem.at[6 + i])
                 for i, (a, b) in enumerate(((rl_h, rl), (dst_h, dst), (cl_h, cl), (fq_h, fq)))]
        XC = 4
        x_in = [pltpu.make_async_copy(x_h.at[pl.ds(i * (R // XC), R // XC), :], xs.at[pl.ds(i * (R // XC), R // XC), :],
                                      in_sem.at[10 + i]) for i in range(XC)]
        y_in = pltpu.make_async_copy(y_h, ys, in_sem.at[1])
        for cp in small + x_in + [y_in]:
            cp.start()
        start_qkv(0)

        peers = [(partner, tp), (left, tp), (right, tp), (side, at(1)), (side, at(tp_size - 1)), (side, at(2)),
                 (partner, at(1)), (partner, at(tp_size - 1))]
        barrier = pltpu.get_barrier_semaphore()
        for s, t in peers:
            pl.semaphore_signal(barrier, inc=1, device_id=dev(s, t), device_id_type=MESH)

        kc_in = pltpu.make_async_copy(kc_h, kcs, in_sem.at[2])
        vc_in = pltpu.make_async_copy(vc_h, vcs, in_sem.at[3])
        row_t = mult(tp * RT, RT)
        my_cols = mult(core * DH, 128)
        xres_l = [pltpu.make_async_copy(x_h.at[pl.ds(row_t, RT), pl.ds(my_cols, DH)],
                                        xres.at[pl.ds(mult(core * RT, RT), RT), :], in_sem.at[4]),
                  pltpu.make_async_copy(y_h.at[:, pl.ds(my_cols, DH)],
                                        xres.at[pl.ds(mult(2 * RT + core * B, B), B), :], in_sem.at[5])]

        def seg_of(rows):
            seg = jnp.zeros_like(rows)
            total = jnp.int32(0)
            for r in range(nblk):
                total = total + rl[r]
                seg = jnp.where(rows >= total, total, seg)
            return seg

        for cp in small:
            cp.wait()
        idx = lax.broadcasted_iota(jnp.int32, (M1, 1), 0)
        rows = idx + side * R
        pos = rows - seg_of(rows)
        for b in range(B):
            pos = jnp.where(idx == R + b, cl[b], pos)
        ang = pos.astype(F32) * fq[0:1, :]
        cos_s[...] = jnp.cos(ang)
        sin_s[...] = jnp.sin(ang) * fq[1:2, :]

        def norm(v):
            w = v.astype(F32)
            sc = lax.rsqrt(jnp.sum(w * w, axis=-1, keepdims=True) / D + NORM_EPS)
            return (w * sc).astype(BF)

        for i in range(XC):
            x_in[i].wait()
            start_qkv(i + 1)

            def norm_x(k, c, i=i):
                r = pl.ds(mult(i * (R // XC) + k * 32, 32), 32)
                xn[r, :] = norm(xs[r, :])
                return c

            lax.fori_loop(0, R // XC // 32, norm_x, 0, unroll=True)
        for u in range(XC + 1, n_kv + n_q):
            start_qkv(u)
        y_in.wait()
        xn[pl.ds(R, B), :] = norm(ys[...])

        def remote(src, dst_ref, ss, rs, s, t):
            return pltpu.make_async_remote_copy(src_ref=src, dst_ref=dst_ref, send_sem=ss, recv_sem=rs,
                                                device_id=dev(s, t), device_id_type=MESH)

        his_cols = mult(oc * DH, 128)
        xres_r = [remote(x_h.at[pl.ds(row_t, RT), pl.ds(his_cols, DH)], xres.at[pl.ds(mult(core * RT, RT), RT), :],
                         xr_s.at[0], xr_r.at[0], partner, tp),
                  remote(y_h.at[:, pl.ds(his_cols, DH)], xres.at[pl.ds(mult(2 * RT + core * B, B), B), :],
                         xr_s.at[1], xr_r.at[1], partner, tp)]

        def project(u):
            w = slab[pl.ds(mult(u * D, 256), D), :]
            raw[pl.ds(mult(u * M1, 16), M1), :] = jnp.dot(xn[...], w, preferred_element_type=F32).astype(BF)

        def rope(v):
            w = v.astype(F32)
            return (w * cos_s[...] + pltpu.roll(w, HD // 2, 1) * sin_s[...]).astype(BF)


        def blk(b, i0, n):
            return kva.at[pl.ds(i0, n), pl.ds(mult(b * R, R), R), :]

        plan = [(side, 0, 1, right, left), (side, 1, 1, right, left),
                (side, 0, 1, partner, partner), (side, 1, 1, partner, partner),
                (side, 0, 2, left, right),
                (left, 0, 1, partner, p_left), (left, 1, 1, partner, p_left),
                (left, 0, 1, right, far),
                (right, 0, 2, partner, p_right), (right, 1, 1, left, far),
                (far, 0, 1, partner, p_far), (far, 1, 1, partner, p_far)]
        kx = [remote(blk(b, i0, n), blk(b, i0, n), kx_s.at[i], kx_r.at[i], to, tp)
              for i, (b, i0, n, to, _) in enumerate(plan)]

        def got(i):
            ref = blk(plan[i][4], plan[i][1], plan[i][2])
            pltpu.make_async_copy(ref, ref, kx_r.at[i]).wait()

        own_rows = pl.ds(mult(side * R, R), R)
        pl.semaphore_wait(barrier, len(peers))

        def keys_values(j, c):
            slab_wait(mult(j * D, 256), D, w_sem.at[j])
            project(j)
            k_j = rope(raw[pl.ds(mult(j * M1, 16), M1), pl.ds(0, HD)])
            v_j = raw[pl.ds(mult(j * M1, 16), M1), pl.ds(HD, HD)]
            kva[j, own_rows, pl.ds(0, HD)] = k_j[:R]
            kva[j, own_rows, pl.ds(HD, HD)] = v_j[:R]
            ref = blk(side, j, 1)
            remote(ref, ref, kx_s.at[j], kx_r.at[j], right, tp).start()
            remote(ref, ref, kx_s.at[2 + j], kx_r.at[2 + j], partner, tp).start()
            knv[pl.ds(mult(j * B, B), B), pl.ds(0, HD)] = k_j[R:]
            knv[pl.ds(mult(j * B, B), B), pl.ds(HD, HD)] = v_j[R:]
            return c

        lax.fori_loop(0, 2, keys_values, 0)
        kx[4].start()
        for cp in xres_r:
            cp.start()
        knv[:, pl.ds(2 * HD, HD)] = jnp.ones((2 * B, HD), BF)

        for cp in [kc_in, vc_in] + xres_l:
            cp.start()
        for u in range(n_o):
            start_wo(u)
        for u in range(n_kv, n_kv + n_q):
            slab_wait(u * D, D, w_sem.at[u])

        def queries(i, c):
            for u in range(n_q):
                raw[pl.ds((n_kv + u) * M1, M1), :] = jnp.dot(xn[...], slab[pl.ds(mult((n_kv + u + i) * D, 256), D), :], preferred_element_type=F32).astype(BF)
            return c

        lax.fori_loop(0, tp // tp_size + 1, queries, 0)
        for slot in range(GU_SLOTS):
            start_gu(slot, slot)
        for n in range(n_first):
            d_copy(n).start()
        for h in range(heads_local):
            u, off = divmod(h * HD, CW)
            qs[h] = rope(raw[pl.ds((n_kv + u) * M1, M1), pl.ds(off, HD)])

        kc_in.wait()
        vc_in.wait()
        lane2 = lax.broadcasted_iota(jnp.int32, (1, 2 * B), 1)
        len2 = jnp.zeros((1, 2 * B), jnp.int32)
        for b in range(B):
            len2 = jnp.where(lax.rem(lane2, B) == b, cl[b], len2)
        code2 = (lax.rem(lane2, B) * T + len2) * 2 + lane2 // B
        CH = 256

        def insert(i, c):
            r0 = mult(i * CH, CH)
            rr = lax.broadcasted_iota(jnp.int32, (CH, 1), 0) + r0
            pick = jnp.where(rr == code2, 1.0, 0.0).astype(BF)
            new = jnp.dot(pick, knv[...], preferred_element_type=F32)
            hit = new[:, 2 * HD:] > 0.5
            sl = pl.ds(r0, CH)
            kcs[sl, :] = jnp.where(hit, new[:, :HD], kcs[sl, :].astype(F32)).astype(BF)
            vcs[sl, :] = jnp.where(hit, new[:, HD:2 * HD], vcs[sl, :].astype(F32)).astype(BF)
            return c

        lax.fori_loop(0, CK // CH, insert, 0)
        inner = side >= 2

        @pl.when(inner)
        def _():
            got(0)
            kx[5].start()
            kx[7].start()

        kn_out = pltpu.make_async_copy(kcs, kn_o, o_sem.at[0])
        vn_out = pltpu.make_async_copy(vcs, vn_o, o_sem.at[1])
        kn_out.start()
        vn_out.start()

        HB = heads_local * B
        q_dec = qs[:, pl.ds(R, B), :].reshape(HB, HD)
        s_dec = lax.dot_general(q_dec, kcs[...], (((1,), (1,)), ((), ())), preferred_element_type=F32) * scale
        qi = lax.broadcasted_iota(jnp.int32, (HB, 1), 0)
        ki = lax.broadcasted_iota(jnp.int32, (1, CK), 1)
        q_len = jnp.zeros((HB, 1), jnp.int32)
        for b in range(B):
            q_len = jnp.where(lax.rem(qi, B) == b, cl[b], q_len)
        q_code = lax.rem(qi, B) * 2 + qi // (rep * B)
        k_code = (ki // (2 * T)) * 2 + lax.rem(ki, 2)
        k_pos = lax.rem(ki // 2, T)
        s_dec = jnp.where((q_code == k_code) & (k_pos <= q_len), s_dec, -1e30)
        e_dec = jnp.exp(s_dec - jnp.max(s_dec, axis=-1, keepdims=True))
        p_dec = (e_dec / jnp.sum(e_dec, axis=-1, keepdims=True)).astype(BF)
        c_dec = jnp.dot(p_dec, vcs[...], preferred_element_type=F32).astype(BF)
        for h in range(heads_local):
            dcs[h // rep, :, pl.ds((h % rep) * HD, HD)] = c_dec[h * B:(h + 1) * B]
        dec_rows = pl.ds(mult(2 * RT + core * B, B), B)
        hops = (2, 1, 3, 0)
        srcs = (2, 3, 1)
        dec_at = lambda t, rows_: ctxr.at[:, rows_, pl.ds(mult(t * hw, 128), hw)]
        dx = [remote(dcs, dec_at(tp, dec_rows), dx_s.at[k], dx_r.at[k], side, at(hops[k])) for k in range(3)]
        for cp in dx:
            cp.start()
        dec_at(tp, dec_rows)[...] = dcs[...]
        df_own = remote(dcs, dec_at(tp, dec_rows), df_s.at[3], df_r.at[3], partner, tp)
        df_own.start()

        win = []
        for k in range(4):
            r0 = mult(at(hops[k]) * RT, RT)
            lead = side * R + r0 - max_req
            lead = lead * ((lead + 2 * nblk * R) // (2 * nblk * R))
            win.append((r0, mult(lead, RT)))
            q_row = side * R + r0 + lax.broadcasted_iota(jnp.int32, (RT, 1), 0)
            key_row = lead + lax.broadcasted_iota(jnp.int32, (1, WK), 1)
            bias = jnp.where((key_row >= seg_of(q_row)) & (key_row <= q_row), 0.0, -1e30)
            for i in range(WK // CW):
                bias_s[i, pl.ds(k * RT, RT), :] = bias[:, i * CW:(i + 1) * CW]
        got(2)

        @pl.when(inner)
        def _():
            got(5)

        pre_rows = pl.ds(mult(core * RT, RT), RT)
        QR = rep * RT

        def attend(j, k):
            r0, lead = win[k]
            q = qs[pl.ds(j * rep, rep), pl.ds(r0, RT), :].reshape(QR, HD)
            held = lambda i: kva[j, pl.ds(lead, WK), pl.ds(i * HD, HD)]
            s = lax.dot_general(q, held(0), (((1,), (1,)), ((), ())), preferred_element_type=F32)
            s = s.reshape(rep, RT, WK) * scale + jnp.concatenate([bias_s[i, pl.ds(k * RT, RT), :] for i in range(WK // CW)], axis=-1)[None]
            e = jnp.exp(s - jnp.max(s, axis=-1, keepdims=True))
            p = (e * (1.0 / jnp.sum(e, axis=-1, keepdims=True))).astype(BF).reshape(QR, WK)
            o = jnp.dot(p, held(1), preferred_element_type=F32)
            o = o.astype(BF)
            for h in range(rep):
                cst[j, k, :, pl.ds(h * HD, HD)] = o[h * RT:(h + 1) * RT]

        def ctx_at(t, rows_, j):
            return ctxr.at[j, rows_, pl.ds(mult(t * hw, 128), hw)]

        cx = [[remote(cst.at[j, k], ctx_at(tp, pre_rows, j), cx_s.at[j, k], cx_r.at[j, k], side, at(hops[k]))
               for k in range(3)] for j in range(2)]
        cf = [[remote(ctx_at(at(srcs[k]), pre_rows, j), ctx_at(at(srcs[k]), pre_rows, j), cf_s.at[j, k], cf_r.at[j, k], partner, tp)
               for k in range(3)] + [remote(cst.at[j, 3], ctx_at(tp, pre_rows, j), cf_s.at[j, 3], cf_r.at[j, 3], partner, tp)]
              for j in range(2)]

        def pass_ctx(j, k):
            ref = ctx_at(at(srcs[k]), pre_rows, j)
            pltpu.make_async_copy(ref, ref, cx_r.at[j, k]).wait()
            cf[j][k].start()

        df = []
        for j in range(2):
            for k in range(4):
                if k % 2 == 0:
                    attend(j, k)
                    attend(j, k + 1)
                if k < 3:
                    cx[j][k].start()
                else:
                    ctx_at(tp, pre_rows, j)[...] = cst[j, 3]
                    cf[j][3].start()
                if j == 0 and k == 1:
                    @pl.when(inner)
                    def _():
                        got(1)
                        kx[6].start()
            if j == 0:
                got(3)

                @pl.when(inner)
                def _():
                    got(6)

        for k in (1, 0, 2):
            pass_ctx(0, k)
        for k in range(3):
            ref = dec_at(at(srcs[k]), dec_rows)
            pltpu.make_async_copy(ref, ref, dx_r.at[k]).wait()
            df.append(remote(ref, ref, df_s.at[k], df_r.at[k], partner, tp))
            df[k].start()
        for k in (1, 0, 2):
            pass_ctx(1, k)
        p_pre = pl.ds(mult(oc * RT, RT), RT)
        p_dec_rows = pl.ds(mult(2 * RT + oc * B, B), B)
        for k in range(4):
            t = at(srcs[k]) if k < 3 else tp
            for j in range(2):
                ref = ctx_at(t, p_pre, j)
                pltpu.make_async_copy(ref, ref, cf_r.at[j, k]).wait()
            ref = dec_at(t, p_dec_rows)
            pltpu.make_async_copy(ref, ref, df_r.at[k]).wait()
        for cp in xres_l:
            cp.wait()
        for i, cp in enumerate(xres_r):
            cp.wait_send()
        ref = xres.at[p_pre, :]
        pltpu.make_async_copy(ref, ref, xr_r.at[0]).wait()
        ref = xres.at[p_dec_rows, :]
        pltpu.make_async_copy(ref, ref, xr_r.at[1]).wait()

        def h_copy(u):
            ref = hf.at[:, pl.ds(mult(core * DH + u * CW, CW), CW)]
            return remote(ref, ref, h_s.at[u], h_r.at[u], partner, tp)

        OU = 2

        def out_proj(i, c):
            for k in range(OU):
                u = i * OU + k
                slab_wait(mult(wo_base + u * Q, 256), Q, w_sem.at[n_kv + n_q + u])
            for k in range(OU):
                u = i * OU + k
                acc = jnp.zeros((M2, CW), F32)
                for j in range(2):
                    acc = acc + jnp.dot(ctxr[j], slab[pl.ds(mult(wo_base + u * Q + j * (Q // 2), 256), Q // 2), :],
                                        preferred_element_type=F32)
                res = xres[:, pl.ds(mult(u * CW, CW), CW)].astype(F32)
                hf[:, pl.ds(mult(core * DH + u * CW, CW), CW)] = (res + acc.astype(BF).astype(F32)).astype(BF)
            for k in range(OU):
                h_copy(i * OU + k).start()
            for n in range(n_first, n_d):
                if (n + 1) * F <= gu_base:
                    @pl.when(i == (min((n + 1) * F - wo_base, n_o * Q) - 1) // (OU * Q))
                    def _(n=n):
                        d_copy(n).start()
            return c

        lax.fori_loop(0, n_o // OU, out_proj, 0)
        @pl.when(side < 2)
        def _():
            for i in (0, 1):
                got(i)
            for i in (5, 6, 7):
                kx[i].start()

        got(4)
        kx[8].start()
        kx[9].start()
        for u in range(n_o):
            ref = hf.at[:, pl.ds(mult(oc * DH + u * CW, CW), CW)]
            pltpu.make_async_copy(ref, ref, h_r.at[u]).wait()

        for cp in df + [df_own] + cf[0] + cf[1]:
            cp.wait_send()

        def norm_h(i, c):
            r = pl.ds(mult(i * 32, 32), 32)
            v = norm(hf[r, :])
            for j in range(2):
                ctxr[j, r, :] = v[:, j * DH:(j + 1) * DH]
            return c

        lax.fori_loop(0, M2 // 32, norm_h, 0, unroll=True)

        def act_at(c_of, j):
            g = c_of * n_g + j
            return ub.at[pl.ds(mult((g // AB) * M2, 16), M2), pl.ds(mult(lax.rem(g, AB) * CW, CW), CW)]

        def a_copy(j):
            ref = act_at(core, j)
            return remote(ref, ref, a_s.at[j], a_r.at[j], partner, tp)

        def last_slot(n):
            top = (n + 1) * F - gu_base
            slot = (top - 1) // (2 * D)
            return slot + ((n_g - 1 - slot) // GU_SLOTS) * GU_SLOTS

        def gu_base_of(j):
            return mult(gu_base + lax.rem(j, GU_SLOTS) * (2 * D), 256)

        def gu_next(j):
            @pl.when(j + GU_SLOTS < n_g)
            def _():
                start_gu(j + GU_SLOTS, lax.rem(j, GU_SLOTS))

            for n in range(gu_base // F, n_d):
                @pl.when(j == last_slot(n))
                def _(n=n):
                    d_copy(n).start()

        GU = 2

        def gate_up(i, c):
            for k in range(GU):
                j = i * GU + k
                slab_wait(gu_base_of(j), 2 * D, g_sem.at[lax.rem(j, GU_SLOTS)])
            for k in range(GU):
                j = i * GU + k
                base = gu_base_of(j)
                half = lambda i: slab[pl.ds(mult(base + i * DH, 256), DH), :]
                g = jnp.dot(ctxr[0], half(0), preferred_element_type=F32) + jnp.dot(ctxr[1], half(1), preferred_element_type=F32)
                u = jnp.dot(ctxr[0], half(2), preferred_element_type=F32) + jnp.dot(ctxr[1], half(3), preferred_element_type=F32)
                g = g.astype(BF).astype(F32)
                u = u.astype(BF).astype(F32)
                act_at(core, j)[...] = (g * jax.nn.sigmoid(g) * u).astype(BF)
            for k in range(GU):
                a_copy(i * GU + k).start()
            for k in range(GU):
                gu_next(i * GU + k)
            return c

        lax.fori_loop(0, n_g // GU, gate_up, 0)

        def a_got(j, c):
            ref = act_at(oc, j)
            pltpu.make_async_copy(ref, ref, a_r.at[j]).wait()
            return c

        for i in (7, 9):
            got(i)
        kx[10].start()
        kx[11].start()

        up, down = at(1), at(tp_size - 1)
        own_out = pl.ds(mult(core * RT, RT), RT)
        his_out = pl.ds(mult(oc * RT, RT), RT)
        own_dec = pl.ds(mult(2 * RT + core * B, B), B)
        his_dec = pl.ds(mult(2 * RT + oc * B, B), B)
        rows_of = lambda t: pl.ds(mult(t * RT, RT), RT)

        def f_copies(n):
            cols = pl.ds(mult(core * DH + n * CW, CW), CW)
            there = hid.at[rows_of(tp), cols]
            mine, his = outst.at[n, own_out, :], outst.at[n, his_out, :]
            return [remote(mine, there, f_s.at[0, n], f_r.at[0, n], side, up),
                    remote(mine, there, f_s.at[1, n], f_r.at[1, n], side, down),
                    remote(his, there, f_s.at[2, n], f_r.at[2, n], partner, up),
                    remote(his, there, f_s.at[3, n], f_r.at[3, n], partner, down),
                    remote(his, there, f_s.at[4, n], f_r.at[4, n], partner, tp),
                    remote(outst.at[n, his_dec, :], decb.at[:, cols], f_s.at[5, n], f_r.at[5, n], partner, tp)]

        def down_part(n, c_of):
            acc = None
            for i in range(AN):
                g = c_of * AN + i
                part = jnp.dot(ub[pl.ds(mult(g * M2, 16), M2), pl.ds(0, AW)],
                               slab[pl.ds(mult(n * F + g * AW, 256), AW), :], preferred_element_type=F32)
                acc = part if acc is None else acc + part
            return acc

        def down_end(n, acc):
            cols = pl.ds(mult(core * DH + n * CW, CW), CW)
            outst[n] = (hf[:, cols].astype(F32) + acc.astype(BF).astype(F32)).astype(BF)
            for cp in f_copies(n):
                cp.start()
            hid[rows_of(tp), cols] = outst[n, own_out, :]
            decb[:, cols] = outst[n, own_dec, :]

        EARLY = 2

        def down_first(n, c):
            d_copy(n).wait()
            bias_s[n, pl.ds(0, M2), :] = down_part(n, core)
            return c

        lax.fori_loop(0, EARLY, down_first, 0)
        lax.fori_loop(0, n_g, a_got, 0)

        def down_second(n, c):
            down_end(n, bias_s[n, pl.ds(0, M2), :] + down_part(n, oc))
            return c

        lax.fori_loop(0, EARLY, down_second, 0)

        def down_proj(n, c):
            d_copy(n).wait()
            down_end(n, down_part(n, core) + down_part(n, oc))
            return c

        lax.fori_loop(EARLY, n_d, down_proj, 0)

        def piece(t, c_from, n, of=hid):
            return of.at[rows_of(t), pl.ds(mult(c_from * DH + n * CW, CW), CW)]

        def arrived(ref, sem):
            pltpu.make_async_copy(ref, ref, sem).wait()

        kind = {(0, 1): 0, (1, 1): 1, (0, 0): 2, (1, 0): 3}
        relays = []
        for n in range(n_d):
            for same in (1, 0):
                c_from = core if same else oc
                if n % 2 == 0:
                    ref = piece(down, c_from, n)
                    arrived(ref, f_r.at[kind[(0, same)], n])
                    cp = remote(ref, piece(down, c_from, n, hid_o), r_s.at[same, n], r_r.at[same, n], side, up)
                else:
                    ref = piece(up, c_from, n)
                    arrived(ref, f_r.at[kind[(1, same)], n])
                    cp = remote(ref, piece(up, c_from, n, hid_o), r_s.at[same, n], r_r.at[same, n], side, down)
                cp.start()
                relays.append(cp)

        @pl.when(side < 2)
        def _():
            for i in (5, 6):
                got(i)

        for i in (8, 10, 11):
            got(i)
        start, length, total = jnp.int32(0), jnp.int32(0), jnp.int32(0)
        for r in range(nblk):
            mine = dst[r] == side
            start = start + jnp.where(mine, total, 0)
            length = length + jnp.where(mine, rl[r], 0)
            total = total + rl[r]
        IR = 128
        col = lax.broadcasted_iota(jnp.int32, (1, 2 * nblk * R), 1)

        def install(i, c):
            r = pl.ds(mult(i * IR, IR), IR)
            o_row = lax.broadcasted_iota(jnp.int32, (IR, 1), 0) + i * IR
            code = jnp.where(o_row // 2 < length, o_row // 2 + start + lax.rem(o_row, 2) * (nblk * R), -1)
            pick = jnp.where(code == col, 1.0, 0.0).astype(BF)
            out = jnp.dot(pick, kva[...].reshape(2 * nblk * R, 2 * HD), preferred_element_type=F32).astype(BF)
            raw[r, :] = out
            return c

        lax.fori_loop(0, PR // IR, install, 0)
        outs = [pltpu.make_async_copy(raw.at[pl.ds(0, PR), pl.ds(i * HD, HD)], o, o_sem.at[2 + i]) for i, o in enumerate((kp_o, vp_o))]
        for cp in outs:
            cp.start()

        def flush(t, i):
            r = rows_of(t)
            cp = pltpu.make_async_copy(hid.at[r, :], hid_o.at[r, :], o_sem.at[4 + i])
            cp.start()
            outs.append(cp)

        for n in range(n_d):
            arrived(piece(tp, oc, n), f_r.at[4, n])
            arrived(decb.at[:, pl.ds(mult(oc * DH + n * CW, CW), CW)], f_r.at[5, n])
        flush(tp, 0)
        cp = pltpu.make_async_copy(decb, dec_o, o_sem.at[8])
        cp.start()
        outs.append(cp)
        for n in range(n_d):
            for same in (1, 0):
                c_from = core if same else oc
                if n % 2 == 0:
                    arrived(piece(up, c_from, n), f_r.at[kind[(1, same)], n])
                else:
                    arrived(piece(down, c_from, n), f_r.at[kind[(0, same)], n])
        flush(up, 1)
        flush(down, 2)
        for n in range(n_d):
            for same in (1, 0):
                arrived(piece(at(2), core if same else oc, n, hid_o), r_r.at[same, n])

        for cp in kx + dx + cx[0] + cx[1] + relays:
            cp.wait_send()

        def h_done(u, c):
            h_copy(u).wait_send()
            return c

        def a_done(j, c):
            a_copy(j).wait_send()
            return c

        def f_done(n, c):
            for cp in f_copies(n):
                cp.wait_send()
            return c

        lax.fori_loop(0, n_o, h_done, 0)
        lax.fori_loop(0, n_g, a_done, 0)
        lax.fori_loop(0, n_d, f_done, 0)
        kn_out.wait()
        vn_out.wait()
        for cp in outs:
            cp.wait()

    dma = lambda *s: pltpu.SemaphoreType.DMA(s)
    scratch = [
        pltpu.SMEM((side_size,), jnp.int32), pltpu.SMEM((side_size,), jnp.int32), pltpu.SMEM((B,), jnp.int32), pltpu.VMEM((8, HD), F32),
        pltpu.VMEM((slab_rows, CW), BF),
        pltpu.VMEM((max(R + M1, 2 * AN * M2), D), BF), pltpu.VMEM((B, D), BF),
        pltpu.VMEM((max((n_kv + n_q) * M1, PR), CW), BF), pltpu.VMEM((heads_local, M1, HD), BF),
        pltpu.VMEM((2, nblk * R, 2 * HD), BF), pltpu.VMEM((2 * B, 3 * HD), BF),
        pltpu.VMEM((CK, HD), BF), pltpu.VMEM((CK, HD), BF),
        pltpu.VMEM((M1, HD), F32), pltpu.VMEM((M1, HD), F32), pltpu.VMEM((WK // CW, max(4 * RT, M2), CW), F32),
        pltpu.VMEM((2, B, hw), BF), pltpu.VMEM((2, 4, RT, hw), BF), pltpu.VMEM((2, M2, Q // 2), BF),
        pltpu.VMEM((M2, DH), BF), pltpu.VMEM((M2, D), BF),
        pltpu.VMEM((n_d, M2, CW), BF), pltpu.VMEM((R, D), BF), pltpu.VMEM((B, D), BF),
        dma(14), dma(n_kv + n_q + n_o), dma(GU_SLOTS), dma(n_d),
        dma(2), dma(2), dma(12), dma(12), dma(2, 3), dma(2, 3), dma(2, 4), dma(2, 4),
        dma(3), dma(3), dma(4), dma(4), dma(n_o), dma(n_o), dma(n_g), dma(n_g),
        dma(6, n_d), dma(6, n_d), dma(2, n_d), dma(2, n_d), dma(9),
    ]
    return kernel, scratch, (R, D, B, PR, HD, CK)


def write_out(*arrays):
    n = len(arrays)
    cuts = []
    for i, a in enumerate(arrays):
        parts = 4 if i == 0 else 1
        step = a.shape[0] // parts
        cuts += [(i, p * step, step) for p in range(parts)]

    def kernel(*refs):
        ins, outs, bufs, sem_in, sem_out = refs[:n], refs[n:2 * n], refs[2 * n:3 * n], refs[3 * n], refs[3 * n + 1]
        reads = [pltpu.make_async_copy(ins[i].at[pl.ds(r, w), :], bufs[i].at[pl.ds(r, w), :], sem_in.at[k])
                 for k, (i, r, w) in enumerate(cuts)]
        writes = [pltpu.make_async_copy(bufs[i].at[pl.ds(r, w), :], outs[i].at[pl.ds(r, w), :], sem_out.at[k])
                  for k, (i, r, w) in enumerate(cuts)]
        for cp in reads:
            cp.start()
        for rd, wr in zip(reads, writes):
            rd.wait()
            wr.start()
        for wr in writes:
            wr.wait()

    any_spec = pl.BlockSpec(memory_space=pl.ANY)
    return pl.pallas_call(
        kernel,
        name='write_out',
        out_shape=[jax.ShapeDtypeStruct(a.shape, a.dtype) for a in arrays],
        in_specs=[any_spec] * n,
        out_specs=[any_spec] * n,
        scratch_shapes=[pltpu.VMEM(a.shape, a.dtype) for a in arrays]
        + [pltpu.SemaphoreType.DMA((len(cuts),)), pltpu.SemaphoreType.DMA((len(cuts),))],
        compiler_params=pltpu.CompilerParams(vmem_limit_bytes=67043328),
    )(*arrays)


def solution(mesh):
    tp_size = mesh.shape['tp']
    side_size = mesh.shape['side']
    rows_spec = P(('pair', 'side'), None)
    batch_spec = P(('pair', 'side'), None, None)
    cache_spec = P(('pair', 'side'), None, None, None, 'tp', None)
    prompt_spec = P(('pair', 'side'), None, None, 'tp', None)

    def local_step(x_loc, req_len, dest, w_qkv, w_out, w_gate, w_up, w_down, y_loc, kc_loc, vc_loc, clen_loc):
        R, D = x_loc.shape
        B, T, slots, HD = kc_loc.shape[2:]
        Q, F = w_out.shape[1], w_gate.shape[2]
        KV = (w_qkv.shape[2] - Q) // 2
        max_req = 2 * R - R // 4
        kernel, scratch, _ = make_kernel(tp_size, side_size, R, D, B, T, Q, KV, HD, F, max_req)
        half = HD // 2
        inv_freq = np.float32(ROPE_BASE) ** (-np.arange(half, dtype=np.float32) / np.float32(half))
        table = np.zeros((8, HD), np.float32)
        table[0] = np.concatenate([inv_freq, inv_freq])
        table[1] = np.concatenate([-np.ones(half), np.ones(half)])
        fq = jnp.asarray(table)
        any_spec = pl.BlockSpec(memory_space=pl.ANY)
        CK = B * T * slots
        hid, dec, kp, vp, kn, vn = pl.pallas_call(
            kernel,
            name='prefill_decode',
            out_shape=[jax.ShapeDtypeStruct(s, BF) for s in
                       ((R, D), (B, D), (max_req * 2, HD), (max_req * 2, HD), (CK, HD), (CK, HD))],
            in_specs=[any_spec] * 13,
            out_specs=[any_spec] * 6,
            scratch_shapes=scratch,
            compiler_params=pltpu.CompilerParams(collective_id=0, has_side_effects=True, vmem_limit_bytes=67043328),
        )(x_loc, y_loc[0], w_qkv[0], w_out[0], w_gate[0], w_up[0], w_down[0],
          kc_loc.reshape(CK, HD), vc_loc.reshape(CK, HD), req_len, dest, clen_loc[0], fq)
        hid, dec, kp, vp, kn, vn = write_out(hid, dec, kp, vp, kn, vn)
        cache = (1, 1, B, T, slots, HD)
        prompt = (1, 1, max_req, slots, HD)
        return hid, dec[None], kp.reshape(prompt), vp.reshape(prompt), kn.reshape(cache), vn.reshape(cache)

    return jax.shard_map(local_step, mesh=mesh,
                         in_specs=(rows_spec, P('pair'), P('pair'), P(), P(), P(), P(), P(), batch_spec, cache_spec, cache_spec, rows_spec),
                         out_specs=(rows_spec, batch_spec, prompt_spec, prompt_spec, cache_spec, cache_spec),
                         check_vma=False)
```
